512 devices in a mesh: cells: 128 (over z, x_hi, y), genes: 4 (over x_lo, core).
Axes of the slice: x: 4 (x_hi: 2, x_lo: 2; x = x_hi * 2 + x_lo), y: 4, z: 16, core: 2. Of those that a mesh axis runs over, the one named last changes fastest.
Arguments:
- counts: bfloat16 [16384, 16384], P('cells', 'genes'), may hold values from 0 to 254
- occupancy: int32 [128, 128], P('cells', 'genes'), may hold values 0 or 1
- start_basis: bfloat16 [64, 16384], P(None, 'genes'), may hold values from -0.046875 to 0.046875
Outputs:
- new_basis: float32 [64, 16384], P(None, ('genes', 'cells'))
The draws below stay inside these ranges and needn't reach their ends.
All inputs are finite; a program needn't handle non-finite values. No bound on the sum of `occupancy` on one device may be relied on, other than what follows from the above.
Results may differ from the reference program's by a relative error of at most 0.01.
Values sent between devices are 32-bit elements; how exact they have to be, the bound alone decides.
A program may use at most 64 MiB of HBM per device.

```python
import math
import jax
import jax.numpy as jnp
from jax import lax

GENES = 16384
COMPS = 64
TILE = 128
CELLS = 16384


def draw_counts(key, part):
    key_rows, key_cols, key_cells = jax.random.split(jax.random.fold_in(key, 17), 3)
    row_high = jax.random.randint(key_rows, (CELLS, 1), 2, 18)
    col_high = jax.random.randint(key_cols, (1, GENES), 1, 16)
    whole = jax.random.randint(key_cells, (CELLS, GENES), 0, row_high * col_high)
    return whole.astype(jnp.float32).astype(jnp.bfloat16)


def with_ends(entries, key, smallest, largest):
    index_at = [jax.random.randint(jax.random.fold_in(key, axis), (), 0, length) for axis, length in enumerate(entries.shape)]
    widest = entries.shape.index(max(entries.shape))
    beside = index_at[:widest] + [(index_at[widest] + 1) % entries.shape[widest]] + index_at[widest + 1:]
    return entries.at[tuple(index_at)].set(smallest).at[tuple(beside)].set(largest)


def shard_levels(own_key, extent, shards, smallest, largest):
    def one(axis_at, blocks):
        heights = jax.random.uniform(jax.random.fold_in(jax.random.fold_in(own_key, 6), axis_at), (blocks,), jnp.float32, smallest / len(shards), largest / len(shards))
        return jnp.repeat(jnp.exp(heights), extent[axis_at] // blocks).reshape((-1,) + (1,) * (len(extent) - axis_at - 1))

    gain = one(*shards[0])
    for cut in shards[1:]:
        gain = gain * one(*cut)
    return gain


def normal_values(rng, dims, width, limit, shards=(), held_as=jnp.bfloat16):
    result = width * jax.random.normal(rng, dims, jnp.float32)
    if shards:
        result = result * shard_levels(rng, dims, shards, -0.22, 0.18)
    return jnp.clip(result, -limit, limit).astype(held_as)


def setup_inputs(seed: int = 0) -> dict:
    arg_keys = jax.random.split(jax.random.key(seed), 4)
    counts = draw_counts(jax.random.fold_in(arg_keys[3], 71), 0)
    occupancy = with_ends((jax.random.randint(arg_keys[1], (CELLS // TILE, GENES // TILE), 0, 4) < 3).astype(jnp.int32), jax.random.fold_in(arg_keys[1], 1), 0, 1)
    start_basis = normal_values(arg_keys[2], (COMPS, GENES), GENES ** -0.5, 0.046875, ((1, 4),))
    return {"counts": counts, "occupancy": occupancy, "start_basis": start_basis}


def reference(counts, occupancy, start_basis):
    tile_rows, tile_cols = occupancy.shape
    logged = jnp.log1p(counts.astype(jnp.float32)).reshape(tile_rows, TILE, tile_cols, TILE)
    logged = (logged * occupancy.astype(jnp.float32)[:, None, :, None]).reshape(counts.shape)
    gene_mean = lax.optimization_barrier(jnp.sum(logged, axis=0)) / CELLS
    centered = (logged - gene_mean).astype(jnp.bfloat16)
    scores = lax.dot_general(start_basis.astype(jnp.float32), centered.astype(jnp.float32), (((1,), (1,)), ((), ())), preferred_element_type=jnp.float32)
    score_high = scores.astype(jnp.bfloat16)
    score_low = (scores - score_high.astype(jnp.float32)).astype(jnp.bfloat16)
    stacked = jnp.concatenate([score_high, score_low], axis=0)
    both = jnp.dot(stacked.astype(jnp.float32), centered.astype(jnp.float32), preferred_element_type=jnp.float32)
    spread = both[:COMPS] + both[COMPS:]
    gram_sum = lax.dot_general(spread.astype(jnp.float32), spread.astype(jnp.float32), (((1,), (1,)), ((), ())), precision=lax.Precision.HIGHEST, preferred_element_type=jnp.float32)
    factor = jnp.linalg.cholesky(gram_sum)
    basis_now = jax.scipy.linalg.solve_triangular(factor, spread, lower=True)
    return basis_now * math.sqrt(GENES)
```

```python
import functools
import math

import jax
import jax.numpy as jnp
from jax import lax
from jax.experimental import pallas as pl
from jax.experimental.pallas import tpu as pltpu
from jax.sharding import PartitionSpec as P

F32 = jnp.float32
BF16 = jnp.bfloat16
MESH = pl.DeviceIdType.MESH
Z, H, Y, XL, CORE = 16, 2, 4, 2, 2
LANES = 128
OFFSETS = (8, 7, 9, 6, 10, 5, 11, 4, 12, 3, 13, 2, 14, 1, 15, 0)
CHUNKS = 4
NT = (((1,), (1,)), ((), ()))


def device(z, h, y, xl, core):
    return ((z * H + h) * Y + y, xl * CORE + core)


def total_of(values):
    values = list(values)
    while len(values) > 1:
        values = [sum(values[i : i + 2][1:], values[i]) for i in range(0, len(values), 2)]
    return values[0]


def solve(gram, right):
    blocks = gram.shape[0] // 8
    left = [gram[8 * b : 8 * b + 8] for b in range(blocks)]
    right = [right[8 * b : 8 * b + 8] for b in range(blocks)]
    row_at = lax.broadcasted_iota(jnp.int32, (8, LANES), 0)
    done = []
    for kb in range(blocks):
        cols = [
            [
                jnp.broadcast_to(left[b][:, 8 * kb + j : 8 * kb + j + 1], (8, LANES))
                for j in range(8)
            ]
            for b in range(kb, blocks)
        ]
        rows_left, rows_right = left[kb], right[kb]
        scale = jnp.zeros((8, LANES), F32)
        steps = []
        for j in range(8):
            pivot = jnp.broadcast_to(cols[0][j][j : j + 1], (8, LANES))
            inv = lax.rsqrt(pivot)
            scale = jnp.where(row_at == j, inv, scale)
            lower = [c[j] * inv for c in cols]
            for m in range(j + 1, 8):
                entry = jnp.broadcast_to(lower[0][m : m + 1], (8, LANES))
                for c, low in zip(cols, lower):
                    c[m] = c[m] - low * entry
            below = jnp.where(row_at > j, lower[0], 0.0)
            unit_left = jnp.broadcast_to(rows_left[j : j + 1], rows_left.shape) * inv[:, : rows_left.shape[1]]
            unit_right = jnp.broadcast_to(rows_right[j : j + 1], rows_right.shape) * inv
            rows_left = rows_left - below[:, : rows_left.shape[1]] * unit_left
            rows_right = rows_right - below * unit_right
            steps.append((lower[1:], unit_left, unit_right))
        done.append(rows_right * scale)
        for at, b in enumerate(range(kb + 1, blocks)):
            for lower, unit_left, unit_right in steps:
                left[b] = left[b] - lower[at][:, : unit_left.shape[1]] * unit_left
                right[b] = right[b] - lower[at] * unit_right
    return jnp.concatenate(done, axis=0)


def kernel(
    scaling,
    counts,
    occupancy,
    basis,
    out,
    cbuf,
    split_mean,
    aux,
    aux_in,
    score,
    score_in,
    part,
    part_in,
    dev_mean,
    mean_xy,
    turned,
    zpart,
    zaux,
    zpart_in,
    zaux_in,
    tile,
    gram,
    gram_in,
    gram_z,
    gram_z_in,
    gram_all,
    sem_score,
    sem_aux,
    sem_part,
    sem_z,
    sem_zaux,
    sem_tile,
    sem_gram,
    sem_gram_z,
    sem_core,
):
    cells_at, genes_at = lax.axis_index("cells"), lax.axis_index("genes")
    z, h, y = cells_at // (H * Y), lax.rem(cells_at // Y, H), lax.rem(cells_at, Y)
    xl, core = genes_at // CORE, lax.rem(genes_at, CORE)
    comps = basis.shape[0]
    rows = comps // Y
    cells = counts.shape[0]

    def send(src, dst, sems, index, to):
        copy = pltpu.make_async_remote_copy(
            src_ref=src,
            dst_ref=dst,
            send_sem=sems.at[(0, *index)],
            recv_sem=sems.at[(1, *index)],
            device_id=to,
            device_id_type=MESH,
        )
        copy.start()
        return copy

    def gene_peer(a):
        other = lax.rem(genes_at + a, XL * CORE)
        return device(z, h, y, other // CORE, lax.rem(other, CORE))

    def xy_place(a, b):
        return lax.rem(h + a, H), lax.rem(y + b, Y)

    def z_peer(o):
        return device(lax.rem(z + o, Z), h, y, xl, core)

    def x_peer(a):
        other = lax.rem((h * XL + xl) * CORE + core + a, H * XL * CORE)
        return device(
            z, other // (XL * CORE), y, lax.rem(other // CORE, XL), lax.rem(other, CORE)
        )

    xy_offsets = [(a, b) for a in range(H) for b in range(Y) if a or b]

    barrier = pltpu.get_barrier_semaphore()
    peers = [gene_peer(a) for a in range(1, XL * CORE)]
    peers += [device(z, *xy_place(a, b), xl, core) for a, b in xy_offsets]
    peers += [z_peer(o) for o in range(1, Z)]
    for a in range(1, XL * CORE):
        other = lax.rem(genes_at + a, XL * CORE)
        peers.append(device(z, 1 - h, y, other // CORE, lax.rem(other, CORE)))
    for peer in peers:
        pl.semaphore_signal(barrier, inc=1, device_id=peer, device_id_type=MESH)

    row_at = lax.broadcasted_iota(jnp.int32, (16, LANES), 0)
    aux[:, 16:24, :] = jnp.zeros((H, 8, LANES), F32)

    def center(zt, carry):
        for ht in range(H):
            at = pl.multiple_of((zt * H + ht) * LANES, LANES)
            entries = counts[:, pl.ds(at, LANES)].astype(F32)
            stored = occupancy[0, zt * H + ht].astype(F32)
            logged = jnp.log(1.0 + entries) * stored
            mean = jnp.sum(logged, axis=0, keepdims=True) * (1.0 / cells)
            cbuf[:, pl.ds(at, LANES)] = (logged - mean).astype(BF16)
            aux[ht, pl.ds(zt, 1), :] = mean
            high = mean.astype(BF16).astype(F32)
            middle = (mean - high).astype(BF16).astype(F32)
            low = mean - high - middle
            stacked = jnp.where(
                row_at == 0, high, jnp.where(row_at == 1, middle, jnp.where(row_at == 2, low, 0.0))
            )
            split_mean[:, pl.ds(at, LANES)] = stacked.astype(BF16)
        return carry

    lax.fori_loop(0, Z, center, 0)

    score[0:comps, :] = lax.dot_general(basis[...], cbuf[...], NT, preferred_element_type=F32)
    of_mean = lax.dot_general(split_mean[...], basis[...], NT, preferred_element_type=F32)
    score[comps : comps + 8, :] = jnp.zeros((8, LANES), F32)
    score[comps : comps + 1, 0:comps] = of_mean[0:1] + of_mean[1:2] + of_mean[2:3]

    pl.semaphore_wait(barrier, len(peers))
    copies = [
        send(score, score_in.at[a - 1], sem_score, (a - 1,), gene_peer(a))
        for a in range(1, XL * CORE)
    ]
    for copy in copies:
        copy.wait()
    whole = total_of([score[...]] + [score_in[a] for a in range(XL * CORE - 1)])
    scores, own_mean = whole[0:comps], whole[comps : comps + 1]
    for ht in range(H):
        aux[ht, 16:17, :] = own_mean

    aux_copies = []
    for s, (a, b) in enumerate(xy_offsets):
        ht, yt = xy_place(a, b)
        aux_copies.append(
            send(aux.at[ht], aux_in.at[s], sem_aux, (s,), device(z, ht, yt, xl, core))
        )

    score_high = scores.astype(BF16)
    score_low = (scores - score_high.astype(F32)).astype(BF16)
    stacked = jnp.concatenate([score_high, score_low], axis=0)
    per_chunk = Z // CHUNKS
    part_copies = []
    for chunk in range(CHUNKS):
        span = pl.ds(chunk * per_chunk, per_chunk)
        for i in range(chunk * per_chunk, (chunk + 1) * per_chunk):
            zt = lax.rem(z + OFFSETS[i], Z)
            at = pl.multiple_of(zt * (H * LANES), H * LANES)
            both = jnp.dot(stacked, cbuf[:, pl.ds(at, H * LANES)], preferred_element_type=F32)
            product = both[:comps] + both[comps:]
            for ht in range(H):
                for yt in range(Y):
                    part[ht, yt, i] = product[
                        yt * rows : (yt + 1) * rows, ht * LANES : (ht + 1) * LANES
                    ]
        sent = []
        for s, (a, b) in enumerate(xy_offsets):
            ht, yt = xy_place(a, b)
            sent.append(
                send(
                    part.at[ht, yt, span],
                    part_in.at[s, span],
                    sem_part,
                    (s, chunk),
                    device(z, ht, yt, xl, core),
                )
            )
        part_copies.append(sent)

    def deviations(weight, means):
        middle = total_of(means) * (1.0 / len(means))
        turned[...] = jnp.zeros((LANES, LANES), F32)
        for p, value in enumerate(means):
            turned[p : p + 1, :] = (value - middle) * weight
        turned[...] = turned[...].T
        own = turned[pl.ds(pl.multiple_of(y * rows, rows), rows), :]
        return middle, [
            jnp.broadcast_to(own[:, p : p + 1], (rows, LANES)) for p in range(len(means))
        ]

    for copy in aux_copies:
        copy.wait()
    groups = len(xy_offsets) + 1
    score_xy, away = deviations(
        float(cells), [own_mean] + [aux_in[s, 16:17, :] for s in range(groups - 1)]
    )
    means = [aux[h, 0:16, :]] + [aux_in[s, 0:16, :] for s in range(groups - 1)]
    middle = total_of(means) * (1.0 / groups)
    mean_xy[...] = middle
    for p, value in enumerate(means):
        dev_mean[p] = value - middle

    z_copies = []
    for chunk in range(CHUNKS):
        for copy in part_copies[chunk]:
            copy.wait()
        for i in range(chunk * per_chunk, (chunk + 1) * per_chunk):
            zt = lax.rem(z + OFFSETS[i], Z)
            terms = [part[h, y, i]] + [part_in[s, i] for s in range(groups - 1)]
            terms += [away[p] * dev_mean[p, pl.ds(zt, 1), :] for p in range(groups)]
            zpart[i] = total_of(terms)
            zaux[i, 0:1, :] = mean_xy[pl.ds(zt, 1), :]
            zaux[i, 1:2, :] = score_xy
            if OFFSETS[i]:
                to = z_peer(OFFSETS[i])
                z_copies.append(send(zpart.at[i], zpart_in.at[i], sem_z, (i,), to))
                z_copies.append(send(zaux.at[i], zaux_in.at[i], sem_zaux, (i,), to))
    for copy in z_copies:
        copy.wait()
    _, away = deviations(
        float(cells * groups), [zaux[Z - 1, 1:2, :]] + [zaux_in[i, 1:2, :] for i in range(Z - 1)]
    )
    means = [zaux[Z - 1, 0:1, :]] + [zaux_in[i, 0:1, :] for i in range(Z - 1)]
    middle = total_of(means) * (1.0 / Z)
    terms = [zpart[Z - 1]] + [zpart_in[i] for i in range(Z - 1)]
    terms += [far * (value - middle) for far, value in zip(away, means)]
    tile[y] = total_of(terms)

    copies = [
        send(tile.at[y], tile.at[y], sem_tile, (b - 1,), device(z, h, lax.rem(y + b, Y), xl, core))
        for b in range(1, Y)
    ]
    for copy in copies:
        copy.wait()
    spread = tile[...].reshape(comps, LANES)
    own_gram = lax.dot_general(
        spread, spread, NT, precision=lax.Precision.HIGHEST, preferred_element_type=F32
    )
    half = comps // 2
    gram[:, 0:comps] = own_gram[0:half]
    gram[:, comps : 2 * comps] = own_gram[half:]
    along_x = H * XL * CORE
    copies = [send(gram, gram_in.at[a - 1], sem_gram, (a - 1,), x_peer(a)) for a in range(1, along_x)]
    spread = pltpu.roll(spread, lax.rem((Y - y) * (LANES // Y), LANES), 1)
    for copy in copies:
        copy.wait()
    quarter = half // CORE
    here = pl.ds(pl.multiple_of(core * quarter, quarter), quarter)
    gram_z[...] = total_of([gram[here, :]] + [gram_in[a, here, :] for a in range(along_x - 1)])
    copies = [
        send(gram_z, gram_z_in.at[o - 1], sem_gram_z, (o - 1,), z_peer(o)) for o in OFFSETS[: Z - 1]
    ]
    for copy in copies:
        copy.wait()
    gram_all[core] = total_of([gram_z[...]] + [gram_z_in[o] for o in range(Z - 1)])
    send(gram_all.at[core], gram_all.at[core], sem_core, (0,), device(z, h, y, xl, 1 - core)).wait()
    packed = gram_all[...].reshape(half, LANES)
    gram_sum = jnp.concatenate([packed[:, 0:comps], packed[:, comps : 2 * comps]], axis=0)
    result = solve(gram_sum, spread)
    out[...] = result[:, 0 : LANES // Y] * scaling


def on_device(counts, occupancy, start_basis):
    comps, genes = start_basis.shape
    cells = counts.shape[0]
    rows = comps // Y
    scaling = math.sqrt(genes * XL * CORE)
    dma = pltpu.SemaphoreType.DMA
    vmem = pl.BlockSpec(memory_space=pltpu.VMEM)
    return pl.pallas_call(
        functools.partial(kernel, scaling),
        out_shape=jax.ShapeDtypeStruct((comps, LANES // Y), F32),
        in_specs=[vmem, pl.BlockSpec(memory_space=pltpu.SMEM), vmem],
        out_specs=vmem,
        scratch_shapes=[
            pltpu.VMEM((cells, genes), BF16),
            pltpu.VMEM((16, genes), BF16),
            pltpu.VMEM((H, 24, LANES), F32),
            pltpu.VMEM((H * Y - 1, 24, LANES), F32),
            pltpu.VMEM((comps + 8, LANES), F32),
            pltpu.VMEM((XL * CORE - 1, comps + 8, LANES), F32),
            pltpu.VMEM((H, Y, Z, rows, LANES), F32),
            pltpu.VMEM((H * Y - 1, Z, rows, LANES), F32),
            pltpu.VMEM((H * Y, Z, LANES), F32),
            pltpu.VMEM((Z, LANES), F32),
            pltpu.VMEM((LANES, LANES), F32),
            pltpu.VMEM((Z, rows, LANES), F32),
            pltpu.VMEM((Z, 2, LANES), F32),
            pltpu.VMEM((Z - 1, rows, LANES), F32),
            pltpu.VMEM((Z - 1, 2, LANES), F32),
            pltpu.VMEM((Y, rows, LANES), F32),
            pltpu.VMEM((comps // 2, LANES), F32),
            pltpu.VMEM((H * XL * CORE - 1, comps // 2, LANES), F32),
            pltpu.VMEM((comps // 2 // CORE, LANES), F32),
            pltpu.VMEM((Z - 1, comps // 2 // CORE, LANES), F32),
            pltpu.VMEM((CORE, comps // 2 // CORE, LANES), F32),
            dma((2, XL * CORE - 1)),
            dma((2, H * Y - 1)),
            dma((2, H * Y - 1, CHUNKS)),
            dma((2, Z - 1)),
            dma((2, Z - 1)),
            dma((2, Y - 1)),
            dma((2, H * XL * CORE - 1)),
            dma((2, Z - 1)),
            dma((2, 1)),
        ],
        compiler_params=pltpu.CompilerParams(collective_id=0, has_side_effects=True),
        name="subspace_step",
    )(counts, occupancy, start_basis)


def solution(mesh):
    placed = (P("cells", "genes"), P("cells", "genes"), P(None, "genes"))
    return jax.shard_map(
        on_device, mesh=mesh, in_specs=placed, out_specs=P(None, ("genes", "cells")), check_vma=False
    )
```

```python
import math

import jax
import jax.numpy as jnp
from jax import lax
from jax.experimental import pallas as pl
from jax.experimental.pallas import tpu as pltpu
from jax.sharding import PartitionSpec as P

F32 = jnp.float32
BF16 = jnp.bfloat16
MESH = pl.DeviceIdType.MESH
Z, H, Y, XL, CORE = 16, 2, 4, 2, 2
LANES = 128
OFFSETS = (8, 7, 9, 6, 10, 5, 11, 4, 12, 3, 13, 2, 14, 1, 15, 0)
CHUNKS = 4
NEAR = 4
NT = (((1,), (1,)), ((), ()))


def device(z, h, y, xl, core):
    return ((z * H + h) * Y + y, xl * CORE + core)


def total_of(values):
    values = list(values)
    while len(values) > 1:
        values = [sum(values[i : i + 2][1:], values[i]) for i in range(0, len(values), 2)]
    return values[0]


def solve(gram, right):
    blocks = gram.shape[0] // 8
    left = [gram[8 * b : 8 * b + 8] for b in range(blocks)]
    right = [right[8 * b : 8 * b + 8] for b in range(blocks)]
    row_at = lax.broadcasted_iota(jnp.int32, (8, LANES), 0)
    done = []
    for kb in range(blocks):
        cols = [
            [
                jnp.broadcast_to(left[b][:, 8 * kb + j : 8 * kb + j + 1], (8, LANES))
                for j in range(8)
            ]
            for b in range(kb, blocks)
        ]
        rows_left, rows_right = left[kb], right[kb]
        scale = jnp.zeros((8, LANES), F32)
        steps = []
        for j in range(8):
            pivot = jnp.broadcast_to(cols[0][j][j : j + 1], (8, LANES))
            inv = lax.rsqrt(pivot)
            scale = jnp.where(row_at == j, inv, scale)
            lower = [c[j] * inv for c in cols]
            for m in range(j + 1, 8):
                entry = jnp.broadcast_to(lower[0][m : m + 1], (8, LANES))
                for c, low in zip(cols, lower):
                    c[m] = c[m] - low * entry
            below = jnp.where(row_at > j, lower[0], 0.0)
            unit_left = jnp.broadcast_to(rows_left[j : j + 1], rows_left.shape) * inv[:, : rows_left.shape[1]]
            unit_right = jnp.broadcast_to(rows_right[j : j + 1], rows_right.shape) * inv
            rows_left = rows_left - below[:, : rows_left.shape[1]] * unit_left
            rows_right = rows_right - below * unit_right
            steps.append((lower[1:], unit_left, unit_right))
        done.append(rows_right * scale)
        for at, b in enumerate(range(kb + 1, blocks)):
            for lower, unit_left, unit_right in steps:
                left[b] = left[b] - lower[at][:, : unit_left.shape[1]] * unit_left
                right[b] = right[b] - lower[at] * unit_right
    return jnp.concatenate(done, axis=0)


def kernel(
    counts_hbm,
    occupancy_hbm,
    basis_hbm,
    out,
    counts,
    occupancy,
    basis,
    cbuf,
    split_mean,
    aux,
    aux_in,
    score,
    score_in,
    part,
    part_in,
    dev_mean,
    mean_xy,
    turned,
    zpart,
    zaux,
    zpart_in,
    zaux_in,
    gram,
    gram_in,
    gram_z,
    gram_z_in,
    gram_all,
    sem_in,
    sem_score,
    sem_aux,
    sem_part,
    sem_z,
    sem_zaux,
    sem_gram,
    sem_gram_z,
    sem_all,
    sem_far,
):
    cells_at, genes_at = lax.axis_index("cells"), lax.axis_index("genes")
    z, h, y = cells_at // (H * Y), lax.rem(cells_at // Y, H), lax.rem(cells_at, Y)
    xl, core = genes_at // CORE, lax.rem(genes_at, CORE)
    comps = basis.shape[0]
    rows = comps // Y
    cells = counts.shape[0]
    width = LANES // Y
    plane = H * XL * CORE * Y

    loads = [pltpu.make_async_copy(occupancy_hbm, occupancy, sem_in.at[0])]
    wide = counts.shape[1] // CHUNKS
    for c in range(CHUNKS):
        span = pl.ds(c * wide, wide)
        loads.append(pltpu.make_async_copy(counts_hbm.at[:, span], counts.at[:, span], sem_in.at[c + 1]))
    loads.append(pltpu.make_async_copy(basis_hbm, basis, sem_in.at[CHUNKS + 1]))
    for load in loads:
        load.start()

    def send(src, dst, sems, index, to):
        copy = pltpu.make_async_remote_copy(
            src_ref=src,
            dst_ref=dst,
            send_sem=sems.at[(0, *index)],
            recv_sem=sems.at[(1, *index)],
            device_id=to,
            device_id_type=MESH,
        )
        copy.start()
        return copy

    def gene_peer(a):
        other = lax.rem(genes_at + a, XL * CORE)
        return device(z, h, y, other // CORE, lax.rem(other, CORE))

    def xy_place(a, b):
        return lax.rem(h + a, H), lax.rem(y + b, Y)

    def z_peer(o):
        return device(lax.rem(z + o, Z), h, y, xl, core)

    place = ((h * XL + xl) * CORE + core) * Y + y

    def plane_place(a):
        return lax.rem(place + a, plane)

    def plane_peer(a):
        other = plane_place(a)
        in_x = other // Y
        return device(
            z, in_x // (XL * CORE), lax.rem(other, Y), lax.rem(in_x // CORE, XL), lax.rem(in_x, CORE)
        )

    xy_offsets = [(a, b) for a in range(H) for b in range(Y) if a or b]

    barrier = pltpu.get_barrier_semaphore()
    near = [o for o in range(1, Z) if min(o, Z - o) <= NEAR]
    peers = [gene_peer(a) for a in range(1, XL * CORE)]
    peers += [device(z, *xy_place(a, b), xl, core) for a, b in xy_offsets]
    peers += [z_peer(o) for o in near]
    for peer in peers:
        pl.semaphore_signal(barrier, inc=1, device_id=peer, device_id_type=MESH)

    row_at = lax.broadcasted_iota(jnp.int32, (16, LANES), 0)
    group_at = lax.broadcasted_iota(jnp.int32, (16, LANES), 1) // width
    aux[:, 16:24, :] = jnp.zeros((H, 8, LANES), F32)
    turned[...] = jnp.zeros((LANES, LANES), F32)

    def center(zt, carry):
        for ht in range(H):
            at = pl.multiple_of((zt * H + ht) * LANES, LANES)
            entries = counts[:, pl.ds(at, LANES)].astype(F32)
            stored = occupancy[0, zt * H + ht].astype(F32)
            logged = jnp.log(1.0 + entries) * stored
            mean = jnp.sum(logged, axis=0, keepdims=True) * (1.0 / cells)
            cbuf[:, pl.ds(at, LANES)] = (logged - mean).astype(BF16)
            aux[ht, pl.ds(zt, 1), :] = mean
            high = mean.astype(BF16).astype(F32)
            middle = (mean - high).astype(BF16).astype(F32)
            low = mean - high - middle
            stacked = jnp.where(
                row_at == 0, high, jnp.where(row_at == 1, middle, jnp.where(row_at == 2, low, 0.0))
            )
            split_mean[:, pl.ds(at, LANES)] = stacked.astype(BF16)
        return carry

    per_chunk = Z // CHUNKS
    loads[0].wait()
    for c in range(CHUNKS):
        loads[c + 1].wait()
        lax.fori_loop(c * per_chunk, (c + 1) * per_chunk, center, 0)
    loads[-1].wait()

    score[0:comps, :] = lax.dot_general(basis[...], cbuf[...], NT, preferred_element_type=F32)
    of_mean = lax.dot_general(split_mean[...], basis[...], NT, preferred_element_type=F32)
    score[comps : comps + 8, :] = jnp.zeros((8, LANES), F32)
    score[comps : comps + 1, 0:comps] = of_mean[0:1] + of_mean[1:2] + of_mean[2:3]

    pl.semaphore_wait(barrier, len(peers))
    for o in (NEAR, Z - NEAR):
        pl.semaphore_signal(sem_far, inc=1, device_id=z_peer(o), device_id_type=MESH)
    copies = [
        send(score, score_in.at[a - 1], sem_score, (a - 1,), gene_peer(a))
        for a in range(1, XL * CORE)
    ]
    for copy in copies:
        copy.wait()
    whole = total_of([score[...]] + [score_in[a] for a in range(XL * CORE - 1)])
    scores, own_mean = whole[0:comps], whole[comps : comps + 1]
    for ht in range(H):
        aux[ht, 16:17, :] = own_mean

    aux_copies = []
    for s, (a, b) in enumerate(xy_offsets):
        ht, yt = xy_place(a, b)
        aux_copies.append(
            send(aux.at[ht], aux_in.at[s], sem_aux, (s,), device(z, ht, yt, xl, core))
        )

    score_high = scores.astype(BF16)
    score_low = (scores - score_high.astype(F32)).astype(BF16)
    stacked = jnp.concatenate([score_high, score_low], axis=0)
    part_copies = []
    for chunk in range(CHUNKS):
        span = pl.ds(chunk * per_chunk, per_chunk)
        for i in range(chunk * per_chunk, (chunk + 1) * per_chunk):
            zt = lax.rem(z + OFFSETS[i], Z)
            at = pl.multiple_of(zt * (H * LANES), H * LANES)
            both = jnp.dot(stacked, cbuf[:, pl.ds(at, H * LANES)], preferred_element_type=F32)
            product = both[:comps] + both[comps:]
            for ht in range(H):
                turns = []
                for b in range(Y):
                    block = product[b * rows : (b + 1) * rows, ht * LANES : (ht + 1) * LANES]
                    turns.append([block] + [pltpu.roll(block, k * width, 1) for k in range(1, Y)])
                for yt in range(Y):
                    piece = turns[0][(0 - yt) % Y]
                    for b in range(1, Y):
                        piece = jnp.where(group_at == b, turns[b][(b - yt) % Y], piece)
                    part[ht, yt, i] = piece
        sent = []
        for s, (a, b) in enumerate(xy_offsets):
            ht, yt = xy_place(a, b)
            sent.append(
                send(
                    part.at[ht, yt, span],
                    part_in.at[s, span],
                    sem_part,
                    (s, chunk),
                    device(z, ht, yt, xl, core),
                )
            )
        part_copies.append(sent)

    def deviations(weight, means):
        middle = total_of(means) * (1.0 / len(means))
        for p, value in enumerate(means):
            turned[p : p + 1, :] = (value - middle) * weight
        flat = turned[...].T
        away = []
        for p in range(len(means)):
            folded = jnp.broadcast_to(flat[0:rows, p : p + 1], (rows, LANES))
            for b in range(1, Y):
                block = jnp.broadcast_to(flat[b * rows : (b + 1) * rows, p : p + 1], (rows, LANES))
                folded = jnp.where(group_at == b, block, folded)
            away.append(folded)
        return middle, away

    def own_columns(means):
        kept = jnp.where(group_at == y, means, 0.0)
        return total_of([kept] + [pltpu.roll(kept, k * width, 1) for k in range(1, Y)])

    for copy in aux_copies:
        copy.wait()
    groups = len(xy_offsets) + 1
    score_xy, away = deviations(
        float(cells), [own_mean] + [aux_in[s, 16:17, :] for s in range(groups - 1)]
    )
    means = [aux[h, 0:16, :]] + [aux_in[s, 0:16, :] for s in range(groups - 1)]
    middle = total_of(means) * (1.0 / groups)
    mean_xy[...] = own_columns(middle)
    for p, value in enumerate(means):
        dev_mean[p] = own_columns(value - middle)

    pl.semaphore_wait(sem_far, 2)
    z_copies = []
    for chunk in range(CHUNKS):
        for copy in part_copies[chunk]:
            copy.wait()
        for i in range(chunk * per_chunk, (chunk + 1) * per_chunk):
            zt = lax.rem(z + OFFSETS[i], Z)
            terms = [part[h, y, i]] + [part_in[s, i] for s in range(groups - 1)]
            terms += [away[p] * dev_mean[p, pl.ds(zt, 1), :] for p in range(groups)]
            zpart[i] = total_of(terms)
            zaux[i, 0:1, :] = mean_xy[pl.ds(zt, 1), :]
            zaux[i, 1:2, :] = score_xy
            if OFFSETS[i]:
                to = z_peer(OFFSETS[i])
                z_copies.append(send(zpart.at[i], zpart_in.at[i], sem_z, (i,), to))
                z_copies.append(send(zaux.at[i], zaux_in.at[i], sem_zaux, (i,), to))
    for copy in z_copies:
        copy.wait()
    _, away = deviations(
        float(cells * groups), [zaux[Z - 1, 1:2, :]] + [zaux_in[i, 1:2, :] for i in range(Z - 1)]
    )
    means = [zaux[Z - 1, 0:1, :]] + [zaux_in[i, 0:1, :] for i in range(Z - 1)]
    middle = total_of(means) * (1.0 / Z)
    terms = [zpart[Z - 1]] + [zpart_in[i] for i in range(Z - 1)]
    terms += [far * (value - middle) for far, value in zip(away, means)]
    folded = total_of(terms)

    blocks = [folded] + [pltpu.roll(folded, (Y - b) * width, 1) for b in range(1, Y)]
    spread = jnp.concatenate([jnp.where(group_at == 0, block, 0.0) for block in blocks], axis=0)
    own_gram = lax.dot_general(
        spread, spread, NT, precision=lax.Precision.HIGHEST, preferred_element_type=F32
    )
    packed = jnp.concatenate([own_gram[0:plane], own_gram[plane:]], axis=1)
    for e in range(plane):
        gram[e] = packed[e : e + 1]
    for a in range(1, plane):
        send(gram.at[plane_place(a)], gram_in.at[a - 1], sem_gram, (), plane_peer(a))
    all_of(gram.at[pl.ds(0, plane - 1)], gram_in, sem_gram)
    gram_z[...] = jnp.sum(gram_in[...], axis=0) + gram[place]
    for a, o in enumerate(OFFSETS[: Z - 1]):
        send(gram_z, gram_z_in.at[a], sem_gram_z, (), z_peer(o))
    all_of(gram_z_in, gram_z_in, sem_gram_z)
    gram_all[place] = jnp.sum(gram_z_in[...], axis=0) + gram_z[...]
    for a in range(1, plane):
        send(gram_all.at[place], gram_all.at[place], sem_all, (), plane_peer(a))
    all_of(gram_all.at[pl.ds(0, plane - 1)], gram_all.at[pl.ds(0, plane - 1)], sem_all)
    packed = gram_all[...].reshape(plane, LANES)
    gram_sum = jnp.concatenate([packed[:, 0:comps], packed[:, comps : 2 * comps]], axis=0)
    out[...] = solve(gram_sum, spread).T[0:width]


def all_of(sent, received, sems):
    pltpu.make_async_remote_copy(
        src_ref=sent,
        dst_ref=received,
        send_sem=sems.at[0],
        recv_sem=sems.at[1],
        device_id=(0, 0),
        device_id_type=MESH,
    ).wait()


def on_device(counts, occupancy, start_basis):
    comps, genes = start_basis.shape
    cells = counts.shape[0]
    rows = comps // Y
    plane = H * XL * CORE * Y
    dma = pltpu.SemaphoreType.DMA
    hbm = pl.BlockSpec(memory_space=pltpu.HBM)
    basis_now = pl.pallas_call(
        kernel,
        out_shape=jax.ShapeDtypeStruct((LANES // Y, comps), F32),
        in_specs=[hbm, hbm, hbm],
        out_specs=pl.BlockSpec(memory_space=pltpu.VMEM),
        scratch_shapes=[
            pltpu.VMEM((cells, genes), BF16),
            pltpu.SMEM(occupancy.shape, jnp.int32),
            pltpu.VMEM((comps, genes), BF16),
            pltpu.VMEM((cells, genes), BF16),
            pltpu.VMEM((16, genes), BF16),
            pltpu.VMEM((H, 24, LANES), F32),
            pltpu.VMEM((H * Y - 1, 24, LANES), F32),
            pltpu.VMEM((comps + 8, LANES), F32),
            pltpu.VMEM((XL * CORE - 1, comps + 8, LANES), F32),
            pltpu.VMEM((H, Y, Z, rows, LANES), F32),
            pltpu.VMEM((H * Y - 1, Z, rows, LANES), F32),
            pltpu.VMEM((H * Y, Z, LANES), F32),
            pltpu.VMEM((Z, LANES), F32),
            pltpu.VMEM((LANES, LANES), F32),
            pltpu.VMEM((Z, rows, LANES), F32),
            pltpu.VMEM((Z, 2, LANES), F32),
            pltpu.VMEM((Z - 1, rows, LANES), F32),
            pltpu.VMEM((Z - 1, 2, LANES), F32),
            pltpu.VMEM((plane, 1, LANES), F32),
            pltpu.VMEM((plane - 1, 1, LANES), F32),
            pltpu.VMEM((1, LANES), F32),
            pltpu.VMEM((Z - 1, 1, LANES), F32),
            pltpu.VMEM((plane, 1, LANES), F32),
            dma((CHUNKS + 2,)),
            dma((2, XL * CORE - 1)),
            dma((2, H * Y - 1)),
            dma((2, H * Y - 1, CHUNKS)),
            dma((2, Z - 1)),
            dma((2, Z - 1)),
            dma((2,)),
            dma((2,)),
            dma((2,)),
            pltpu.SemaphoreType.REGULAR,
        ],
        compiler_params=pltpu.CompilerParams(
            collective_id=0, has_side_effects=True, vmem_limit_bytes=24 << 20
        ),
        name="subspace_step",
    )(*(pltpu.with_memory_space_constraint(a, pltpu.HBM) for a in (counts, occupancy, start_basis)))
    return basis_now.T * math.sqrt(genes * XL * CORE)


def solution(mesh):
    placed = (P("cells", "genes"), P("cells", "genes"), P(None, "genes"))
    return jax.shard_map(
        on_device, mesh=mesh, in_specs=placed, out_specs=P(None, ("genes", "cells")), check_vma=False
    )
```

```python
import math

import jax
import jax.numpy as jnp
from jax import lax
from jax.experimental import pallas as pl
from jax.experimental.pallas import tpu as pltpu
from jax.sharding import PartitionSpec as P

F32 = jnp.float32
BF16 = jnp.bfloat16
MESH = pl.DeviceIdType.MESH
Z, H, Y, XL, CORE = 16, 2, 4, 2, 2
LANES = 128
DIRECT = (8, 6, 10)
PAIRED = (4, 12, 2, 14, 0)
PAIRED_CHUNKS = ((0, 2), (2, 5))
CHUNKS = 4
NEAR = 4
NT = (((1,), (1,)), ((), ()))


def device(z, h, y, xl, core):
    return ((z * H + h) * Y + y, xl * CORE + core)


def total_of(values):
    values = list(values)
    while len(values) > 1:
        values = [sum(values[i : i + 2][1:], values[i]) for i in range(0, len(values), 2)]
    return values[0]


def solve(gram, right):
    blocks = gram.shape[0] // 8
    left = [gram[8 * b : 8 * b + 8] for b in range(blocks)]
    right = [right[8 * b : 8 * b + 8] for b in range(blocks)]
    row_at = lax.broadcasted_iota(jnp.int32, (8, LANES), 0)
    done = []
    for kb in range(blocks):
        cols = [
            [
                jnp.broadcast_to(left[b][:, 8 * kb + j : 8 * kb + j + 1], (8, LANES))
                for j in range(8)
            ]
            for b in range(kb, blocks)
        ]
        rows_left, rows_right = left[kb], right[kb]
        scale = jnp.zeros((8, LANES), F32)
        steps = []
        for j in range(8):
            pivot = jnp.broadcast_to(cols[0][j][j : j + 1], (8, LANES))
            inv = lax.rsqrt(pivot)
            scale = jnp.where(row_at == j, inv, scale)
            lower = [c[j] * inv for c in cols]
            for m in range(j + 1, 8):
                entry = jnp.broadcast_to(lower[0][m : m + 1], (8, LANES))
                for c, low in zip(cols, lower):
                    c[m] = c[m] - low * entry
            below = jnp.where(row_at > j, lower[0], 0.0)
            unit_left = jnp.broadcast_to(rows_left[j : j + 1], rows_left.shape) * inv[:, : rows_left.shape[1]]
            unit_right = jnp.broadcast_to(rows_right[j : j + 1], rows_right.shape) * inv
            rows_left = rows_left - below[:, : rows_left.shape[1]] * unit_left
            rows_right = rows_right - below * unit_right
            steps.append((lower[1:], unit_left, unit_right))
        done.append(rows_right * scale)
        for at, b in enumerate(range(kb + 1, blocks)):
            for lower, unit_left, unit_right in steps:
                left[b] = left[b] - lower[at][:, : unit_left.shape[1]] * unit_left
                right[b] = right[b] - lower[at] * unit_right
    return jnp.concatenate(done, axis=0)


def kernel(
    counts_hbm,
    occupancy_hbm,
    basis_hbm,
    out,
    counts,
    occupancy,
    basis,
    cbuf,
    split_mean,
    aux,
    aux_in,
    score,
    score_in,
    aux_pair,
    aux_pair_in,
    aux_paired_in,
    direct,
    direct_in,
    paired,
    paired_in,
    pair_out,
    pair_in,
    pair_dev,
    dev_mean,
    mean_xy,
    turned,
    zpart,
    zaux,
    zpart_in,
    zaux_in,
    gram,
    gram_in,
    gram_z,
    gram_z_in,
    gram_all,
    sem_in,
    sem_score,
    sem_aux,
    sem_aux_pair,
    sem_aux_paired,
    sem_direct,
    sem_pair,
    sem_paired,
    sem_z,
    sem_zaux,
    sem_gram,
    sem_gram_z,
    sem_all,
    sem_far,
):
    cells_at, genes_at = lax.axis_index("cells"), lax.axis_index("genes")
    z, h, y = cells_at // (H * Y), lax.rem(cells_at // Y, H), lax.rem(cells_at, Y)
    xl, core = genes_at // CORE, lax.rem(genes_at, CORE)
    comps = basis.shape[0]
    rows = comps // Y
    cells = counts.shape[0]
    width = LANES // Y
    plane = H * XL * CORE * Y

    loads = [pltpu.make_async_copy(occupancy_hbm, occupancy, sem_in.at[0])]
    wide = counts.shape[1] // CHUNKS
    for c in range(CHUNKS):
        span = pl.ds(c * wide, wide)
        loads.append(pltpu.make_async_copy(counts_hbm.at[:, span], counts.at[:, span], sem_in.at[c + 1]))
    loads.append(pltpu.make_async_copy(basis_hbm, basis, sem_in.at[CHUNKS + 1]))
    for load in loads:
        load.start()

    def send(src, dst, sems, index, to):
        copy = pltpu.make_async_remote_copy(
            src_ref=src,
            dst_ref=dst,
            send_sem=sems.at[(0, *index)],
            recv_sem=sems.at[(1, *index)],
            device_id=to,
            device_id_type=MESH,
        )
        copy.start()
        return copy

    def gene_peer(a):
        other = lax.rem(genes_at + a, XL * CORE)
        return device(z, h, y, other // CORE, lax.rem(other, CORE))

    def xy_place(a, b):
        return lax.rem(h + a, H), lax.rem(y + b, Y)

    def z_peer(o):
        return device(lax.rem(z + o + Z, Z), h, y, xl, core)

    place = ((h * XL + xl) * CORE + core) * Y + y

    def plane_place(a):
        return lax.rem(place + a, plane)

    def plane_peer(a):
        other = plane_place(a)
        in_x = other // Y
        return device(
            z, in_x // (XL * CORE), lax.rem(other, Y), lax.rem(in_x // CORE, XL), lax.rem(in_x, CORE)
        )

    def z_tile(o):
        return lax.rem(z + o + Z, Z)

    beside = [1 - 2 * lax.rem(z + ht, 2) for ht in range(H)]
    own_beside = 1 - 2 * lax.rem(z + h, 2)

    xy_offsets = [(a, b) for a in range(H) for b in range(Y) if a or b]

    barrier = pltpu.get_barrier_semaphore()
    near = [o for o in range(1, Z) if min(o, Z - o) <= NEAR]
    peers = [gene_peer(a) for a in range(1, XL * CORE)]
    peers += [device(z, *xy_place(a, b), xl, core) for a, b in xy_offsets]
    peers += [z_peer(o) for o in near]
    for peer in peers:
        pl.semaphore_signal(barrier, inc=1, device_id=peer, device_id_type=MESH)

    row_at = lax.broadcasted_iota(jnp.int32, (16, LANES), 0)
    group_at = lax.broadcasted_iota(jnp.int32, (16, LANES), 1) // width
    aux[:, 16:24, :] = jnp.zeros((H, 8, LANES), F32)
    aux_pair[:, 16:24, :] = jnp.zeros((H, 8, LANES), F32)
    turned[...] = jnp.zeros((LANES, LANES), F32)

    def center(zt, carry):
        for ht in range(H):
            at = pl.multiple_of((zt * H + ht) * LANES, LANES)
            entries = counts[:, pl.ds(at, LANES)].astype(F32)
            stored = occupancy[0, zt * H + ht].astype(F32)
            logged = jnp.log(1.0 + entries) * stored
            mean = jnp.sum(logged, axis=0, keepdims=True) * (1.0 / cells)
            cbuf[:, pl.ds(at, LANES)] = (logged - mean).astype(BF16)
            aux[ht, pl.ds(zt, 1), :] = mean
            high = mean.astype(BF16).astype(F32)
            middle = (mean - high).astype(BF16).astype(F32)
            low = mean - high - middle
            stacked = jnp.where(
                row_at == 0, high, jnp.where(row_at == 1, middle, jnp.where(row_at == 2, low, 0.0))
            )
            split_mean[:, pl.ds(at, LANES)] = stacked.astype(BF16)
        return carry

    per_chunk = Z // CHUNKS
    loads[0].wait()
    for c in range(CHUNKS):
        loads[c + 1].wait()
        lax.fori_loop(c * per_chunk, (c + 1) * per_chunk, center, 0)
    loads[-1].wait()

    score[0:comps, :] = lax.dot_general(basis[...], cbuf[...], NT, preferred_element_type=F32)
    of_mean = lax.dot_general(split_mean[...], basis[...], NT, preferred_element_type=F32)
    score[comps : comps + 8, :] = jnp.zeros((8, LANES), F32)
    score[comps : comps + 1, 0:comps] = of_mean[0:1] + of_mean[1:2] + of_mean[2:3]

    pl.semaphore_wait(barrier, len(peers))
    for o in (NEAR, Z - NEAR):
        pl.semaphore_signal(sem_far, inc=1, device_id=z_peer(o), device_id_type=MESH)
    copies = [
        send(score, score_in.at[a - 1], sem_score, (a - 1,), gene_peer(a))
        for a in range(1, XL * CORE)
    ]
    for copy in copies:
        copy.wait()
    whole = total_of([score[...]] + [score_in[a] for a in range(XL * CORE - 1)])
    scores, own_mean = whole[0:comps], whole[comps : comps + 1]
    for ht in range(H):
        aux[ht, 16:17, :] = own_mean

    aux_copies = []
    for s, (a, b) in enumerate(xy_offsets):
        ht, yt = xy_place(a, b)
        aux_copies.append(
            send(aux.at[ht], aux_in.at[s], sem_aux, (s,), device(z, ht, yt, xl, core))
        )

    pair_aux_copies = [
        send(aux.at[ht], aux_pair_in.at[ht], sem_aux_pair, (ht,), z_peer(beside[ht])) for ht in range(H)
    ]

    score_high = scores.astype(BF16)
    score_low = (scores - score_high.astype(F32)).astype(BF16)
    stacked = jnp.concatenate([score_high, score_low], axis=0)

    def pieces(tiles):
        columns = [
            cbuf[:, pl.ds(pl.multiple_of((tiles[ht] * H + ht) * LANES, LANES), LANES)] for ht in range(H)
        ]
        both = jnp.dot(stacked, jnp.concatenate(columns, axis=1), preferred_element_type=F32)
        product = both[:comps] + both[comps:]
        result = []
        for ht in range(H):
            turns = []
            for b in range(Y):
                block = product[b * rows : (b + 1) * rows, ht * LANES : (ht + 1) * LANES]
                turns.append([block] + [pltpu.roll(block, k * width, 1) for k in range(1, Y)])
            for yt in range(Y):
                piece = turns[0][(0 - yt) % Y]
                for b in range(1, Y):
                    piece = jnp.where(group_at == b, turns[b][(b - yt) % Y], piece)
                result.append((ht, yt, piece))
        return result

    def exchange(src, dst, sems, chunk, span):
        sent = []
        for s, (a, b) in enumerate(xy_offsets):
            ht, yt = xy_place(a, b)
            sent.append(
                send(
                    src.at[ht, yt, span],
                    dst.at[s, span],
                    sems,
                    (s, chunk),
                    device(z, ht, yt, xl, core),
                )
            )
        return sent

    def start_direct(j):
        tiles = [z_tile(DIRECT[j])] * H
        for ht, yt, piece in pieces(tiles):
            direct[ht, yt, 2 * j] = piece
        for ht, yt, piece in pieces([z_tile(DIRECT[j] + beside[ht]) for ht in range(H)]):
            direct[ht, yt, 2 * j + 1] = piece
        return exchange(direct, direct_in, sem_direct, j, pl.ds(2 * j, 2))

    def start_pair(chunk):
        first, last = PAIRED_CHUNKS[chunk]
        for j in range(first, last):
            for ht, yt, piece in pieces([z_tile(PAIRED[j] + beside[ht]) for ht in range(H)]):
                pair_out[ht, j, yt] = piece
        span = pl.ds(first, last - first)
        return [
            send(
                pair_out.at[ht, span], pair_in.at[ht, span], sem_pair, (ht, chunk), z_peer(beside[ht])
            )
            for ht in range(H)
        ]

    direct_copies = [start_direct(0)]
    pair_copies = [start_pair(chunk) for chunk in range(len(PAIRED_CHUNKS))]
    direct_copies += [start_direct(j) for j in range(1, len(DIRECT))]
    for j, e in enumerate(PAIRED):
        for ht, yt, piece in pieces([z_tile(e)] * H):
            paired[ht, yt, j] = piece

    def fold_rows(values):
        for p, value in enumerate(values):
            turned[p : p + 1, :] = value
        flat = turned[...].T
        result = []
        for p in range(len(values)):
            folded = jnp.broadcast_to(flat[0:rows, p : p + 1], (rows, LANES))
            for b in range(1, Y):
                block = jnp.broadcast_to(flat[b * rows : (b + 1) * rows, p : p + 1], (rows, LANES))
                folded = jnp.where(group_at == b, block, folded)
            result.append(folded)
        return result

    def columns_of(means, yt):
        kept = jnp.where(group_at == yt, means, 0.0)
        return total_of([kept] + [pltpu.roll(kept, k * width, 1) for k in range(1, Y)])

    groups = len(xy_offsets) + 1

    def plane_terms(level, weight, own, others):
        scores_of = [own[h, 16:17, :]] + [others[s, 16:17, :] for s in range(groups - 1)]
        middle = total_of(scores_of) * (1.0 / groups)
        away = fold_rows([(value - middle) * weight for value in scores_of])
        means = [own[h, 0:16, :]] + [others[s, 0:16, :] for s in range(groups - 1)]
        mean = total_of(means) * (1.0 / groups)
        mean_xy[level] = columns_of(mean, y)
        for p, value in enumerate(means):
            dev_mean[level, p] = columns_of(value - mean, y)
        return middle, away

    for copy in pair_aux_copies:
        copy.wait()
    pair_away = fold_rows(
        [(aux[ht, 16:17, :] - aux_pair_in[ht, 16:17, :]) * (0.5 * cells) for ht in range(H)]
    )
    for ht in range(H):
        aux_pair[ht, 0:17, :] = 0.5 * (aux[ht, 0:17, :] + aux_pair_in[ht, 0:17, :])
        apart = aux[ht, 0:16, :] - aux_pair_in[ht, 0:16, :]
        for yt in range(Y):
            pair_dev[ht, yt] = columns_of(apart, yt)
    aux_paired_copies = []
    for s, (a, b) in enumerate(xy_offsets):
        ht, yt = xy_place(a, b)
        aux_paired_copies.append(
            send(
                aux_pair.at[ht],
                aux_paired_in.at[s],
                sem_aux_paired,
                (s,),
                device(z, ht, yt, xl, core),
            )
        )
    for copy in aux_copies:
        copy.wait()
    score_direct, away_direct = plane_terms(0, float(cells), aux, aux_in)
    paired_copies = []
    for chunk, (first, last) in enumerate(PAIRED_CHUNKS):
        for copy in pair_copies[chunk]:
            copy.wait()
        for j in range(first, last):
            zt = z_tile(PAIRED[j])
            for ht in range(H):
                for yt in range(Y):
                    paired[ht, yt, j] = (paired[ht, yt, j] + pair_in[ht, j, yt]) + pair_away[
                        ht
                    ] * pair_dev[ht, yt, pl.ds(zt, 1), :]
        paired_copies.append(
            exchange(paired, paired_in, sem_paired, chunk, pl.ds(first, last - first))
        )

    pl.semaphore_wait(sem_far, 2)
    z_copies = []

    def plane_sum(level, slot, own, others, i, zt, away, middle, to):
        terms = [own[h, y, i]] + [others[s, i] for s in range(groups - 1)]
        terms += [away[p] * dev_mean[level, p, pl.ds(zt, 1), :] for p in range(groups)]
        zpart[slot] = total_of(terms)
        zaux[slot, 0:1, :] = mean_xy[level, pl.ds(zt, 1), :]
        zaux[slot, 1:2, :] = middle
        if to is not None:
            z_copies.append(send(zpart.at[slot], zpart_in.at[slot], sem_z, (slot,), to))
            z_copies.append(send(zaux.at[slot], zaux_in.at[slot], sem_zaux, (slot,), to))

    for j, e in enumerate(DIRECT):
        for copy in direct_copies[j]:
            copy.wait()
        for i, o in ((2 * j, e), (2 * j + 1, e + own_beside)):
            plane_sum(0, i, direct, direct_in, i, z_tile(o), away_direct, score_direct, z_peer(o))
    for copy in aux_paired_copies:
        copy.wait()
    score_paired, away_paired = plane_terms(1, 2.0 * cells, aux_pair, aux_paired_in)
    alone = 2 * len(DIRECT)
    for chunk, (first, last) in enumerate(PAIRED_CHUNKS):
        for copy in paired_copies[chunk]:
            copy.wait()
        for j in range(first, last):
            e = PAIRED[j]
            to = z_peer(e) if e else None
            plane_sum(
                1, alone + j, paired, paired_in, j, z_tile(e), away_paired, score_paired, to
            )
    for copy in z_copies:
        copy.wait()
    last = alone + len(PAIRED) - 1
    shares = [1.0] * alone + [2.0] * len(PAIRED)
    means = [zaux_in[i, 0:1, :] for i in range(last)] + [zaux[last, 0:1, :]]
    scores_of = [zaux_in[i, 1:2, :] for i in range(last)] + [zaux[last, 1:2, :]]
    middle = total_of([v * w for v, w in zip(scores_of, shares)]) * (1.0 / Z)
    away = fold_rows([(v - middle) * (w * cells * groups) for v, w in zip(scores_of, shares)])
    middle = total_of([v * w for v, w in zip(means, shares)]) * (1.0 / Z)
    terms = [zpart[last]] + [zpart_in[i] for i in range(last)]
    terms += [far * (value - middle) for far, value in zip(away, means)]
    folded = total_of(terms)

    blocks = [folded] + [pltpu.roll(folded, (Y - b) * width, 1) for b in range(1, Y)]
    spread = jnp.concatenate([jnp.where(group_at == 0, block, 0.0) for block in blocks], axis=0)
    own_gram = lax.dot_general(
        spread, spread, NT, precision=lax.Precision.HIGHEST, preferred_element_type=F32
    )
    packed = jnp.concatenate([own_gram[0:plane], own_gram[plane:]], axis=1)
    for e in range(plane):
        gram[e] = packed[e : e + 1]
    for a in range(1, plane):
        send(gram.at[plane_place(a)], gram_in.at[a - 1], sem_gram, (), plane_peer(a))
    all_of(gram.at[pl.ds(0, plane - 1)], gram_in, sem_gram)
    gram_z[...] = jnp.sum(gram_in[...], axis=0) + gram[place]
    for a, o in enumerate(sorted(range(1, Z), key=lambda o: -min(o, Z - o))):
        send(gram_z, gram_z_in.at[a], sem_gram_z, (), z_peer(o))
    all_of(gram_z_in, gram_z_in, sem_gram_z)
    gram_all[place] = jnp.sum(gram_z_in[...], axis=0) + gram_z[...]
    for a in range(1, plane):
        send(gram_all.at[place], gram_all.at[place], sem_all, (), plane_peer(a))
    all_of(gram_all.at[pl.ds(0, plane - 1)], gram_all.at[pl.ds(0, plane - 1)], sem_all)
    packed = gram_all[...].reshape(plane, LANES)
    gram_sum = jnp.concatenate([packed[:, 0:comps], packed[:, comps : 2 * comps]], axis=0)
    out[...] = solve(gram_sum, spread).T[0:width]


def all_of(sent, received, sems):
    pltpu.make_async_remote_copy(
        src_ref=sent,
        dst_ref=received,
        send_sem=sems.at[0],
        recv_sem=sems.at[1],
        device_id=(0, 0),
        device_id_type=MESH,
    ).wait()


def on_device(counts, occupancy, start_basis):
    comps, genes = start_basis.shape
    cells = counts.shape[0]
    rows = comps // Y
    plane = H * XL * CORE * Y
    tiles = 2 * len(DIRECT) + len(PAIRED)
    dma = pltpu.SemaphoreType.DMA
    hbm = pl.BlockSpec(memory_space=pltpu.HBM)
    basis_now = pl.pallas_call(
        kernel,
        out_shape=jax.ShapeDtypeStruct((LANES // Y, comps), F32),
        in_specs=[hbm, hbm, hbm],
        out_specs=pl.BlockSpec(memory_space=pltpu.VMEM),
        scratch_shapes=[
            pltpu.VMEM((cells, genes), BF16),
            pltpu.SMEM(occupancy.shape, jnp.int32),
            pltpu.VMEM((comps, genes), BF16),
            pltpu.VMEM((cells, genes), BF16),
            pltpu.VMEM((16, genes), BF16),
            pltpu.VMEM((H, 24, LANES), F32),
            pltpu.VMEM((H * Y - 1, 24, LANES), F32),
            pltpu.VMEM((comps + 8, LANES), F32),
            pltpu.VMEM((XL * CORE - 1, comps + 8, LANES), F32),
            pltpu.VMEM((H, 24, LANES), F32),
            pltpu.VMEM((H, 24, LANES), F32),
            pltpu.VMEM((H * Y - 1, 24, LANES), F32),
            pltpu.VMEM((H, Y, 2 * len(DIRECT), rows, LANES), F32),
            pltpu.VMEM((H * Y - 1, 2 * len(DIRECT), rows, LANES), F32),
            pltpu.VMEM((H, Y, len(PAIRED), rows, LANES), F32),
            pltpu.VMEM((H * Y - 1, len(PAIRED), rows, LANES), F32),
            pltpu.VMEM((H, len(PAIRED), Y, rows, LANES), F32),
            pltpu.VMEM((H, len(PAIRED), Y, rows, LANES), F32),
            pltpu.VMEM((H, Y, Z, LANES), F32),
            pltpu.VMEM((2, H * Y, Z, LANES), F32),
            pltpu.VMEM((2, Z, LANES), F32),
            pltpu.VMEM((LANES, LANES), F32),
            pltpu.VMEM((tiles, rows, LANES), F32),
            pltpu.VMEM((tiles, 2, LANES), F32),
            pltpu.VMEM((tiles - 1, rows, LANES), F32),
            pltpu.VMEM((tiles - 1, 2, LANES), F32),
            pltpu.VMEM((plane, 1, LANES), F32),
            pltpu.VMEM((plane - 1, 1, LANES), F32),
            pltpu.VMEM((1, LANES), F32),
            pltpu.VMEM((Z - 1, 1, LANES), F32),
            pltpu.VMEM((plane, 1, LANES), F32),
            dma((CHUNKS + 2,)),
            dma((2, XL * CORE - 1)),
            dma((2, H * Y - 1)),
            dma((2, H)),
            dma((2, H * Y - 1)),
            dma((2, H * Y - 1, len(DIRECT))),
            dma((2, H, len(PAIRED_CHUNKS))),
            dma((2, H * Y - 1, len(PAIRED_CHUNKS))),
            dma((2, tiles - 1)),
            dma((2, tiles - 1)),
            dma((2,)),
            dma((2,)),
            dma((2,)),
            pltpu.SemaphoreType.REGULAR,
        ],
        compiler_params=pltpu.CompilerParams(
            collective_id=0, has_side_effects=True, vmem_limit_bytes=24 << 20
        ),
        name="subspace_step",
    )(*(pltpu.with_memory_space_constraint(a, pltpu.HBM) for a in (counts, occupancy, start_basis)))
    return basis_now.T * math.sqrt(genes * XL * CORE)


def solution(mesh):
    placed = (P("cells", "genes"), P("cells", "genes"), P(None, "genes"))
    return jax.shard_map(
        on_device, mesh=mesh, in_specs=placed, out_specs=P(None, ("genes", "cells")), check_vma=False
    )
```

```python
import math

import jax
import jax.numpy as jnp
from jax import lax
from jax.experimental import pallas as pl
from jax.experimental.pallas import tpu as pltpu
from jax.sharding import PartitionSpec as P

F32 = jnp.float32
BF16 = jnp.bfloat16
MESH = pl.DeviceIdType.MESH
Z, H, Y, XL, CORE = 16, 2, 4, 2, 2
LANES = 128
DIRECT = (8, 6, 10)
PAIRED = (4, 12, 2, 14, 0)
PAIRED_CHUNKS = ((0, 2), (2, 4), (4, 5))
CHUNKS = 4
NEAR = 4
NT = (((1,), (1,)), ((), ()))


def device(z, h, y, xl, core):
    return ((z * H + h) * Y + y, xl * CORE + core)


def far_first(offsets, weights, sizes):
    def far(offset):
        return -sum(w * min(o, n - o) for o, w, n in zip(offset, weights, sizes))

    return sorted((o for o in offsets if any(o)), key=far)


def total_of(values):
    values = list(values)
    while len(values) > 1:
        values = [sum(values[i : i + 2][1:], values[i]) for i in range(0, len(values), 2)]
    return values[0]


def solve(gram, right):
    blocks = gram.shape[0] // 8
    left = [gram[8 * b : 8 * b + 8] for b in range(blocks)]
    right = [right[8 * b : 8 * b + 8] for b in range(blocks)]
    row_at = lax.broadcasted_iota(jnp.int32, (8, LANES), 0)
    done = []
    for kb in range(blocks):
        cols = [
            [
                jnp.broadcast_to(left[b][:, 8 * kb + j : 8 * kb + j + 1], (8, LANES))
                for j in range(8)
            ]
            for b in range(kb, blocks)
        ]
        rows_left, rows_right = left[kb], right[kb]
        scale = jnp.zeros((8, LANES), F32)
        steps = []
        for j in range(8):
            pivot = jnp.broadcast_to(cols[0][j][j : j + 1], (8, LANES))
            inv = lax.rsqrt(pivot)
            scale = jnp.where(row_at == j, inv, scale)
            lower = [c[j] * inv for c in cols]
            for m in range(j + 1, 8):
                entry = jnp.broadcast_to(lower[0][m : m + 1], (8, LANES))
                for c, low in zip(cols, lower):
                    c[m] = c[m] - low * entry
            below = jnp.where(row_at > j, lower[0], 0.0)
            unit_left = jnp.broadcast_to(rows_left[j : j + 1], rows_left.shape) * inv[:, : rows_left.shape[1]]
            unit_right = jnp.broadcast_to(rows_right[j : j + 1], rows_right.shape) * inv
            rows_left = rows_left - below[:, : rows_left.shape[1]] * unit_left
            rows_right = rows_right - below * unit_right
            steps.append((lower[1:], unit_left, unit_right))
        done.append(rows_right * scale)
        for at, b in enumerate(range(kb + 1, blocks)):
            for lower, unit_left, unit_right in steps:
                left[b] = left[b] - lower[at][:, : unit_left.shape[1]] * unit_left
                right[b] = right[b] - lower[at] * unit_right
    return jnp.concatenate(done, axis=0)


def kernel(
    counts_hbm,
    occupancy_hbm,
    basis_hbm,
    out,
    counts,
    occupancy,
    basis,
    cbuf,
    split_mean,
    aux,
    aux_in,
    score,
    score_in,
    aux_pair,
    aux_pair_in,
    aux_paired_in,
    direct,
    direct_in,
    paired,
    paired_in,
    pair_out,
    pair_in,
    pair_dev,
    dev_mean,
    mean_xy,
    turned,
    zpart,
    zaux,
    zpart_in,
    zaux_in,
    gram,
    gram_in,
    gram_z,
    gram_z_in,
    gram_all,
    sem_in,
    sem_score,
    sem_aux,
    sem_aux_pair,
    sem_aux_paired,
    sem_direct,
    sem_pair,
    sem_paired,
    sem_z,
    sem_gram,
    sem_gram_z,
    sem_all,
    sem_far,
):
    cells_at, genes_at = lax.axis_index("cells"), lax.axis_index("genes")
    z, h, y = cells_at // (H * Y), lax.rem(cells_at // Y, H), lax.rem(cells_at, Y)
    xl, core = genes_at // CORE, lax.rem(genes_at, CORE)
    comps = basis.shape[0]
    rows = comps // Y
    cells = counts.shape[0]
    width = LANES // Y
    plane = H * XL * CORE * Y

    loads = [pltpu.make_async_copy(occupancy_hbm, occupancy, sem_in.at[0])]
    wide = counts.shape[1] // CHUNKS
    for c in range(CHUNKS):
        span = pl.ds(c * wide, wide)
        loads.append(pltpu.make_async_copy(counts_hbm.at[:, span], counts.at[:, span], sem_in.at[c + 1]))
    loads.append(pltpu.make_async_copy(basis_hbm, basis, sem_in.at[CHUNKS + 1]))
    for load in loads:
        load.start()

    def send(src, dst, sems, to, step=0):
        pltpu.make_async_remote_copy(
            src_ref=src,
            dst_ref=dst,
            send_sem=sems.at[0, step],
            recv_sem=sems.at[1, step],
            device_id=to,
            device_id_type=MESH,
        ).start()

    def wait(all_bytes, sems, step=0):
        pltpu.make_async_remote_copy(
            src_ref=all_bytes,
            dst_ref=all_bytes,
            send_sem=sems.at[0, step],
            recv_sem=sems.at[1, step],
            device_id=(cells_at, genes_at),
            device_id_type=MESH,
        ).wait()

    def gene_peer(a, b):
        return device(z, h, y, lax.rem(xl + a, XL), lax.rem(core + b, CORE))

    def xy_place(a, b):
        return lax.rem(h + a, H), lax.rem(y + b, Y)

    def z_peer(o):
        return device(lax.rem(z + o + Z, Z), h, y, xl, core)

    in_x = h * XL + xl
    place = (in_x * CORE + core) * Y + y

    def plane_peer(a, b, c):
        xt = lax.rem(in_x + a, H * XL)
        coret, yt = lax.rem(core + b, CORE), lax.rem(y + c, Y)
        return (xt * CORE + coret) * Y + yt, device(z, xt // XL, yt, lax.rem(xt, XL), coret)

    def z_tile(o):
        return lax.rem(z + o + Z, Z)

    beside = [1 - 2 * lax.rem(z + ht, 2) for ht in range(H)]
    own_beside = 1 - 2 * lax.rem(z + h, 2)

    gene_offsets = [(1, 0), (1, 1), (0, 1)]
    xy_offsets = far_first([(a, b) for a in range(H) for b in range(Y)], (4, 2), (H, Y))
    plane_offsets = far_first(
        [(a, b, c) for a in range(H * XL) for b in range(CORE) for c in range(Y)],
        (2, 1, 2),
        (H * XL, CORE, Y),
    )
    z_offsets = far_first([(o,) for o in range(Z)], (1,), (Z,))

    barrier = pltpu.get_barrier_semaphore()
    near = [o for o in range(1, Z) if min(o, Z - o) <= NEAR]
    peers = [gene_peer(a, b) for a, b in gene_offsets]
    peers += [device(z, *xy_place(a, b), xl, core) for a, b in xy_offsets]
    peers += [z_peer(o) for o in near]
    for peer in peers:
        pl.semaphore_signal(barrier, inc=1, device_id=peer, device_id_type=MESH)

    row_at = lax.broadcasted_iota(jnp.int32, (16, LANES), 0)
    group_at = lax.broadcasted_iota(jnp.int32, (16, LANES), 1) // width
    aux[:, 16:24, :] = jnp.zeros((H, 8, LANES), F32)
    aux_pair[:, 16:24, :] = jnp.zeros((H, 8, LANES), F32)
    turned[...] = jnp.zeros((LANES, LANES), F32)

    def center(j):
        at = pl.ds(j * LANES, LANES)
        entries = counts[:, at].astype(F32)
        logged = jnp.log(1.0 + entries) * occupancy[0, j].astype(F32)
        mean = jnp.sum(logged, axis=0, keepdims=True) * (1.0 / cells)
        cbuf[:, at] = (logged - mean).astype(BF16)
        aux[j % H, j // H : j // H + 1, :] = mean
        high = mean.astype(BF16).astype(F32)
        middle = (mean - high).astype(BF16).astype(F32)
        low = mean - high - middle
        stacked = jnp.where(
            row_at == 0, high, jnp.where(row_at == 1, middle, jnp.where(row_at == 2, low, 0.0))
        )
        split_mean[:, at] = stacked.astype(BF16)

    def product_of(c):
        span = pl.ds(c * wide, wide)
        return (
            lax.dot_general(basis[:, span], cbuf[:, span], NT, preferred_element_type=F32),
            lax.dot_general(split_mean[:, span], basis[:, span], NT, preferred_element_type=F32),
        )

    loads[0].wait()
    products = []
    for c in range(CHUNKS):
        loads[c + 1].wait()
        if c == 1:
            loads[-1].wait()
        if c:
            products.append(product_of(c - 1))
        for j in range(c * wide // LANES, (c + 1) * wide // LANES):
            center(j)
    products.append(product_of(CHUNKS - 1))
    score[0:comps, :] = total_of([p for p, _ in products])
    of_mean = total_of([p for _, p in products])
    score[comps : comps + 8, :] = jnp.zeros((8, LANES), F32)
    score[comps : comps + 1, 0:comps] = of_mean[0:1] + of_mean[1:2] + of_mean[2:3]

    pl.semaphore_wait(barrier, len(peers))
    for o in (NEAR, Z - NEAR):
        pl.semaphore_signal(sem_far, inc=1, device_id=z_peer(o), device_id_type=MESH)
    for s, (a, b) in enumerate(gene_offsets):
        send(score, score_in.at[s], sem_score, gene_peer(a, b))
    wait(score_in, sem_score)
    whole = total_of([score[...]] + [score_in[a] for a in range(XL * CORE - 1)])
    scores, own_mean = whole[0:comps], whole[comps : comps + 1]
    for ht in range(H):
        aux[ht, 16:17, :] = own_mean

    for s, (a, b) in enumerate(xy_offsets):
        ht, yt = xy_place(a, b)
        send(aux.at[ht], aux_in.at[s], sem_aux, device(z, ht, yt, xl, core))
    for ht in range(H):
        send(aux.at[ht], aux_pair_in.at[ht], sem_aux_pair, z_peer(beside[ht]))

    score_high = scores.astype(BF16)
    score_low = (scores - score_high.astype(F32)).astype(BF16)
    stacked = jnp.concatenate([score_high, score_low], axis=0)

    def pieces(tiles):
        columns = [
            cbuf[:, pl.ds(pl.multiple_of((tiles[ht] * H + ht) * LANES, LANES), LANES)] for ht in range(H)
        ]
        both = jnp.dot(stacked, jnp.concatenate(columns, axis=1), preferred_element_type=F32)
        product = both[:comps] + both[comps:]
        result = []
        for ht in range(H):
            turns = []
            for b in range(Y):
                block = product[b * rows : (b + 1) * rows, ht * LANES : (ht + 1) * LANES]
                turns.append([block] + [pltpu.roll(block, k * width, 1) for k in range(1, Y)])
            for yt in range(Y):
                piece = turns[0][(0 - yt) % Y]
                for b in range(1, Y):
                    piece = jnp.where(group_at == b, turns[b][(b - yt) % Y], piece)
                result.append((ht, yt, piece))
        return result

    def exchange(src, dst, sems, chunk, span):
        for s, (a, b) in enumerate(xy_offsets):
            ht, yt = xy_place(a, b)
            send(src.at[ht, yt, span], dst.at[span, s], sems, device(z, ht, yt, xl, core), chunk)

    def start_direct(j):
        tiles = [z_tile(DIRECT[j])] * H
        for ht, yt, piece in pieces(tiles):
            direct[ht, yt, 2 * j] = piece
        for ht, yt, piece in pieces([z_tile(DIRECT[j] + beside[ht]) for ht in range(H)]):
            direct[ht, yt, 2 * j + 1] = piece
        exchange(direct, direct_in, sem_direct, j, pl.ds(2 * j, 2))

    def start_pair(chunk):
        first, last = PAIRED_CHUNKS[chunk]
        for j in range(first, last):
            for ht, yt, piece in pieces([z_tile(PAIRED[j] + beside[ht]) for ht in range(H)]):
                pair_out[ht, j, yt] = piece
        span = pl.ds(first, last - first)
        for ht in range(H):
            send(pair_out.at[ht, span], pair_in.at[ht, span], sem_pair, z_peer(beside[ht]), chunk)

    start_direct(0)
    for chunk in range(len(PAIRED_CHUNKS)):
        start_pair(chunk)
    for j in range(1, len(DIRECT)):
        start_direct(j)
    for j, e in enumerate(PAIRED):
        for ht, yt, piece in pieces([z_tile(e)] * H):
            paired[ht, yt, j] = piece

    def fold_rows(values):
        for p, value in enumerate(values):
            turned[p : p + 1, :] = value
        flat = turned[...].T
        result = []
        for p in range(len(values)):
            folded = jnp.broadcast_to(flat[0:rows, p : p + 1], (rows, LANES))
            for b in range(1, Y):
                block = jnp.broadcast_to(flat[b * rows : (b + 1) * rows, p : p + 1], (rows, LANES))
                folded = jnp.where(group_at == b, block, folded)
            result.append(folded)
        return result

    def columns_of(means, yt):
        kept = jnp.where(group_at == yt, means, 0.0)
        return total_of([kept] + [pltpu.roll(kept, k * width, 1) for k in range(1, Y)])

    groups = len(xy_offsets) + 1

    def plane_terms(level, weight, own, others):
        scores_of = [own[h, 16:17, :]] + [others[s, 16:17, :] for s in range(groups - 1)]
        middle = total_of(scores_of) * (1.0 / groups)
        away = fold_rows([(value - middle) * weight for value in scores_of])
        means = [own[h, 0:16, :]] + [others[s, 0:16, :] for s in range(groups - 1)]
        mean = total_of(means) * (1.0 / groups)
        mean_xy[level] = columns_of(mean, y)
        for p, value in enumerate(means):
            dev_mean[level, p] = columns_of(value - mean, y)
        return middle, away

    wait(aux_pair_in, sem_aux_pair)
    pair_away = fold_rows(
        [(aux[ht, 16:17, :] - aux_pair_in[ht, 16:17, :]) * (0.5 * cells) for ht in range(H)]
    )
    for ht in range(H):
        aux_pair[ht, 0:17, :] = 0.5 * (aux[ht, 0:17, :] + aux_pair_in[ht, 0:17, :])
        apart = aux[ht, 0:16, :] - aux_pair_in[ht, 0:16, :]
        for yt in range(Y):
            pair_dev[ht, yt] = columns_of(apart, yt)
    for s, (a, b) in enumerate(xy_offsets):
        ht, yt = xy_place(a, b)
        send(aux_pair.at[ht], aux_paired_in.at[s], sem_aux_paired, device(z, ht, yt, xl, core))
    for chunk, (first, last) in enumerate(PAIRED_CHUNKS):
        wait(pair_in.at[:, pl.ds(first, last - first)], sem_pair, chunk)
        for j in range(first, last):
            zt = z_tile(PAIRED[j])
            for ht in range(H):
                for yt in range(Y):
                    paired[ht, yt, j] = (paired[ht, yt, j] + pair_in[ht, j, yt]) + pair_away[
                        ht
                    ] * pair_dev[ht, yt, pl.ds(zt, 1), :]
        exchange(paired, paired_in, sem_paired, chunk, pl.ds(first, last - first))

    wait(aux_in, sem_aux)
    score_direct, away_direct = plane_terms(0, float(cells), aux, aux_in)
    pl.semaphore_wait(sem_far, 2)

    def plane_sum(level, slot, own, others, i, zt, away, middle, to):
        terms = [own[h, y, i]] + [others[i, s] for s in range(groups - 1)]
        terms += [away[p] * dev_mean[level, p, pl.ds(zt, 1), :] for p in range(groups)]
        zpart[slot] = total_of(terms)
        zaux[slot, 0:1, :] = mean_xy[level, pl.ds(zt, 1), :]
        zaux[slot, 1:2, :] = middle
        if to is not None:
            send(zpart.at[slot], zpart_in.at[slot], sem_z, to)
            send(zaux.at[slot], zaux_in.at[slot], sem_z, to, 1)

    for j, e in enumerate(DIRECT):
        wait(direct_in.at[pl.ds(2 * j, 2)], sem_direct, j)
        for i, o in ((2 * j, e), (2 * j + 1, e + own_beside)):
            plane_sum(0, i, direct, direct_in, i, z_tile(o), away_direct, score_direct, z_peer(o))
    wait(aux_paired_in, sem_aux_paired)
    score_paired, away_paired = plane_terms(1, 2.0 * cells, aux_pair, aux_paired_in)
    alone = 2 * len(DIRECT)
    for chunk, (first, last) in enumerate(PAIRED_CHUNKS):
        wait(paired_in.at[pl.ds(first, last - first)], sem_paired, chunk)
        for j in range(first, last):
            e = PAIRED[j]
            to = z_peer(e) if e else None
            plane_sum(
                1, alone + j, paired, paired_in, j, z_tile(e), away_paired, score_paired, to
            )
    wait(zpart_in, sem_z)
    wait(zaux_in, sem_z, 1)
    last = alone + len(PAIRED) - 1
    shares = [1.0] * alone + [2.0] * len(PAIRED)
    means = [zaux_in[i, 0:1, :] for i in range(last)] + [zaux[last, 0:1, :]]
    scores_of = [zaux_in[i, 1:2, :] for i in range(last)] + [zaux[last, 1:2, :]]
    middle = total_of([v * w for v, w in zip(scores_of, shares)]) * (1.0 / Z)
    away = fold_rows([(v - middle) * (w * cells * groups) for v, w in zip(scores_of, shares)])
    middle = total_of([v * w for v, w in zip(means, shares)]) * (1.0 / Z)
    terms = [zpart[last]] + [zpart_in[i] for i in range(last)]
    terms += [far * (value - middle) for far, value in zip(away, means)]
    folded = total_of(terms)

    blocks = [folded] + [pltpu.roll(folded, (Y - b) * width, 1) for b in range(1, Y)]
    spread = jnp.concatenate([jnp.where(group_at == 0, block, 0.0) for block in blocks], axis=0)
    own_gram = lax.dot_general(
        spread, spread, NT, precision=lax.Precision.HIGHEST, preferred_element_type=F32
    )
    packed = jnp.concatenate([own_gram[0:plane], own_gram[plane:]], axis=1)
    for e in range(plane):
        gram[e] = packed[e : e + 1]
    for s, offset in enumerate(plane_offsets):
        at, to = plane_peer(*offset)
        send(gram.at[at], gram_in.at[s], sem_gram, to)
    wait(gram_in, sem_gram)
    gram_z[...] = jnp.sum(gram_in[...], axis=0) + gram[place]
    for s, (o,) in enumerate(z_offsets):
        send(gram_z, gram_z_in.at[s], sem_gram_z, z_peer(o))
    wait(gram_z_in, sem_gram_z)
    gram_all[place] = jnp.sum(gram_z_in[...], axis=0) + gram_z[...]
    for offset in plane_offsets:
        send(gram_all.at[place], gram_all.at[place], sem_all, plane_peer(*offset)[1])
    wait(gram_all.at[pl.ds(0, plane - 1)], sem_all)
    packed = gram_all[...].reshape(plane, LANES)
    gram_sum = jnp.concatenate([packed[:, 0:comps], packed[:, comps : 2 * comps]], axis=0)
    out[...] = solve(gram_sum, spread).T[0:width]


def on_device(counts, occupancy, start_basis):
    comps, genes = start_basis.shape
    cells = counts.shape[0]
    rows = comps // Y
    plane = H * XL * CORE * Y
    tiles = 2 * len(DIRECT) + len(PAIRED)
    dma = pltpu.SemaphoreType.DMA
    hbm = pl.BlockSpec(memory_space=pltpu.HBM)
    basis_now = pl.pallas_call(
        kernel,
        out_shape=jax.ShapeDtypeStruct((LANES // Y, comps), F32),
        in_specs=[hbm, hbm, hbm],
        out_specs=pl.BlockSpec(memory_space=pltpu.VMEM),
        scratch_shapes=[
            pltpu.VMEM((cells, genes), BF16),
            pltpu.SMEM(occupancy.shape, jnp.int32),
            pltpu.VMEM((comps, genes), BF16),
            pltpu.VMEM((cells, genes), BF16),
            pltpu.VMEM((16, genes), BF16),
            pltpu.VMEM((H, 24, LANES), F32),
            pltpu.VMEM((H * Y - 1, 24, LANES), F32),
            pltpu.VMEM((comps + 8, LANES), F32),
            pltpu.VMEM((XL * CORE - 1, comps + 8, LANES), F32),
            pltpu.VMEM((H, 24, LANES), F32),
            pltpu.VMEM((H, 24, LANES), F32),
            pltpu.VMEM((H * Y - 1, 24, LANES), F32),
            pltpu.VMEM((H, Y, 2 * len(DIRECT), rows, LANES), F32),
            pltpu.VMEM((2 * len(DIRECT), H * Y - 1, rows, LANES), F32),
            pltpu.VMEM((H, Y, len(PAIRED), rows, LANES), F32),
            pltpu.VMEM((len(PAIRED), H * Y - 1, rows, LANES), F32),
            pltpu.VMEM((H, len(PAIRED), Y, rows, LANES), F32),
            pltpu.VMEM((H, len(PAIRED), Y, rows, LANES), F32),
            pltpu.VMEM((H, Y, Z, LANES), F32),
            pltpu.VMEM((2, H * Y, Z, LANES), F32),
            pltpu.VMEM((2, Z, LANES), F32),
            pltpu.VMEM((LANES, LANES), F32),
            pltpu.VMEM((tiles, rows, LANES), F32),
            pltpu.VMEM((tiles, 2, LANES), F32),
            pltpu.VMEM((tiles - 1, rows, LANES), F32),
            pltpu.VMEM((tiles - 1, 2, LANES), F32),
            pltpu.VMEM((plane, 1, LANES), F32),
            pltpu.VMEM((plane - 1, 1, LANES), F32),
            pltpu.VMEM((1, LANES), F32),
            pltpu.VMEM((Z - 1, 1, LANES), F32),
            pltpu.VMEM((plane, 1, LANES), F32),
            dma((CHUNKS + 2,)),
            dma((2, 1)),
            dma((2, 1)),
            dma((2, 1)),
            dma((2, 1)),
            dma((2, len(DIRECT))),
            dma((2, len(PAIRED_CHUNKS))),
            dma((2, len(PAIRED_CHUNKS))),
            dma((2, 2)),
            dma((2, 1)),
            dma((2, 1)),
            dma((2, 1)),
            pltpu.SemaphoreType.REGULAR,
        ],
        compiler_params=pltpu.CompilerParams(
            collective_id=0, has_side_effects=True, vmem_limit_bytes=24 << 20
        ),
        name="subspace_step",
    )(*(pltpu.with_memory_space_constraint(a, pltpu.HBM) for a in (counts, occupancy, start_basis)))
    return basis_now.T * math.sqrt(genes * XL * CORE)


def solution(mesh):
    placed = (P("cells", "genes"), P("cells", "genes"), P(None, "genes"))
    return jax.shard_map(
        on_device, mesh=mesh, in_specs=placed, out_specs=P(None, ("genes", "cells")), check_vma=False
    )
```

```python
import math

import jax
import jax.numpy as jnp
from jax import lax
from jax.experimental import pallas as pl
from jax.experimental.pallas import tpu as pltpu
from jax.sharding import PartitionSpec as P

F32 = jnp.float32
BF16 = jnp.bfloat16
MESH = pl.DeviceIdType.MESH
Z, H, Y, XL, CORE = 16, 2, 4, 2, 2
LANES = 128
DIRECT = (8, 10)
PAIRED = (6, 4, 12, 2, 14, 0)
SCORE_ROW = 7
CHUNKS = 4
NEAR = 4
NT = (((1,), (1,)), ((), ()))


def device(z, h, y, xl, core):
    return ((z * H + h) * Y + y, xl * CORE + core)


def far_first(offsets, weights, sizes):
    def far(offset):
        return -sum(w * min(o, n - o) for o, w, n in zip(offset, weights, sizes))

    return sorted((o for o in offsets if any(o)), key=far)


def total_of(values):
    values = list(values)
    while len(values) > 1:
        values = [sum(values[i : i + 2][1:], values[i]) for i in range(0, len(values), 2)]
    return values[0]


def solve(gram, right):
    blocks = gram.shape[0] // 8
    left = [gram[8 * b : 8 * b + 8] for b in range(blocks)]
    right = [right[8 * b : 8 * b + 8] for b in range(blocks)]
    row_at = lax.broadcasted_iota(jnp.int32, (8, LANES), 0)
    done = []
    for kb in range(blocks):
        cols = [
            [
                jnp.broadcast_to(left[b][:, 8 * kb + j : 8 * kb + j + 1], (8, LANES))
                for j in range(8)
            ]
            for b in range(kb, blocks)
        ]
        rows_left, rows_right = left[kb], right[kb]
        scale = jnp.zeros((8, LANES), F32)
        steps = []
        for j in range(8):
            pivot = jnp.broadcast_to(cols[0][j][j : j + 1], (8, LANES))
            inv = lax.rsqrt(pivot)
            scale = jnp.where(row_at == j, inv, scale)
            lower = [c[j] * inv for c in cols]
            for m in range(j + 1, 8):
                entry = jnp.broadcast_to(lower[0][m : m + 1], (8, LANES))
                for c, low in zip(cols, lower):
                    c[m] = c[m] - low * entry
            below = jnp.where(row_at > j, lower[0], 0.0)
            unit_left = jnp.broadcast_to(rows_left[j : j + 1], rows_left.shape) * inv[:, : rows_left.shape[1]]
            unit_right = jnp.broadcast_to(rows_right[j : j + 1], rows_right.shape) * inv
            rows_left = rows_left - below[:, : rows_left.shape[1]] * unit_left
            rows_right = rows_right - below * unit_right
            steps.append((lower[1:], unit_left, unit_right))
        done.append(rows_right * scale)
        for at, b in enumerate(range(kb + 1, blocks)):
            for lower, unit_left, unit_right in steps:
                left[b] = left[b] - lower[at][:, : unit_left.shape[1]] * unit_left
                right[b] = right[b] - lower[at] * unit_right
    return jnp.concatenate(done, axis=0)


def kernel(
    counts_hbm,
    occupancy_hbm,
    basis_hbm,
    out,
    counts,
    occupancy,
    basis,
    cbuf,
    split_mean,
    mean_all,
    means_direct,
    means_direct_in,
    means_out,
    means_out_in,
    means_paired,
    means_paired_in,
    score,
    score_in,
    direct,
    direct_in,
    paired,
    paired_in,
    pair_out,
    pair_in,
    pair_dev,
    dev_mean,
    mean_xy,
    turned,
    zpart,
    zaux,
    zpart_in,
    zaux_in,
    gram,
    gram_in,
    gram_z,
    gram_z_in,
    gram_all,
    sem_in,
    sem_score,
    sem_means,
    sem_means_out,
    sem_means_paired,
    sem_direct,
    sem_pair,
    sem_paired,
    sem_z,
    sem_gram,
    sem_gram_z,
    sem_all,
    sem_far,
):
    cells_at, genes_at = lax.axis_index("cells"), lax.axis_index("genes")
    z, h, y = cells_at // (H * Y), lax.rem(cells_at // Y, H), lax.rem(cells_at, Y)
    xl, core = genes_at // CORE, lax.rem(genes_at, CORE)
    comps = basis.shape[0]
    rows = comps // Y
    cells = counts.shape[0]
    width = LANES // Y
    plane = H * XL * CORE * Y

    loads = [pltpu.make_async_copy(occupancy_hbm, occupancy, sem_in.at[0])]
    wide = counts.shape[1] // CHUNKS
    for c in range(CHUNKS):
        span = pl.ds(c * wide, wide)
        loads.append(pltpu.make_async_copy(counts_hbm.at[:, span], counts.at[:, span], sem_in.at[c + 1]))
    loads.append(pltpu.make_async_copy(basis_hbm, basis, sem_in.at[CHUNKS + 1]))
    for load in loads:
        load.start()

    def send(src, dst, sems, to, step=0):
        pltpu.make_async_remote_copy(
            src_ref=src,
            dst_ref=dst,
            send_sem=sems.at[0, step],
            recv_sem=sems.at[1, step],
            device_id=to,
            device_id_type=MESH,
        ).start()

    def wait(all_bytes, sems, step=0):
        pltpu.make_async_remote_copy(
            src_ref=all_bytes,
            dst_ref=all_bytes,
            send_sem=sems.at[0, step],
            recv_sem=sems.at[1, step],
            device_id=(cells_at, genes_at),
            device_id_type=MESH,
        ).wait()

    def gene_peer(a, b):
        return device(z, h, y, lax.rem(xl + a, XL), lax.rem(core + b, CORE))

    def xy_place(a, b):
        return lax.rem(h + a, H), lax.rem(y + b, Y)

    def z_peer(o):
        return device(lax.rem(z + o + Z, Z), h, y, xl, core)

    in_x = h * XL + xl
    place = (in_x * CORE + core) * Y + y

    def plane_peer(a, b, c):
        xt = lax.rem(in_x + a, H * XL)
        coret, yt = lax.rem(core + b, CORE), lax.rem(y + c, Y)
        return (xt * CORE + coret) * Y + yt, device(z, xt // XL, yt, lax.rem(xt, XL), coret)

    def z_tile(o):
        return lax.rem(z + o + Z, Z)

    beside = [1 - 2 * lax.rem(z + ht, 2) for ht in range(H)]
    own_beside = 1 - 2 * lax.rem(z + h, 2)

    gene_offsets = [(1, 0), (1, 1), (0, 1)]
    xy_offsets = far_first([(a, b) for a in range(H) for b in range(Y)], (4, 2), (H, Y))
    plane_offsets = far_first(
        [(a, b, c) for a in range(H * XL) for b in range(CORE) for c in range(Y)],
        (2, 1, 2),
        (H * XL, CORE, Y),
    )
    z_offsets = far_first([(o,) for o in range(Z)], (1,), (Z,))

    barrier = pltpu.get_barrier_semaphore()
    near = [o for o in range(1, Z) if min(o, Z - o) <= NEAR]
    peers = [gene_peer(a, b) for a, b in gene_offsets]
    peers += [device(z, *xy_place(a, b), xl, core) for a, b in xy_offsets]
    peers += [z_peer(o) for o in near]
    for peer in peers:
        pl.semaphore_signal(barrier, inc=1, device_id=peer, device_id_type=MESH)

    row_at = lax.broadcasted_iota(jnp.int32, (16, LANES), 0)
    group_at = lax.broadcasted_iota(jnp.int32, (16, LANES), 1) // width
    for ref in (means_direct, means_out, means_paired):
        ref[...] = jnp.zeros(ref.shape, F32)
    turned[...] = jnp.zeros((LANES, LANES), F32)

    def center(j):
        at = pl.ds(j * LANES, LANES)
        entries = counts[:, at].astype(F32)
        logged = jnp.log(1.0 + entries) * occupancy[0, j].astype(F32)
        mean = jnp.sum(logged, axis=0, keepdims=True) * (1.0 / cells)
        cbuf[:, at] = (logged - mean).astype(BF16)
        mean_all[j % H, j // H : j // H + 1, :] = mean
        high = mean.astype(BF16).astype(F32)
        middle = (mean - high).astype(BF16).astype(F32)
        low = mean - high - middle
        stacked = jnp.where(
            row_at == 0, high, jnp.where(row_at == 1, middle, jnp.where(row_at == 2, low, 0.0))
        )
        split_mean[:, at] = stacked.astype(BF16)

    def product_of(c):
        span = pl.ds(c * wide, wide)
        return (
            lax.dot_general(basis[:, span], cbuf[:, span], NT, preferred_element_type=F32),
            lax.dot_general(split_mean[:, span], basis[:, span], NT, preferred_element_type=F32),
        )

    loads[0].wait()
    products = []
    for c in range(CHUNKS):
        loads[c + 1].wait()
        if c == 1:
            loads[-1].wait()
        if c:
            products.append(product_of(c - 1))
        for j in range(c * wide // LANES, (c + 1) * wide // LANES):
            center(j)
    products.append(product_of(CHUNKS - 1))
    score[0:comps, :] = total_of([p for p, _ in products])
    of_mean = total_of([p for _, p in products])
    score[comps : comps + 8, :] = jnp.zeros((8, LANES), F32)
    score[comps : comps + 1, 0:comps] = of_mean[0:1] + of_mean[1:2] + of_mean[2:3]

    pl.semaphore_wait(barrier, len(peers))
    for o in (NEAR, Z - NEAR):
        pl.semaphore_signal(sem_far, inc=1, device_id=z_peer(o), device_id_type=MESH)
    of_cells, of_means = pl.ds(0, comps), pl.ds(comps, 8)
    for step, span in enumerate((of_cells, of_means)):
        for s, (a, b) in enumerate(gene_offsets):
            send(score.at[span], score_in.at[s, span], sem_score, gene_peer(a, b), step)
    for ht in range(H):
        for i in range(2 * len(DIRECT)):
            at = z_tile(DIRECT[i // 2] + i % 2 * beside[ht])
            means_direct[ht, i : i + 1, :] = mean_all[ht, pl.ds(at, 1), :]
        for j, e in enumerate(PAIRED):
            means_out[ht, j : j + 1, :] = mean_all[ht, pl.ds(z_tile(e + beside[ht]), 1), :]
            means_paired[ht, j : j + 1, :] = mean_all[ht, pl.ds(z_tile(e), 1), :]
    wait(score_in.at[:, of_cells], sem_score)
    scores = total_of([score[0:comps]] + [score_in[a, 0:comps] for a in range(XL * CORE - 1)])
    score_high = scores.astype(BF16)
    score_low = (scores - score_high.astype(F32)).astype(BF16)
    stacked = jnp.concatenate([score_high, score_low], axis=0)

    def pieces(tiles):
        columns = [
            cbuf[:, pl.ds(pl.multiple_of((tiles[ht] * H + ht) * LANES, LANES), LANES)] for ht in range(H)
        ]
        both = jnp.dot(stacked, jnp.concatenate(columns, axis=1), preferred_element_type=F32)
        product = both[:comps] + both[comps:]
        result = []
        for ht in range(H):
            turns = []
            for b in range(Y):
                block = product[b * rows : (b + 1) * rows, ht * LANES : (ht + 1) * LANES]
                turns.append([block] + [pltpu.roll(block, k * width, 1) for k in range(1, Y)])
            for yt in range(Y):
                piece = turns[0][(0 - yt) % Y]
                for b in range(1, Y):
                    piece = jnp.where(group_at == b, turns[b][(b - yt) % Y], piece)
                result.append((ht, yt, piece))
        return result

    def exchange(src, dst, sems, chunk, span):
        for s, (a, b) in enumerate(xy_offsets):
            ht, yt = xy_place(a, b)
            send(src.at[ht, yt, span], dst.at[span, s], sems, device(z, ht, yt, xl, core), chunk)

    def start_direct(j):
        tiles = [z_tile(DIRECT[j])] * H
        for ht, yt, piece in pieces(tiles):
            direct[ht, yt, 2 * j] = piece
        for ht, yt, piece in pieces([z_tile(DIRECT[j] + beside[ht]) for ht in range(H)]):
            direct[ht, yt, 2 * j + 1] = piece
        exchange(direct, direct_in, sem_direct, j, pl.ds(2 * j, 2))

    def start_pair(j):
        for ht, yt, piece in pieces([z_tile(PAIRED[j] + beside[ht]) for ht in range(H)]):
            pair_out[ht, j, yt] = piece
        for ht in range(H):
            send(pair_out.at[ht, j], pair_in.at[ht, j], sem_pair, z_peer(beside[ht]), j)

    def send_means():
        wait(score_in.at[:, of_means], sem_score, 1)
        whole = total_of(
            [score[comps : comps + 1]]
            + [score_in[a, comps : comps + 1] for a in range(XL * CORE - 1)]
        )
        for ht in range(H):
            for ref in (means_direct, means_out, means_paired):
                ref[ht, SCORE_ROW : SCORE_ROW + 1, :] = whole
            send(means_out.at[ht], means_out_in.at[ht], sem_means_out, z_peer(beside[ht]))
        for s, (a, b) in enumerate(xy_offsets):
            ht, yt = xy_place(a, b)
            send(means_direct.at[ht], means_direct_in.at[s], sem_means, device(z, ht, yt, xl, core))

    start_pair(0)
    send_means()
    start_direct(0)
    start_pair(1)
    start_direct(1)
    for j in range(2, len(PAIRED)):
        start_pair(j)
    for j, e in enumerate(PAIRED):
        for ht, yt, piece in pieces([z_tile(e)] * H):
            paired[ht, yt, j] = piece

    def fold_rows(values):
        for p, value in enumerate(values):
            turned[p : p + 1, :] = value
        flat = turned[...].T
        result = []
        for p in range(len(values)):
            folded = jnp.broadcast_to(flat[0:rows, p : p + 1], (rows, LANES))
            for b in range(1, Y):
                block = jnp.broadcast_to(flat[b * rows : (b + 1) * rows, p : p + 1], (rows, LANES))
                folded = jnp.where(group_at == b, block, folded)
            result.append(folded)
        return result

    def columns_of(means, yt):
        kept = jnp.where(group_at[0:8] == yt, means, 0.0)
        return total_of([kept] + [pltpu.roll(kept, k * width, 1) for k in range(1, Y)])

    groups = len(xy_offsets) + 1

    def plane_terms(level, weight, own, others):
        values = [own[h]] + [others[s] for s in range(groups - 1)]
        middle = total_of(values) * (1.0 / groups)
        apart = [value - middle for value in values]
        away = fold_rows([a[SCORE_ROW : SCORE_ROW + 1] * weight for a in apart])
        mean_xy[level] = columns_of(middle, y)
        for p, value in enumerate(apart):
            dev_mean[level, p] = columns_of(value, y)
        return middle[SCORE_ROW : SCORE_ROW + 1], away

    wait(means_out_in, sem_means_out)
    apart = [means_paired[ht] - means_out_in[ht] for ht in range(H)]
    pair_away = fold_rows([a[SCORE_ROW : SCORE_ROW + 1] * (0.5 * cells) for a in apart])
    for ht in range(H):
        means_paired[ht] = 0.5 * (means_paired[ht] + means_out_in[ht])
        for yt in range(Y):
            pair_dev[ht, yt] = columns_of(apart[ht], yt)
    for s, (a, b) in enumerate(xy_offsets):
        ht, yt = xy_place(a, b)
        send(
            means_paired.at[ht],
            means_paired_in.at[s],
            sem_means_paired,
            device(z, ht, yt, xl, core),
        )
    def add_pair(j):
        wait(pair_in.at[:, j], sem_pair, j)
        for ht in range(H):
            for yt in range(Y):
                paired[ht, yt, j] = (paired[ht, yt, j] + pair_in[ht, j, yt]) + pair_away[
                    ht
                ] * pair_dev[ht, yt, j : j + 1, :]
        exchange(paired, paired_in, sem_paired, j, pl.ds(j, 1))

    def plane_sum(level, slot, own, others, i, away, middle, to):
        terms = [own[h, y, i]] + [others[i, s] for s in range(groups - 1)]
        terms += [away[p] * dev_mean[level, p, i : i + 1, :] for p in range(groups)]
        zpart[slot] = total_of(terms)
        zaux[slot, 0:1, :] = mean_xy[level, i : i + 1, :]
        zaux[slot, 1:2, :] = middle
        if to is not None:
            send(zpart.at[slot], zpart_in.at[slot], sem_z, to)
            send(zaux.at[slot], zaux_in.at[slot], sem_z, to, 1)

    def sum_direct(j):
        wait(direct_in.at[pl.ds(2 * j, 2)], sem_direct, j)
        for i, o in ((2 * j, DIRECT[j]), (2 * j + 1, DIRECT[j] + own_beside)):
            plane_sum(0, i, direct, direct_in, i, away_direct, score_direct, z_peer(o))

    for j in range(len(PAIRED) - 1):
        add_pair(j)
    wait(means_direct_in, sem_means)
    score_direct, away_direct = plane_terms(0, float(cells), means_direct, means_direct_in)
    pl.semaphore_wait(sem_far, 2)
    sum_direct(0)
    add_pair(len(PAIRED) - 1)
    sum_direct(1)
    wait(means_paired_in, sem_means_paired)
    score_paired, away_paired = plane_terms(1, 2.0 * cells, means_paired, means_paired_in)
    alone = 2 * len(DIRECT)
    for j, e in enumerate(PAIRED):
        wait(paired_in.at[pl.ds(j, 1)], sem_paired, j)
        to = z_peer(e) if e else None
        plane_sum(1, alone + j, paired, paired_in, j, away_paired, score_paired, to)
    wait(zpart_in, sem_z)
    wait(zaux_in, sem_z, 1)
    last = alone + len(PAIRED) - 1
    shares = [1.0] * alone + [2.0] * len(PAIRED)
    means = [zaux_in[i, 0:1, :] for i in range(last)] + [zaux[last, 0:1, :]]
    scores_of = [zaux_in[i, 1:2, :] for i in range(last)] + [zaux[last, 1:2, :]]
    middle = total_of([v * w for v, w in zip(scores_of, shares)]) * (1.0 / Z)
    away = fold_rows([(v - middle) * (w * cells * groups) for v, w in zip(scores_of, shares)])
    middle = total_of([v * w for v, w in zip(means, shares)]) * (1.0 / Z)
    terms = [zpart[last]] + [zpart_in[i] for i in range(last)]
    terms += [far * (value - middle) for far, value in zip(away, means)]
    folded = total_of(terms)

    blocks = [folded] + [pltpu.roll(folded, (Y - b) * width, 1) for b in range(1, Y)]
    spread = jnp.concatenate([jnp.where(group_at == 0, block, 0.0) for block in blocks], axis=0)
    own_gram = lax.dot_general(
        spread, spread, NT, precision=lax.Precision.HIGHEST, preferred_element_type=F32
    )
    packed = jnp.concatenate([own_gram[0:plane], own_gram[plane:]], axis=1)
    for e in range(plane):
        gram[e] = packed[e : e + 1]
    for s, offset in enumerate(plane_offsets):
        at, to = plane_peer(*offset)
        send(gram.at[at], gram_in.at[s], sem_gram, to)
    wait(gram_in, sem_gram)
    gram_z[...] = jnp.sum(gram_in[...], axis=0) + gram[place]
    for s, (o,) in enumerate(z_offsets):
        send(gram_z, gram_z_in.at[s], sem_gram_z, z_peer(o))
    wait(gram_z_in, sem_gram_z)
    gram_all[place] = jnp.sum(gram_z_in[...], axis=0) + gram_z[...]
    for offset in plane_offsets:
        send(gram_all.at[place], gram_all.at[place], sem_all, plane_peer(*offset)[1])
    wait(gram_all.at[pl.ds(0, plane - 1)], sem_all)
    packed = gram_all[...].reshape(plane, LANES)
    gram_sum = jnp.concatenate([packed[:, 0:comps], packed[:, comps : 2 * comps]], axis=0)
    out[...] = solve(gram_sum, spread).T[0:width]


def on_device(counts, occupancy, start_basis):
    comps, genes = start_basis.shape
    cells = counts.shape[0]
    rows = comps // Y
    plane = H * XL * CORE * Y
    tiles = 2 * len(DIRECT) + len(PAIRED)
    dma = pltpu.SemaphoreType.DMA
    hbm = pl.BlockSpec(memory_space=pltpu.HBM)
    basis_now = pl.pallas_call(
        kernel,
        out_shape=jax.ShapeDtypeStruct((LANES // Y, comps), F32),
        in_specs=[hbm, hbm, hbm],
        out_specs=pl.BlockSpec(memory_space=pltpu.VMEM),
        scratch_shapes=[
            pltpu.VMEM((cells, genes), BF16),
            pltpu.SMEM(occupancy.shape, jnp.int32),
            pltpu.VMEM((comps, genes), BF16),
            pltpu.VMEM((cells, genes), BF16),
            pltpu.VMEM((16, genes), BF16),
            pltpu.VMEM((H, Z, LANES), F32),
            pltpu.VMEM((H, 8, LANES), F32),
            pltpu.VMEM((H * Y - 1, 8, LANES), F32),
            pltpu.VMEM((H, 8, LANES), F32),
            pltpu.VMEM((H, 8, LANES), F32),
            pltpu.VMEM((H, 8, LANES), F32),
            pltpu.VMEM((H * Y - 1, 8, LANES), F32),
            pltpu.VMEM((comps + 8, LANES), F32),
            pltpu.VMEM((XL * CORE - 1, comps + 8, LANES), F32),
            pltpu.VMEM((H, Y, 2 * len(DIRECT), rows, LANES), F32),
            pltpu.VMEM((2 * len(DIRECT), H * Y - 1, rows, LANES), F32),
            pltpu.VMEM((H, Y, len(PAIRED), rows, LANES), F32),
            pltpu.VMEM((len(PAIRED), H * Y - 1, rows, LANES), F32),
            pltpu.VMEM((H, len(PAIRED), Y, rows, LANES), F32),
            pltpu.VMEM((H, len(PAIRED), Y, rows, LANES), F32),
            pltpu.VMEM((H, Y, 8, LANES), F32),
            pltpu.VMEM((2, H * Y, 8, LANES), F32),
            pltpu.VMEM((2, 8, LANES), F32),
            pltpu.VMEM((LANES, LANES), F32),
            pltpu.VMEM((tiles, rows, LANES), F32),
            pltpu.VMEM((tiles, 2, LANES), F32),
            pltpu.VMEM((tiles - 1, rows, LANES), F32),
            pltpu.VMEM((tiles - 1, 2, LANES), F32),
            pltpu.VMEM((plane, 1, LANES), F32),
            pltpu.VMEM((plane - 1, 1, LANES), F32),
            pltpu.VMEM((1, LANES), F32),
            pltpu.VMEM((Z - 1, 1, LANES), F32),
            pltpu.VMEM((plane, 1, LANES), F32),
            dma((CHUNKS + 2,)),
            dma((2, 2)),
            dma((2, 1)),
            dma((2, 1)),
            dma((2, 1)),
            dma((2, len(DIRECT))),
            dma((2, len(PAIRED))),
            dma((2, len(PAIRED))),
            dma((2, 2)),
            dma((2, 1)),
            dma((2, 1)),
            dma((2, 1)),
            pltpu.SemaphoreType.REGULAR,
        ],
        compiler_params=pltpu.CompilerParams(
            collective_id=0, has_side_effects=True, vmem_limit_bytes=24 << 20
        ),
        name="subspace_step",
    )(*(pltpu.with_memory_space_constraint(a, pltpu.HBM) for a in (counts, occupancy, start_basis)))
    return basis_now.T * math.sqrt(genes * XL * CORE)


def solution(mesh):
    placed = (P("cells", "genes"), P("cells", "genes"), P(None, "genes"))
    return jax.shard_map(
        on_device, mesh=mesh, in_specs=placed, out_specs=P(None, ("genes", "cells")), check_vma=False
    )
```

```python
import math

import jax
import jax.numpy as jnp
from jax import lax
from jax.experimental import pallas as pl
from jax.experimental.pallas import tpu as pltpu
from jax.sharding import PartitionSpec as P

F32 = jnp.float32
BF16 = jnp.bfloat16
MESH = pl.DeviceIdType.MESH
Z, H, Y, XL, CORE = 16, 2, 4, 2, 2
LANES = 128
DIRECT = (8, 10)
PAIRED = (6, 4, 12, 2, 14, 0)
SCORE_ROW = 7
LEAD = 1
CHUNKS = 4
NEAR = 4
NT = (((1,), (1,)), ((), ()))


def device(z, h, y, xl, core):
    return ((z * H + h) * Y + y, xl * CORE + core)


def far_first(offsets, weights, sizes):
    def far(offset):
        return -sum(w * min(o, n - o) for o, w, n in zip(offset, weights, sizes))

    return sorted((o for o in offsets if any(o)), key=far)


def total_of(values):
    values = list(values)
    while len(values) > 1:
        values = [sum(values[i : i + 2][1:], values[i]) for i in range(0, len(values), 2)]
    return values[0]


def solve(gram, right):
    blocks = gram.shape[0] // 8
    left = [gram[8 * b : 8 * b + 8] for b in range(blocks)]
    right = [right[8 * b : 8 * b + 8] for b in range(blocks)]
    row_at = lax.broadcasted_iota(jnp.int32, (8, LANES), 0)
    done = []
    for kb in range(blocks):
        cols = [
            [
                jnp.broadcast_to(left[b][:, 8 * kb + j : 8 * kb + j + 1], (8, LANES))
                for j in range(8)
            ]
            for b in range(kb, blocks)
        ]
        rows_left, rows_right = left[kb], right[kb]
        scale = jnp.zeros((8, LANES), F32)
        steps = []
        for j in range(8):
            pivot = jnp.broadcast_to(cols[0][j][j : j + 1], (8, LANES))
            inv = lax.rsqrt(pivot)
            scale = jnp.where(row_at == j, inv, scale)
            lower = [c[j] * inv for c in cols]
            for m in range(j + 1, 8):
                entry = jnp.broadcast_to(lower[0][m : m + 1], (8, LANES))
                for c, low in zip(cols, lower):
                    c[m] = c[m] - low * entry
            below = jnp.where(row_at > j, lower[0], 0.0)
            unit_left = jnp.broadcast_to(rows_left[j : j + 1], rows_left.shape) * inv[:, : rows_left.shape[1]]
            unit_right = jnp.broadcast_to(rows_right[j : j + 1], rows_right.shape) * inv
            rows_left = rows_left - below[:, : rows_left.shape[1]] * unit_left
            rows_right = rows_right - below * unit_right
            steps.append((lower[1:], unit_left, unit_right))
        done.append(rows_right * scale)
        for at, b in enumerate(range(kb + 1, blocks)):
            for lower, unit_left, unit_right in steps:
                left[b] = left[b] - lower[at][:, : unit_left.shape[1]] * unit_left
                right[b] = right[b] - lower[at] * unit_right
    return jnp.concatenate(done, axis=0)


def kernel(
    counts_hbm,
    occupancy_hbm,
    basis_hbm,
    out,
    counts,
    occupancy,
    basis,
    cbuf,
    split_mean,
    mean_all,
    means_direct,
    means_direct_in,
    means_out,
    means_out_in,
    means_paired,
    means_paired_in,
    score,
    score_in,
    direct,
    direct_in,
    paired,
    paired_in,
    pair_out,
    pair_in,
    pair_dev,
    dev_mean,
    mean_xy,
    turned,
    zpart,
    zaux,
    zpart_in,
    zaux_in,
    gram,
    gram_in,
    gram_z,
    gram_z_in,
    gram_all,
    sem_in,
    sem_score,
    sem_means,
    sem_means_out,
    sem_means_paired,
    sem_direct,
    sem_pair,
    sem_paired,
    sem_z,
    sem_gram,
    sem_gram_z,
    sem_all,
    sem_far,
):
    cells_at, genes_at = lax.axis_index("cells"), lax.axis_index("genes")
    z, h, y = cells_at // (H * Y), lax.rem(cells_at // Y, H), lax.rem(cells_at, Y)
    xl, core = genes_at // CORE, lax.rem(genes_at, CORE)
    comps = basis.shape[0]
    rows = comps // Y
    cells = counts.shape[0]
    width = LANES // Y
    plane = H * XL * CORE * Y

    loads = [pltpu.make_async_copy(occupancy_hbm, occupancy, sem_in.at[0])]
    wide = counts.shape[1] // CHUNKS
    for c in range(CHUNKS):
        span = pl.ds(c * wide, wide)
        loads.append(pltpu.make_async_copy(counts_hbm.at[:, span], counts.at[:, span], sem_in.at[c + 1]))
    loads.append(pltpu.make_async_copy(basis_hbm, basis, sem_in.at[CHUNKS + 1]))
    for load in loads:
        load.start()

    def send(src, dst, sems, to, step=0):
        pltpu.make_async_remote_copy(
            src_ref=src,
            dst_ref=dst,
            send_sem=sems.at[0, step],
            recv_sem=sems.at[1, step],
            device_id=to if len(to) == 2 else device(*to),
            device_id_type=MESH,
        ).start()

    def waiting(all_bytes, sems, step):
        return pltpu.make_async_remote_copy(
            src_ref=all_bytes,
            dst_ref=all_bytes,
            send_sem=sems.at[0, step],
            recv_sem=sems.at[1, step],
            device_id=(cells_at, genes_at),
            device_id_type=MESH,
        )

    def wait_out(all_bytes, sems, step=0):
        waiting(all_bytes, sems, step).wait_send()

    def wait_in(all_bytes, sems, step=0):
        waiting(all_bytes, sems, step).wait_recv()

    def wait(all_bytes, sems, step=0):
        wait_out(all_bytes, sems, step)
        wait_in(all_bytes, sems, step)

    def gene_peer(a, b):
        return device(z, h, y, lax.rem(xl + a, XL), lax.rem(core + b, CORE))

    def xy_place(a, b):
        return lax.rem(h + a, H), lax.rem(y + b, Y)

    def z_peer(o):
        return device(lax.rem(z + o + Z, Z), h, y, xl, core)

    in_x = h * XL + xl
    chip = in_x * Y + y

    def chip_peer(a, c):
        xt, yt = lax.rem(in_x + a, H * XL), lax.rem(y + c, Y)
        return xt * Y + yt, (z, xt // XL, yt, lax.rem(xt, XL))

    def z_tile(o):
        return lax.rem(z + o + Z, Z)

    beside = [1 - 2 * lax.rem(z + ht, 2) for ht in range(H)]
    own_beside = 1 - 2 * lax.rem(z + h, 2)

    gene_offsets = [(1, 0), (1, 1), (0, 1)]
    xy_offsets = far_first([(a, b) for a in range(H) for b in range(Y)], (4, 2), (H, Y))
    chip_offsets = far_first([(a, c) for a in range(H * XL) for c in range(Y)], (1, 1), (H * XL, Y))
    z_offsets = far_first([(o,) for o in range(Z)], (1,), (Z,))

    barrier = pltpu.get_barrier_semaphore()
    near = [o for o in range(1, Z) if min(o, Z - o) <= NEAR]
    peers = [gene_peer(a, b) for a, b in gene_offsets]
    peers += [device(z, *xy_place(a, b), xl, core) for a, b in xy_offsets]
    peers += [z_peer(o) for o in near]
    for peer in peers:
        pl.semaphore_signal(barrier, inc=1, device_id=peer, device_id_type=MESH)

    row_at = lax.broadcasted_iota(jnp.int32, (16, LANES), 0)
    group_at = lax.broadcasted_iota(jnp.int32, (16, LANES), 1) // width
    for ref in (means_direct, means_out, means_paired):
        ref[...] = jnp.zeros(ref.shape, F32)
    turned[...] = jnp.zeros((LANES, LANES), F32)

    def center(j):
        at = pl.ds(j * LANES, LANES)
        entries = counts[:, at].astype(F32)
        logged = jnp.log(1.0 + entries) * occupancy[0, j].astype(F32)
        mean = jnp.sum(logged, axis=0, keepdims=True) * (1.0 / cells)
        cbuf[:, at] = (logged - mean).astype(BF16)
        mean_all[j % H, j // H : j // H + 1, :] = mean

    def product_of(c):
        span = pl.ds(c * wide, wide)
        return lax.dot_general(basis[:, span], cbuf[:, span], NT, preferred_element_type=F32)

    loads[0].wait()
    products = []
    for c in range(CHUNKS):
        loads[c + 1].wait()
        if c == 1:
            loads[-1].wait()
        if c:
            products.append(product_of(c - 1))
        for j in range(c * wide // LANES, (c + 1) * wide // LANES):
            center(j)
    products.append(product_of(CHUNKS - 1))
    score[0:comps, :] = total_of(products)

    pl.semaphore_wait(barrier, len(peers))
    for o in (NEAR, Z - NEAR):
        pl.semaphore_signal(sem_far, inc=1, device_id=z_peer(o), device_id_type=MESH)
    of_cells, of_means = pl.ds(0, comps), pl.ds(comps, 8)

    def send_scores(span, step):
        for s, (a, b) in enumerate(gene_offsets):
            send(score.at[span], score_in.at[s, span], sem_score, gene_peer(a, b), step)

    send_scores(of_cells, 0)
    for j in range(Z * H):
        mean = mean_all[j % H, j // H : j // H + 1, :]
        high = mean.astype(BF16).astype(F32)
        middle = (mean - high).astype(BF16).astype(F32)
        low = mean - high - middle
        stacked = jnp.where(
            row_at == 0, high, jnp.where(row_at == 1, middle, jnp.where(row_at == 2, low, 0.0))
        )
        split_mean[:, j * LANES : (j + 1) * LANES] = stacked.astype(BF16)
    of_mean = lax.dot_general(split_mean[...], basis[...], NT, preferred_element_type=F32)
    score[comps : comps + 8, :] = jnp.zeros((8, LANES), F32)
    score[comps : comps + 1, 0:comps] = of_mean[0:1] + of_mean[1:2] + of_mean[2:3]
    send_scores(of_means, 1)
    for ht in range(H):
        for i in range(2 * len(DIRECT)):
            at = z_tile(DIRECT[i // 2] + i % 2 * beside[ht])
            means_direct[ht, i : i + 1, :] = mean_all[ht, pl.ds(at, 1), :]
        for j, e in enumerate(PAIRED):
            means_out[ht, j : j + 1, :] = mean_all[ht, pl.ds(z_tile(e + beside[ht]), 1), :]
            means_paired[ht, j : j + 1, :] = mean_all[ht, pl.ds(z_tile(e), 1), :]
    wait(score_in.at[:, of_cells], sem_score)
    scores = total_of([score[0:comps]] + [score_in[a, 0:comps] for a in range(XL * CORE - 1)])
    score_high = scores.astype(BF16)
    score_low = (scores - score_high.astype(F32)).astype(BF16)
    stacked = jnp.concatenate([score_high, score_low], axis=0)

    def pieces(tiles):
        columns = [
            cbuf[:, pl.ds(pl.multiple_of((tiles[ht] * H + ht) * LANES, LANES), LANES)] for ht in range(H)
        ]
        both = jnp.dot(stacked, jnp.concatenate(columns, axis=1), preferred_element_type=F32)
        product = both[:comps] + both[comps:]
        result = []
        for ht in range(H):
            turns = []
            for b in range(Y):
                block = product[b * rows : (b + 1) * rows, ht * LANES : (ht + 1) * LANES]
                turns.append([block] + [pltpu.roll(block, k * width, 1) for k in range(1, Y)])
            for yt in range(Y):
                piece = turns[0][(0 - yt) % Y]
                for b in range(1, Y):
                    piece = jnp.where(group_at == b, turns[b][(b - yt) % Y], piece)
                result.append((ht, yt, piece))
        return result

    def exchange(src, dst, sems, chunk, span):
        for s, (a, b) in enumerate(xy_offsets):
            ht, yt = xy_place(a, b)
            send(src.at[ht, yt, span], dst.at[span, s], sems, device(z, ht, yt, xl, core), chunk)

    def start_direct(i):
        e = DIRECT[i // 2]
        for ht, yt, piece in pieces([z_tile(e + i % 2 * beside[ht]) for ht in range(H)]):
            direct[ht, yt, i] = piece
        exchange(direct, direct_in, sem_direct, i, pl.ds(i, 1))

    def start_pair(j):
        for ht, yt, piece in pieces([z_tile(PAIRED[j] + beside[ht]) for ht in range(H)]):
            pair_out[ht, j, yt] = piece
        for ht in range(H):
            send(pair_out.at[ht, j], pair_in.at[ht, j], sem_pair, z_peer(beside[ht]), j)

    def send_means():
        wait(score_in.at[:, of_means], sem_score, 1)
        whole = total_of(
            [score[comps : comps + 1]]
            + [score_in[a, comps : comps + 1] for a in range(XL * CORE - 1)]
        )
        for ht in range(H):
            for ref in (means_direct, means_out, means_paired):
                ref[ht, SCORE_ROW : SCORE_ROW + 1, :] = whole
            send(means_out.at[ht], means_out_in.at[ht], sem_means_out, z_peer(beside[ht]))
        for s, (a, b) in enumerate(xy_offsets):
            ht, yt = xy_place(a, b)
            send(means_direct.at[ht], means_direct_in.at[s], sem_means, device(z, ht, yt, xl, core))

    start_pair(0)
    start_direct(0)
    send_means()
    start_pair(1)
    start_direct(1)
    for i in range(2, 2 * len(DIRECT)):
        start_direct(i)
    for j in range(2, len(PAIRED)):
        start_pair(j)
    for j, e in enumerate(PAIRED):
        for ht, yt, piece in pieces([z_tile(e)] * H):
            paired[ht, yt, j] = piece

    def fold_rows(values):
        for p, value in enumerate(values):
            turned[p : p + 1, :] = value
        flat = turned[...].T
        result = []
        for p in range(len(values)):
            folded = jnp.broadcast_to(flat[0:rows, p : p + 1], (rows, LANES))
            for b in range(1, Y):
                block = jnp.broadcast_to(flat[b * rows : (b + 1) * rows, p : p + 1], (rows, LANES))
                folded = jnp.where(group_at == b, block, folded)
            result.append(folded)
        return result

    def columns_of(means, yt):
        kept = jnp.where(group_at[0:8] == yt, means, 0.0)
        return total_of([kept] + [pltpu.roll(kept, k * width, 1) for k in range(1, Y)])

    groups = len(xy_offsets) + 1

    def plane_terms(level, weight, own, others):
        values = [own[h]] + [others[s] for s in range(groups - 1)]
        middle = total_of(values) * (1.0 / groups)
        apart = [value - middle for value in values]
        away = fold_rows([a[SCORE_ROW : SCORE_ROW + 1] * weight for a in apart])
        mean_xy[level] = columns_of(middle, y)
        for p, value in enumerate(apart):
            dev_mean[level, p] = columns_of(value, y)
        return middle[SCORE_ROW : SCORE_ROW + 1], away

    wait(means_out_in, sem_means_out)
    apart = [means_paired[ht] - means_out_in[ht] for ht in range(H)]
    pair_away = fold_rows([a[SCORE_ROW : SCORE_ROW + 1] * (0.5 * cells) for a in apart])
    for ht in range(H):
        means_paired[ht] = 0.5 * (means_paired[ht] + means_out_in[ht])
        for yt in range(Y):
            pair_dev[ht, yt] = columns_of(apart[ht], yt)
    for s, (a, b) in enumerate(xy_offsets):
        ht, yt = xy_place(a, b)
        send(
            means_paired.at[ht],
            means_paired_in.at[s],
            sem_means_paired,
            device(z, ht, yt, xl, core),
        )
    def add_pair(j):
        wait(pair_in.at[:, j], sem_pair, j)
        for ht in range(H):
            for yt in range(Y):
                paired[ht, yt, j] = (paired[ht, yt, j] + pair_in[ht, j, yt]) + pair_away[
                    ht
                ] * pair_dev[ht, yt, j : j + 1, :]
        exchange(paired, paired_in, sem_paired, j, pl.ds(j, 1))

    def plane_sum(level, slot, own, others, i, away, middle, to):
        terms = [own[h, y, i]] + [others[i, s] for s in range(groups - 1)]
        terms += [away[p] * dev_mean[level, p, i : i + 1, :] for p in range(groups)]
        zpart[slot] = total_of(terms)
        zaux[slot, 0:1, :] = mean_xy[level, i : i + 1, :]
        zaux[slot, 1:2, :] = middle
        if to is not None:
            send(zpart.at[slot], zpart_in.at[slot], sem_z, to)
            send(zaux.at[slot], zaux_in.at[slot], sem_z, to, 1)

    def sum_direct(i):
        wait(direct_in.at[pl.ds(i, 1)], sem_direct, i)
        to = z_peer(DIRECT[i // 2] + i % 2 * own_beside)
        plane_sum(0, i, direct, direct_in, i, away_direct, score_direct, to)

    for j in range(len(PAIRED) - 1):
        add_pair(j)
    wait(means_direct_in, sem_means)
    score_direct, away_direct = plane_terms(0, float(cells), means_direct, means_direct_in)
    pl.semaphore_wait(sem_far, 2)
    sum_direct(0)
    sum_direct(1)
    add_pair(len(PAIRED) - 1)
    for i in range(2, 2 * len(DIRECT)):
        sum_direct(i)
    wait(means_paired_in, sem_means_paired)
    score_paired, away_paired = plane_terms(1, 2.0 * cells, means_paired, means_paired_in)
    alone = 2 * len(DIRECT)
    for j, e in enumerate(PAIRED):
        wait(paired_in.at[pl.ds(j, 1)], sem_paired, j)
        to = z_peer(e) if e else None
        plane_sum(1, alone + j, paired, paired_in, j, away_paired, score_paired, to)
    wait(zpart_in, sem_z)
    wait(zaux_in, sem_z, 1)
    last = alone + len(PAIRED) - 1
    shares = [1.0] * alone + [2.0] * len(PAIRED)
    means = [zaux_in[i, 0:1, :] for i in range(last)] + [zaux[last, 0:1, :]]
    scores_of = [zaux_in[i, 1:2, :] for i in range(last)] + [zaux[last, 1:2, :]]
    middle = total_of([v * w for v, w in zip(scores_of, shares)]) * (1.0 / Z)
    away = fold_rows([(v - middle) * (w * cells * groups) for v, w in zip(scores_of, shares)])
    middle = total_of([v * w for v, w in zip(means, shares)]) * (1.0 / Z)
    terms = [zpart[last]] + [zpart_in[i] for i in range(last)]
    terms += [far * (value - middle) for far, value in zip(away, means)]
    folded = total_of(terms)

    blocks = [folded] + [pltpu.roll(folded, (Y - b) * width, 1) for b in range(1, Y)]
    spread = jnp.concatenate([jnp.where(group_at == 0, block, 0.0) for block in blocks], axis=0)
    own_gram = lax.dot_general(
        spread, spread, NT, precision=lax.Precision.HIGHEST, preferred_element_type=F32
    )
    packed = jnp.concatenate([own_gram[0 : comps // 2], own_gram[comps // 2 :]], axis=1)
    chips = plane // CORE
    for e in range(chips):
        gram[e] = packed[2 * e : 2 * e + 2]
    leads = core == LEAD
    for s, offset in enumerate(chip_offsets):
        at, to = chip_peer(*offset)
        send(gram.at[at], gram_in.at[s + (CORE - 1 - core) * (chips - 1)], sem_gram, (*to, LEAD))

    @pl.when(jnp.logical_not(leads))
    def _():
        send(gram.at[chip], gram_in.at[plane - 2], sem_gram, (*chip_peer(0, 0)[1], LEAD))
        wait_out(gram, sem_gram)

    @pl.when(leads)
    def _():
        wait_out(gram.at[pl.ds(0, chips - 1)], sem_gram)
        wait_in(gram_in, sem_gram)
        gram_z[...] = jnp.sum(gram_in[...], axis=0) + gram[chip]
        for s, (o,) in enumerate(z_offsets):
            send(gram_z, gram_z_in.at[s], sem_gram_z, z_peer(o))
        wait(gram_z_in, sem_gram_z)
        gram_all[chip] = jnp.sum(gram_z_in[...], axis=0) + gram_z[...]
        for offset in chip_offsets:
            for other in range(CORE):
                send(gram_all.at[chip], gram_all.at[chip], sem_all, (*chip_peer(*offset)[1], other))
        send(gram_all.at[chip], gram_all.at[chip], sem_all, (*chip_peer(0, 0)[1], 1 - LEAD))
        wait_out(gram_in, sem_all)
        wait_in(gram_all.at[pl.ds(0, chips - 1)], sem_all)

    @pl.when(jnp.logical_not(leads))
    def _():
        wait_in(gram_all, sem_all)

    packed = gram_all[...].reshape(comps // 2, LANES)
    gram_sum = jnp.concatenate([packed[:, 0:comps], packed[:, comps : 2 * comps]], axis=0)
    out[...] = solve(gram_sum, spread).T[0:width]


def on_device(counts, occupancy, start_basis):
    comps, genes = start_basis.shape
    cells = counts.shape[0]
    rows = comps // Y
    plane = H * XL * CORE * Y
    tiles = 2 * len(DIRECT) + len(PAIRED)
    dma = pltpu.SemaphoreType.DMA
    hbm = pl.BlockSpec(memory_space=pltpu.HBM)
    basis_now = pl.pallas_call(
        kernel,
        out_shape=jax.ShapeDtypeStruct((LANES // Y, comps), F32),
        in_specs=[hbm, hbm, hbm],
        out_specs=pl.BlockSpec(memory_space=pltpu.VMEM),
        scratch_shapes=[
            pltpu.VMEM((cells, genes), BF16),
            pltpu.SMEM(occupancy.shape, jnp.int32),
            pltpu.VMEM((comps, genes), BF16),
            pltpu.VMEM((cells, genes), BF16),
            pltpu.VMEM((16, genes), BF16),
            pltpu.VMEM((H, Z, LANES), F32),
            pltpu.VMEM((H, 8, LANES), F32),
            pltpu.VMEM((H * Y - 1, 8, LANES), F32),
            pltpu.VMEM((H, 8, LANES), F32),
            pltpu.VMEM((H, 8, LANES), F32),
            pltpu.VMEM((H, 8, LANES), F32),
            pltpu.VMEM((H * Y - 1, 8, LANES), F32),
            pltpu.VMEM((comps + 8, LANES), F32),
            pltpu.VMEM((XL * CORE - 1, comps + 8, LANES), F32),
            pltpu.VMEM((H, Y, 2 * len(DIRECT), rows, LANES), F32),
            pltpu.VMEM((2 * len(DIRECT), H * Y - 1, rows, LANES), F32),
            pltpu.VMEM((H, Y, len(PAIRED), rows, LANES), F32),
            pltpu.VMEM((len(PAIRED), H * Y - 1, rows, LANES), F32),
            pltpu.VMEM((H, len(PAIRED), Y, rows, LANES), F32),
            pltpu.VMEM((H, len(PAIRED), Y, rows, LANES), F32),
            pltpu.VMEM((H, Y, 8, LANES), F32),
            pltpu.VMEM((2, H * Y, 8, LANES), F32),
            pltpu.VMEM((2, 8, LANES), F32),
            pltpu.VMEM((LANES, LANES), F32),
            pltpu.VMEM((tiles, rows, LANES), F32),
            pltpu.VMEM((tiles, 2, LANES), F32),
            pltpu.VMEM((tiles - 1, rows, LANES), F32),
            pltpu.VMEM((tiles - 1, 2, LANES), F32),
            pltpu.VMEM((plane // CORE, 2, LANES), F32),
            pltpu.VMEM((plane - 1, 2, LANES), F32),
            pltpu.VMEM((2, LANES), F32),
            pltpu.VMEM((Z - 1, 2, LANES), F32),
            pltpu.VMEM((plane // CORE, 2, LANES), F32),
            dma((CHUNKS + 2,)),
            dma((2, 2)),
            dma((2, 1)),
            dma((2, 1)),
            dma((2, 1)),
            dma((2, 2 * len(DIRECT))),
            dma((2, len(PAIRED))),
            dma((2, len(PAIRED))),
            dma((2, 2)),
            dma((2, 1)),
            dma((2, 1)),
            dma((2, 1)),
            pltpu.SemaphoreType.REGULAR,
        ],
        compiler_params=pltpu.CompilerParams(
            collective_id=0, has_side_effects=True, vmem_limit_bytes=24 << 20
        ),
        name="subspace_step",
    )(*(pltpu.with_memory_space_constraint(a, pltpu.HBM) for a in (counts, occupancy, start_basis)))
    return basis_now.T * math.sqrt(genes * XL * CORE)


def solution(mesh):
    placed = (P("cells", "genes"), P("cells", "genes"), P(None, "genes"))
    return jax.shard_map(
        on_device, mesh=mesh, in_specs=placed, out_specs=P(None, ("genes", "cells")), check_vma=False
    )
```

```python
import math

import jax
import jax.numpy as jnp
from jax import lax
from jax.experimental import pallas as pl
from jax.experimental.pallas import tpu as pltpu
from jax.sharding import PartitionSpec as P

F32 = jnp.float32
BF16 = jnp.bfloat16
MESH = pl.DeviceIdType.MESH
Z, H, Y, XL, CORE = 16, 2, 4, 2, 2
LANES = 128
DIRECT = (8, 10)
PAIRED = (6, 4, 12, 2, 14, 0)
SCORE_ROW = 7
LEAD = 1
LOADS = (4, 12, 12, 4)
NT = (((1,), (1,)), ((), ()))


def device(z, h, y, xl, core):
    return ((z * H + h) * Y + y, xl * CORE + core)


def far_first(offsets, weights, sizes):
    def far(offset):
        return -sum(w * min(o, n - o) for o, w, n in zip(offset, weights, sizes))

    return sorted((o for o in offsets if any(o)), key=far)


def total_of(values):
    values = list(values)
    while len(values) > 1:
        values = [sum(values[i : i + 2][1:], values[i]) for i in range(0, len(values), 2)]
    return values[0]


def solve(gram, right):
    blocks = gram.shape[0] // 8
    left = [gram[8 * b : 8 * b + 8] for b in range(blocks)]
    right = [right[8 * b : 8 * b + 8] for b in range(blocks)]
    row_at = lax.broadcasted_iota(jnp.int32, (8, LANES), 0)
    done = []
    for kb in range(blocks):
        cols = [
            [
                jnp.broadcast_to(left[b][:, 8 * kb + j : 8 * kb + j + 1], (8, LANES))
                for j in range(8)
            ]
            for b in range(kb, blocks)
        ]
        rows_left, rows_right = left[kb], right[kb]
        scale = jnp.zeros((8, LANES), F32)
        steps = []
        for j in range(8):
            pivot = jnp.broadcast_to(cols[0][j][j : j + 1], (8, LANES))
            inv = lax.rsqrt(pivot)
            scale = jnp.where(row_at == j, inv, scale)
            lower = [c[j] * inv for c in cols]
            for m in range(j + 1, 8):
                entry = jnp.broadcast_to(lower[0][m : m + 1], (8, LANES))
                for c, low in zip(cols, lower):
                    c[m] = c[m] - low * entry
            below = jnp.where(row_at > j, lower[0], 0.0)
            unit_left = jnp.broadcast_to(rows_left[j : j + 1], rows_left.shape) * inv[:, : rows_left.shape[1]]
            unit_right = jnp.broadcast_to(rows_right[j : j + 1], rows_right.shape) * inv
            rows_left = rows_left - below[:, : rows_left.shape[1]] * unit_left
            rows_right = rows_right - below * unit_right
            steps.append((lower[1:], unit_left, unit_right))
        done.append(rows_right * scale)
        for at, b in enumerate(range(kb + 1, blocks)):
            for lower, unit_left, unit_right in steps:
                left[b] = left[b] - lower[at][:, : unit_left.shape[1]] * unit_left
                right[b] = right[b] - lower[at] * unit_right
    return jnp.concatenate(done, axis=0)


def kernel(
    counts_hbm,
    occupancy_hbm,
    basis_hbm,
    out,
    counts,
    occupancy,
    basis,
    cbuf,
    split_mean,
    mean_all,
    means_direct,
    means_direct_in,
    means_out,
    means_out_in,
    means_paired,
    means_paired_in,
    score,
    score_in,
    direct,
    direct_in,
    paired,
    paired_in,
    pair_out,
    pair_in,
    pair_dev,
    dev_mean,
    mean_xy,
    turned,
    zpart,
    zaux,
    zpart_in,
    zaux_in,
    gram,
    gram_in,
    gram_z,
    gram_z_in,
    gram_all,
    sem_in,
    sem_score,
    sem_means,
    sem_means_out,
    sem_means_paired,
    sem_direct,
    sem_pair,
    sem_paired,
    sem_z,
    sem_gram,
    sem_gram_z,
    sem_all,
    sem_beyond,
    sem_far,
):
    cells_at, genes_at = lax.axis_index("cells"), lax.axis_index("genes")
    z, h, y = cells_at // (H * Y), lax.rem(cells_at // Y, H), lax.rem(cells_at, Y)
    xl, core = genes_at // CORE, lax.rem(genes_at, CORE)
    comps = basis.shape[0]
    rows = comps // Y
    cells = counts.shape[0]
    width = LANES // Y
    plane = H * XL * CORE * Y

    loads = [pltpu.make_async_copy(occupancy_hbm, occupancy, sem_in.at[0])]
    tiles = [(sum(LOADS[:c]), sum(LOADS[: c + 1])) for c in range(len(LOADS))]
    spans = [pl.ds(first * LANES, (last - first) * LANES) for first, last in tiles]
    for c, span in enumerate(spans):
        loads.append(
            pltpu.make_async_copy(counts_hbm.at[:, span], counts.at[:, span], sem_in.at[c + 1])
        )
    loads.append(pltpu.make_async_copy(basis_hbm, basis, sem_in.at[len(LOADS) + 1]))
    for load in loads:
        load.start()

    def send(src, dst, sems, to, step=0):
        pltpu.make_async_remote_copy(
            src_ref=src,
            dst_ref=dst,
            send_sem=sems.at[0, step],
            recv_sem=sems.at[1, step],
            device_id=to if len(to) == 2 else device(*to),
            device_id_type=MESH,
        ).start()

    def waiting(all_bytes, sems, step):
        return pltpu.make_async_remote_copy(
            src_ref=all_bytes,
            dst_ref=all_bytes,
            send_sem=sems.at[0, step],
            recv_sem=sems.at[1, step],
            device_id=(cells_at, genes_at),
            device_id_type=MESH,
        )

    def wait_out(all_bytes, sems, step=0):
        waiting(all_bytes, sems, step).wait_send()

    def wait_in(all_bytes, sems, step=0):
        waiting(all_bytes, sems, step).wait_recv()

    def wait(all_bytes, sems, step=0):
        wait_out(all_bytes, sems, step)
        wait_in(all_bytes, sems, step)

    def gene_peer(a, b):
        return device(z, h, y, lax.rem(xl + a, XL), lax.rem(core + b, CORE))

    def z_peer(o):
        return device(lax.rem(z + o + Z, Z), h, y, xl, core)

    in_x = h * XL + xl
    chip = in_x * Y + y

    def chip_peer(a, c):
        xt, yt = lax.rem(in_x + a, H * XL), lax.rem(y + c, Y)
        return xt * Y + yt, (z, xt // XL, yt, lax.rem(xt, XL))

    def z_tile(o):
        return lax.rem(z + o + Z, Z)

    beside = [1 - 2 * lax.rem(z + ht, 2) for ht in range(H)]
    own_beside = 1 - 2 * lax.rem(z + h, 2)

    gene_offsets = [(1, 0), (1, 1), (0, 1)]
    xy_offsets = far_first([(a, b) for a in range(H) for b in range(Y)], (4, 2), (H, Y))
    xy_peers = []
    for a, b in xy_offsets:
        ht, yt = lax.rem(h + a, H), lax.rem(y + b, Y)
        xy_peers.append((ht, yt, device(z, ht, yt, xl, core)))
    chip_offsets = far_first([(a, c) for a in range(H * XL) for c in range(Y)], (1, 1), (H * XL, Y))
    z_offsets = far_first([(o,) for o in range(Z)], (1,), (Z,))

    barrier = pltpu.get_barrier_semaphore()
    beyond = [device(z, h, lax.rem(y + b, Y), xl, core) for b in range(1, Y)] + [z_peer(2), z_peer(-2)]
    peers = [gene_peer(a, b) for a, b in gene_offsets] + beyond
    peers += [device(z, 1 - h, y, xl, core), z_peer(1), z_peer(-1)]
    for peer in peers:
        pl.semaphore_signal(barrier, inc=1, device_id=peer, device_id_type=MESH)

    row_at = lax.broadcasted_iota(jnp.int32, (16, LANES), 0)
    group_at = lax.broadcasted_iota(jnp.int32, (16, LANES), 1) // width
    for ref in (means_direct, means_out, means_paired):
        ref[...] = jnp.zeros(ref.shape, F32)
    turned[...] = jnp.zeros((LANES, LANES), F32)

    def center(j):
        at = pl.ds(j * LANES, LANES)
        entries = counts[:, at].astype(F32)
        logged = jnp.log(1.0 + entries) * occupancy[0, j].astype(F32)
        mean = jnp.sum(logged, axis=0, keepdims=True) * (1.0 / cells)
        cbuf[:, at] = (logged - mean).astype(BF16)
        mean_all[j % H, j // H : j // H + 1, :] = mean

    def product_of(c):
        span = spans[c]
        return lax.dot_general(basis[:, span], cbuf[:, span], NT, preferred_element_type=F32)

    loads[0].wait()
    products = []
    for c in range(len(LOADS)):
        loads[c + 1].wait()
        if c == 1:
            loads[-1].wait()
        if c:
            products.append(product_of(c - 1))
        for j in range(*tiles[c]):
            center(j)
    products.append(product_of(len(LOADS) - 1))
    score[0:comps, :] = total_of(products)

    pl.semaphore_wait(barrier, len(peers))
    for peer in beyond:
        pl.semaphore_signal(sem_beyond, inc=1, device_id=peer, device_id_type=MESH)
    of_cells, of_means = pl.ds(0, comps), pl.ds(comps, 8)

    def send_scores(span, step):
        for s, (a, b) in enumerate(gene_offsets):
            send(score.at[span], score_in.at[s, span], sem_score, gene_peer(a, b), step)

    send_scores(of_cells, 0)
    for j in range(Z * H):
        mean = mean_all[j % H, j // H : j // H + 1, :]
        high = mean.astype(BF16).astype(F32)
        middle = (mean - high).astype(BF16).astype(F32)
        low = mean - high - middle
        stacked = jnp.where(
            row_at == 0, high, jnp.where(row_at == 1, middle, jnp.where(row_at == 2, low, 0.0))
        )
        split_mean[:, j * LANES : (j + 1) * LANES] = stacked.astype(BF16)
    of_mean = lax.dot_general(split_mean[...], basis[...], NT, preferred_element_type=F32)
    score[comps : comps + 8, :] = jnp.zeros((8, LANES), F32)
    score[comps : comps + 1, 0:comps] = of_mean[0:1] + of_mean[1:2] + of_mean[2:3]
    send_scores(of_means, 1)
    for ht in range(H):
        for i in range(2 * len(DIRECT)):
            at = z_tile(DIRECT[i // 2] + i % 2 * beside[ht])
            means_direct[ht, i : i + 1, :] = mean_all[ht, pl.ds(at, 1), :]
        for j, e in enumerate(PAIRED):
            means_out[ht, j : j + 1, :] = mean_all[ht, pl.ds(z_tile(e + beside[ht]), 1), :]
            means_paired[ht, j : j + 1, :] = mean_all[ht, pl.ds(z_tile(e), 1), :]
    pl.semaphore_wait(sem_beyond, len(beyond))
    for o in (4, -4):
        pl.semaphore_signal(sem_far, inc=1, device_id=z_peer(o), device_id_type=MESH)
    wait(score_in.at[:, of_cells], sem_score)
    scores = total_of([score[0:comps]] + [score_in[a, 0:comps] for a in range(XL * CORE - 1)])
    score_high = scores.astype(BF16)
    score_low = (scores - score_high.astype(F32)).astype(BF16)
    stacked = jnp.concatenate([score_high, score_low], axis=0)

    def pieces(tiles):
        columns = [
            cbuf[:, pl.ds(pl.multiple_of((tiles[ht] * H + ht) * LANES, LANES), LANES)] for ht in range(H)
        ]
        both = jnp.dot(stacked, jnp.concatenate(columns, axis=1), preferred_element_type=F32)
        product = both[:comps] + both[comps:]
        result = []
        for ht in range(H):
            turns = []
            for b in range(Y):
                block = product[b * rows : (b + 1) * rows, ht * LANES : (ht + 1) * LANES]
                turns.append([block] + [pltpu.roll(block, k * width, 1) for k in range(1, Y)])
            for yt in range(Y):
                piece = turns[0][(0 - yt) % Y]
                for b in range(1, Y):
                    piece = jnp.where(group_at == b, turns[b][(b - yt) % Y], piece)
                result.append((ht, yt, piece))
        return result

    def exchange(src, dst, sems, chunk, span):
        for s, (ht, yt, to) in enumerate(xy_peers):
            send(src.at[ht, yt, span], dst.at[span, s], sems, to, chunk)

    def start_direct(j):
        for i in (2 * j, 2 * j + 1):
            tiles = [z_tile(DIRECT[j] + i % 2 * beside[ht]) for ht in range(H)]
            for ht, yt, piece in pieces(tiles):
                direct[ht, yt, i] = piece
        exchange(direct, direct_in, sem_direct, j, pl.ds(2 * j, 2))

    def start_pair(j):
        for ht, yt, piece in pieces([z_tile(PAIRED[j] + beside[ht]) for ht in range(H)]):
            pair_out[ht, j, yt] = piece
        for ht in range(H):
            send(pair_out.at[ht, j], pair_in.at[ht, j], sem_pair, z_peer(beside[ht]), j)

    def send_means():
        wait(score_in.at[:, of_means], sem_score, 1)
        whole = total_of(
            [score[comps : comps + 1]]
            + [score_in[a, comps : comps + 1] for a in range(XL * CORE - 1)]
        )
        for ht in range(H):
            for ref in (means_direct, means_out, means_paired):
                ref[ht, SCORE_ROW : SCORE_ROW + 1, :] = whole
            send(means_out.at[ht], means_out_in.at[ht], sem_means_out, z_peer(beside[ht]))
        for s, (ht, _, to) in enumerate(xy_peers):
            send(means_direct.at[ht], means_direct_in.at[s], sem_means, to)

    start_pair(0)
    send_means()
    start_direct(0)
    start_pair(1)
    start_direct(1)
    for j in range(2, len(PAIRED)):
        start_pair(j)
    for j, e in enumerate(PAIRED):
        for ht, yt, piece in pieces([z_tile(e)] * H):
            paired[ht, yt, j] = piece

    def fold_rows(values):
        for p, value in enumerate(values):
            turned[p : p + 1, :] = value
        flat = turned[...].T
        result = []
        for p in range(len(values)):
            folded = jnp.broadcast_to(flat[0:rows, p : p + 1], (rows, LANES))
            for b in range(1, Y):
                block = jnp.broadcast_to(flat[b * rows : (b + 1) * rows, p : p + 1], (rows, LANES))
                folded = jnp.where(group_at == b, block, folded)
            result.append(folded)
        return result

    def columns_of(means, yt):
        kept = jnp.where(group_at[0:8] == yt, means, 0.0)
        return total_of([kept] + [pltpu.roll(kept, k * width, 1) for k in range(1, Y)])

    groups = len(xy_offsets) + 1

    def plane_terms(level, weight, own, others):
        values = [own[h]] + [others[s] for s in range(groups - 1)]
        middle = total_of(values) * (1.0 / groups)
        apart = [value - middle for value in values]
        away = fold_rows([a[SCORE_ROW : SCORE_ROW + 1] * weight for a in apart])
        mean_xy[level] = columns_of(middle, y)
        for p, value in enumerate(apart):
            dev_mean[level, p] = columns_of(value, y)
        return middle[SCORE_ROW : SCORE_ROW + 1], away

    wait(means_out_in, sem_means_out)
    apart = [means_paired[ht] - means_out_in[ht] for ht in range(H)]
    pair_away = fold_rows([a[SCORE_ROW : SCORE_ROW + 1] * (0.5 * cells) for a in apart])
    for ht in range(H):
        means_paired[ht] = 0.5 * (means_paired[ht] + means_out_in[ht])
        for yt in range(Y):
            pair_dev[ht, yt] = columns_of(apart[ht], yt)
    for s, (ht, _, to) in enumerate(xy_peers):
        send(means_paired.at[ht], means_paired_in.at[s], sem_means_paired, to)

    def add_pair(j):
        wait(pair_in.at[:, j], sem_pair, j)
        for ht in range(H):
            for yt in range(Y):
                paired[ht, yt, j] = (paired[ht, yt, j] + pair_in[ht, j, yt]) + pair_away[
                    ht
                ] * pair_dev[ht, yt, j : j + 1, :]
        exchange(paired, paired_in, sem_paired, j, pl.ds(j, 1))

    def plane_sum(level, slot, own, others, i, away, middle, to):
        terms = [own[h, y, i]] + [others[i, s] for s in range(groups - 1)]
        terms += [away[p] * dev_mean[level, p, i : i + 1, :] for p in range(groups)]
        zpart[slot] = total_of(terms)
        zaux[slot, 0:1, :] = mean_xy[level, i : i + 1, :]
        zaux[slot, 1:2, :] = middle
        if to is not None:
            send(zpart.at[slot], zpart_in.at[slot], sem_z, to)
            send(zaux.at[slot], zaux_in.at[slot], sem_z, to, 1)

    def sum_direct(j):
        wait(direct_in.at[pl.ds(2 * j, 2)], sem_direct, j)
        for i in (2 * j, 2 * j + 1):
            to = z_peer(DIRECT[j] + i % 2 * own_beside)
            plane_sum(0, i, direct, direct_in, i, away_direct, score_direct, to)

    for j in range(len(PAIRED) - 1):
        add_pair(j)
    wait(means_direct_in, sem_means)
    score_direct, away_direct = plane_terms(0, float(cells), means_direct, means_direct_in)
    pl.semaphore_wait(sem_far, 2)
    sum_direct(0)
    add_pair(len(PAIRED) - 1)
    sum_direct(1)
    wait(means_paired_in, sem_means_paired)
    score_paired, away_paired = plane_terms(1, 2.0 * cells, means_paired, means_paired_in)
    alone = 2 * len(DIRECT)
    for j, e in enumerate(PAIRED):
        wait(paired_in.at[pl.ds(j, 1)], sem_paired, j)
        to = z_peer(e) if e else None
        plane_sum(1, alone + j, paired, paired_in, j, away_paired, score_paired, to)
    wait(zpart_in, sem_z)
    wait(zaux_in, sem_z, 1)
    last = alone + len(PAIRED) - 1
    shares = [1.0] * alone + [2.0] * len(PAIRED)
    means = [zaux_in[i, 0:1, :] for i in range(last)] + [zaux[last, 0:1, :]]
    scores_of = [zaux_in[i, 1:2, :] for i in range(last)] + [zaux[last, 1:2, :]]
    middle = total_of([v * w for v, w in zip(scores_of, shares)]) * (1.0 / Z)
    away = fold_rows([(v - middle) * (w * cells * groups) for v, w in zip(scores_of, shares)])
    middle = total_of([v * w for v, w in zip(means, shares)]) * (1.0 / Z)
    terms = [zpart[last]] + [zpart_in[i] for i in range(last)]
    terms += [far * (value - middle) for far, value in zip(away, means)]
    folded = total_of(terms)

    blocks = [folded] + [pltpu.roll(folded, (Y - b) * width, 1) for b in range(1, Y)]
    spread = jnp.concatenate([jnp.where(group_at == 0, block, 0.0) for block in blocks], axis=0)
    own_gram = lax.dot_general(
        spread, spread, NT, precision=lax.Precision.HIGHEST, preferred_element_type=F32
    )
    packed = jnp.concatenate([own_gram[0 : comps // 2], own_gram[comps // 2 :]], axis=1)
    chips = plane // CORE
    for e in range(chips):
        gram[e] = packed[2 * e : 2 * e + 2]
    leads = core == LEAD
    for s, offset in enumerate(chip_offsets):
        at, to = chip_peer(*offset)
        send(gram.at[at], gram_in.at[s + (CORE - 1 - core) * (chips - 1)], sem_gram, (*to, LEAD))

    @pl.when(jnp.logical_not(leads))
    def _():
        send(gram.at[chip], gram_in.at[plane - 2], sem_gram, (*chip_peer(0, 0)[1], LEAD))
        wait_out(gram, sem_gram)

    @pl.when(leads)
    def _():
        wait_out(gram.at[pl.ds(0, chips - 1)], sem_gram)
        wait_in(gram_in, sem_gram)
        gram_z[...] = jnp.sum(gram_in[...], axis=0) + gram[chip]
        for s, (o,) in enumerate(z_offsets):
            send(gram_z, gram_z_in.at[s], sem_gram_z, z_peer(o))
        wait(gram_z_in, sem_gram_z)
        gram_all[chip] = jnp.sum(gram_z_in[...], axis=0) + gram_z[...]
        for offset in chip_offsets:
            for other in range(CORE):
                send(gram_all.at[chip], gram_all.at[chip], sem_all, (*chip_peer(*offset)[1], other))
        send(gram_all.at[chip], gram_all.at[chip], sem_all, (*chip_peer(0, 0)[1], 1 - LEAD))
        wait_out(gram_in, sem_all)
        wait_in(gram_all.at[pl.ds(0, chips - 1)], sem_all)

    @pl.when(jnp.logical_not(leads))
    def _():
        wait_in(gram_all, sem_all)

    packed = gram_all[...].reshape(comps // 2, LANES)
    gram_sum = jnp.concatenate([packed[:, 0:comps], packed[:, comps : 2 * comps]], axis=0)
    out[...] = solve(gram_sum, spread).T[0:width]


def on_device(counts, occupancy, start_basis):
    comps, genes = start_basis.shape
    cells = counts.shape[0]
    rows = comps // Y
    plane = H * XL * CORE * Y
    tiles = 2 * len(DIRECT) + len(PAIRED)
    dma = pltpu.SemaphoreType.DMA
    hbm = pl.BlockSpec(memory_space=pltpu.HBM)
    basis_now = pl.pallas_call(
        kernel,
        out_shape=jax.ShapeDtypeStruct((LANES // Y, comps), F32),
        in_specs=[hbm, hbm, hbm],
        out_specs=pl.BlockSpec(memory_space=pltpu.VMEM),
        scratch_shapes=[
            pltpu.VMEM((cells, genes), BF16),
            pltpu.SMEM(occupancy.shape, jnp.int32),
            pltpu.VMEM((comps, genes), BF16),
            pltpu.VMEM((cells, genes), BF16),
            pltpu.VMEM((16, genes), BF16),
            pltpu.VMEM((H, Z, LANES), F32),
            pltpu.VMEM((H, 8, LANES), F32),
            pltpu.VMEM((H * Y - 1, 8, LANES), F32),
            pltpu.VMEM((H, 8, LANES), F32),
            pltpu.VMEM((H, 8, LANES), F32),
            pltpu.VMEM((H, 8, LANES), F32),
            pltpu.VMEM((H * Y - 1, 8, LANES), F32),
            pltpu.VMEM((comps + 8, LANES), F32),
            pltpu.VMEM((XL * CORE - 1, comps + 8, LANES), F32),
            pltpu.VMEM((H, Y, 2 * len(DIRECT), rows, LANES), F32),
            pltpu.VMEM((2 * len(DIRECT), H * Y - 1, rows, LANES), F32),
            pltpu.VMEM((H, Y, len(PAIRED), rows, LANES), F32),
            pltpu.VMEM((len(PAIRED), H * Y - 1, rows, LANES), F32),
            pltpu.VMEM((H, len(PAIRED), Y, rows, LANES), F32),
            pltpu.VMEM((H, len(PAIRED), Y, rows, LANES), F32),
            pltpu.VMEM((H, Y, 8, LANES), F32),
            pltpu.VMEM((2, H * Y, 8, LANES), F32),
            pltpu.VMEM((2, 8, LANES), F32),
            pltpu.VMEM((LANES, LANES), F32),
            pltpu.VMEM((tiles, rows, LANES), F32),
            pltpu.VMEM((tiles, 2, LANES), F32),
            pltpu.VMEM((tiles - 1, rows, LANES), F32),
            pltpu.VMEM((tiles - 1, 2, LANES), F32),
            pltpu.VMEM((plane // CORE, 2, LANES), F32),
            pltpu.VMEM((plane - 1, 2, LANES), F32),
            pltpu.VMEM((2, LANES), F32),
            pltpu.VMEM((Z - 1, 2, LANES), F32),
            pltpu.VMEM((plane // CORE, 2, LANES), F32),
            dma((len(LOADS) + 2,)),
            dma((2, 2)),
            dma((2, 1)),
            dma((2, 1)),
            dma((2, 1)),
            dma((2, len(DIRECT))),
            dma((2, len(PAIRED))),
            dma((2, len(PAIRED))),
            dma((2, 2)),
            dma((2, 1)),
            dma((2, 1)),
            dma((2, 1)),
            pltpu.SemaphoreType.REGULAR,
            pltpu.SemaphoreType.REGULAR,
        ],
        compiler_params=pltpu.CompilerParams(
            collective_id=0, has_side_effects=True, vmem_limit_bytes=24 << 20
        ),
        name="subspace_step",
    )(*(pltpu.with_memory_space_constraint(a, pltpu.HBM) for a in (counts, occupancy, start_basis)))
    return basis_now.T * math.sqrt(genes * XL * CORE)


def solution(mesh):
    placed = (P("cells", "genes"), P("cells", "genes"), P(None, "genes"))
    return jax.shard_map(
        on_device, mesh=mesh, in_specs=placed, out_specs=P(None, ("genes", "cells")), check_vma=False
    )
```

```python
import math

import jax
import jax.numpy as jnp
from jax import lax
from jax.experimental import pallas as pl
from jax.experimental.pallas import tpu as pltpu
from jax.sharding import PartitionSpec as P

F32 = jnp.float32
BF16 = jnp.bfloat16
MESH = pl.DeviceIdType.MESH
Z, H, Y, XL, CORE = 16, 2, 4, 2, 2
LANES = 128
DIRECT = (8, 10)
PAIRED = (6, 4, 12, 2, 14, 0)
SCORE_ROW = 7
LEAD = 1
LOADS = (4, 12, 12, 4)
NT = (((1,), (1,)), ((), ()))


def device(z, h, y, xl, core):
    return ((z * H + h) * Y + y, xl * CORE + core)


def far_first(offsets, weights, sizes):
    def far(offset):
        return -sum(w * min(o, n - o) for o, w, n in zip(offset, weights, sizes))

    return sorted((o for o in offsets if any(o)), key=far)


def total_of(values):
    values = list(values)
    while len(values) > 1:
        values = [sum(values[i : i + 2][1:], values[i]) for i in range(0, len(values), 2)]
    return values[0]


def solve(gram, right):
    blocks = gram.shape[0] // 8
    left = [gram[8 * b : 8 * b + 8] for b in range(blocks)]
    right = [right[8 * b : 8 * b + 8] for b in range(blocks)]
    row_at = lax.broadcasted_iota(jnp.int32, (8, LANES), 0)
    done = []
    for kb in range(blocks):
        cols = [
            [
                jnp.broadcast_to(left[b][:, 8 * kb + j : 8 * kb + j + 1], (8, LANES))
                for j in range(8)
            ]
            for b in range(kb, blocks)
        ]
        rows_left, rows_right = left[kb], right[kb]
        scale = jnp.zeros((8, LANES), F32)
        steps = []
        for j in range(8):
            pivot = jnp.broadcast_to(cols[0][j][j : j + 1], (8, LANES))
            inv = lax.rsqrt(pivot)
            scale = jnp.where(row_at == j, inv, scale)
            lower = [c[j] * inv for c in cols]
            for m in range(j + 1, 8):
                entry = jnp.broadcast_to(lower[0][m : m + 1], (8, LANES))
                for c, low in zip(cols, lower):
                    c[m] = c[m] - low * entry
            below = jnp.where(row_at > j, lower[0], 0.0)
            unit_left = jnp.broadcast_to(rows_left[j : j + 1], rows_left.shape) * inv[:, : rows_left.shape[1]]
            unit_right = jnp.broadcast_to(rows_right[j : j + 1], rows_right.shape) * inv
            rows_left = rows_left - below[:, : rows_left.shape[1]] * unit_left
            rows_right = rows_right - below * unit_right
            steps.append((lower[1:], unit_left, unit_right))
        done.append(rows_right * scale)
        for at, b in enumerate(range(kb + 1, blocks)):
            for lower, unit_left, unit_right in steps:
                left[b] = left[b] - lower[at][:, : unit_left.shape[1]] * unit_left
                right[b] = right[b] - lower[at] * unit_right
    return jnp.concatenate(done, axis=0)


def kernel(
    counts_hbm,
    occupancy_hbm,
    basis_hbm,
    out,
    counts,
    occupancy,
    basis,
    cbuf,
    split_mean,
    mean_all,
    means_direct,
    means_direct_in,
    means_out,
    means_out_in,
    means_paired,
    means_paired_in,
    score,
    score_in,
    direct,
    direct_in,
    paired,
    paired_in,
    pair_out,
    pair_in,
    pair_dev,
    dev_mean,
    mean_xy,
    turned,
    zpart,
    zaux,
    zpart_in,
    zaux_in,
    tile,
    spread,
    gram,
    gram_in,
    gram_z,
    gram_z_in,
    gram_all,
    sem_in,
    sem_score,
    sem_means,
    sem_means_out,
    sem_means_paired,
    sem_direct,
    sem_pair,
    sem_paired,
    sem_z,
    sem_tile,
    sem_gram,
    sem_gram_z,
    sem_all,
    sem_beyond,
    sem_far,
):
    cells_at, genes_at = lax.axis_index("cells"), lax.axis_index("genes")
    z, h, y = cells_at // (H * Y), lax.rem(cells_at // Y, H), lax.rem(cells_at, Y)
    xl, core = genes_at // CORE, lax.rem(genes_at, CORE)
    comps = basis.shape[0]
    rows = comps // Y
    cells = counts.shape[0]
    width = LANES // Y
    plane = H * XL * CORE * Y

    loads = [pltpu.make_async_copy(occupancy_hbm, occupancy, sem_in.at[0])]
    tiles = [(sum(LOADS[:c]), sum(LOADS[: c + 1])) for c in range(len(LOADS))]
    spans = [pl.ds(first * LANES, (last - first) * LANES) for first, last in tiles]
    for c, span in enumerate(spans):
        loads.append(
            pltpu.make_async_copy(counts_hbm.at[:, span], counts.at[:, span], sem_in.at[c + 1])
        )
    loads.append(pltpu.make_async_copy(basis_hbm, basis, sem_in.at[len(LOADS) + 1]))
    for load in loads:
        load.start()

    def send(src, dst, sems, to, step=0):
        pltpu.make_async_remote_copy(
            src_ref=src,
            dst_ref=dst,
            send_sem=sems.at[0, step],
            recv_sem=sems.at[1, step],
            device_id=to if len(to) == 2 else device(*to),
            device_id_type=MESH,
        ).start()

    def waiting(all_bytes, sems, step):
        return pltpu.make_async_remote_copy(
            src_ref=all_bytes,
            dst_ref=all_bytes,
            send_sem=sems.at[0, step],
            recv_sem=sems.at[1, step],
            device_id=(cells_at, genes_at),
            device_id_type=MESH,
        )

    def wait_out(all_bytes, sems, step=0):
        waiting(all_bytes, sems, step).wait_send()

    def wait_in(all_bytes, sems, step=0):
        waiting(all_bytes, sems, step).wait_recv()

    def wait(all_bytes, sems, step=0):
        wait_out(all_bytes, sems, step)
        wait_in(all_bytes, sems, step)

    def gene_peer(a, b):
        return device(z, h, y, lax.rem(xl + a, XL), lax.rem(core + b, CORE))

    def z_peer(o):
        return device(lax.rem(z + o + Z, Z), h, y, xl, core)

    in_x = h * XL + xl
    chip = in_x * Y + y

    def chip_peer(a, c):
        xt, yt = lax.rem(in_x + a, H * XL), lax.rem(y + c, Y)
        return xt * Y + yt, (z, xt // XL, yt, lax.rem(xt, XL))

    def z_tile(o):
        return lax.rem(z + o + Z, Z)

    beside = [1 - 2 * lax.rem(z + ht, 2) for ht in range(H)]
    own_beside = 1 - 2 * lax.rem(z + h, 2)

    gene_offsets = [(1, 0), (1, 1), (0, 1)]
    xy_offsets = far_first([(a, b) for a in range(H) for b in range(Y)], (4, 2), (H, Y))
    xy_peers = []
    for a, b in xy_offsets:
        ht, yt = lax.rem(h + a, H), lax.rem(y + b, Y)
        xy_peers.append((ht, yt, device(z, ht, yt, xl, core)))
    chip_offsets = far_first([(a, c) for a in range(H * XL) for c in range(Y)], (1, 1), (H * XL, Y))
    z_offsets = far_first([(o,) for o in range(Z)], (1,), (Z,))

    barrier = pltpu.get_barrier_semaphore()
    beyond = [device(z, h, lax.rem(y + b, Y), xl, core) for b in range(1, Y)] + [z_peer(2), z_peer(-2)]
    peers = [gene_peer(a, b) for a, b in gene_offsets] + beyond
    peers += [device(z, 1 - h, y, xl, core), z_peer(1), z_peer(-1)]
    peers += [device(z_tile(o), h, y, xl, 1 - core) for o in (1, -1, 2, -2)]
    for peer in peers:
        pl.semaphore_signal(barrier, inc=1, device_id=peer, device_id_type=MESH)

    row_at = lax.broadcasted_iota(jnp.int32, (16, LANES), 0)
    group_at = lax.broadcasted_iota(jnp.int32, (16, LANES), 1) // width
    for ref in (means_direct, means_out, means_paired):
        ref[...] = jnp.zeros(ref.shape, F32)
    turned[...] = jnp.zeros((LANES, LANES), F32)

    def center(j):
        at = pl.ds(j * LANES, LANES)
        entries = counts[:, at].astype(F32)
        logged = jnp.log(1.0 + entries) * occupancy[0, j].astype(F32)
        mean = jnp.sum(logged, axis=0, keepdims=True) * (1.0 / cells)
        cbuf[:, at] = (logged - mean).astype(BF16)
        mean_all[j % H, j // H : j // H + 1, :] = mean

    def product_of(c):
        span = spans[c]
        return lax.dot_general(basis[:, span], cbuf[:, span], NT, preferred_element_type=F32)

    loads[0].wait()
    products = []
    for c in range(len(LOADS)):
        loads[c + 1].wait()
        if c == 1:
            loads[-1].wait()
        if c:
            products.append(product_of(c - 1))
        for j in range(*tiles[c]):
            center(j)
    products.append(product_of(len(LOADS) - 1))
    score[0:comps, :] = total_of(products)

    pl.semaphore_wait(barrier, len(peers))
    for peer in beyond:
        pl.semaphore_signal(sem_beyond, inc=1, device_id=peer, device_id_type=MESH)
    of_cells, of_means = pl.ds(0, comps), pl.ds(comps, 8)

    def send_scores(span, step):
        for s, (a, b) in enumerate(gene_offsets):
            send(score.at[span], score_in.at[s, span], sem_score, gene_peer(a, b), step)

    send_scores(of_cells, 0)
    for j in range(Z * H):
        mean = mean_all[j % H, j // H : j // H + 1, :]
        high = mean.astype(BF16).astype(F32)
        middle = (mean - high).astype(BF16).astype(F32)
        low = mean - high - middle
        stacked = jnp.where(
            row_at == 0, high, jnp.where(row_at == 1, middle, jnp.where(row_at == 2, low, 0.0))
        )
        split_mean[:, j * LANES : (j + 1) * LANES] = stacked.astype(BF16)
    of_mean = lax.dot_general(split_mean[...], basis[...], NT, preferred_element_type=F32)
    score[comps : comps + 8, :] = jnp.zeros((8, LANES), F32)
    score[comps : comps + 1, 0:comps] = of_mean[0:1] + of_mean[1:2] + of_mean[2:3]
    send_scores(of_means, 1)
    for ht in range(H):
        for i in range(2 * len(DIRECT)):
            at = z_tile(DIRECT[i // 2] + i % 2 * beside[ht])
            means_direct[ht, i : i + 1, :] = mean_all[ht, pl.ds(at, 1), :]
        for j, e in enumerate(PAIRED):
            means_out[ht, j : j + 1, :] = mean_all[ht, pl.ds(z_tile(e + beside[ht]), 1), :]
            means_paired[ht, j : j + 1, :] = mean_all[ht, pl.ds(z_tile(e), 1), :]
    pl.semaphore_wait(sem_beyond, len(beyond))
    for o in (4, -4):
        pl.semaphore_signal(sem_far, inc=1, device_id=z_peer(o), device_id_type=MESH)
    wait(score_in.at[:, of_cells], sem_score)
    scores = total_of([score[0:comps]] + [score_in[a, 0:comps] for a in range(XL * CORE - 1)])
    score_high = scores.astype(BF16)
    score_low = (scores - score_high.astype(F32)).astype(BF16)
    stacked = jnp.concatenate([score_high, score_low], axis=0)

    def pieces(tiles):
        columns = [
            cbuf[:, pl.ds(pl.multiple_of((tiles[ht] * H + ht) * LANES, LANES), LANES)] for ht in range(H)
        ]
        both = jnp.dot(stacked, jnp.concatenate(columns, axis=1), preferred_element_type=F32)
        product = both[:comps] + both[comps:]
        result = []
        for ht in range(H):
            turns = []
            for b in range(Y):
                block = product[b * rows : (b + 1) * rows, ht * LANES : (ht + 1) * LANES]
                turns.append([block] + [pltpu.roll(block, k * width, 1) for k in range(1, Y)])
            for yt in range(Y):
                piece = turns[0][(0 - yt) % Y]
                for b in range(1, Y):
                    piece = jnp.where(group_at == b, turns[b][(b - yt) % Y], piece)
                result.append((ht, yt, piece))
        return result

    def exchange(src, dst, sems, chunk, span):
        for s, (ht, yt, to) in enumerate(xy_peers):
            send(src.at[ht, yt, span], dst.at[span, s], sems, to, chunk)

    def start_direct(j):
        for i in (2 * j, 2 * j + 1):
            tiles = [z_tile(DIRECT[j] + i % 2 * beside[ht]) for ht in range(H)]
            for ht, yt, piece in pieces(tiles):
                direct[ht, yt, i] = piece
        exchange(direct, direct_in, sem_direct, j, pl.ds(2 * j, 2))

    def start_pair(j):
        for ht, yt, piece in pieces([z_tile(PAIRED[j] + beside[ht]) for ht in range(H)]):
            pair_out[ht, j, yt] = piece
        for ht in range(H):
            send(pair_out.at[ht, j], pair_in.at[ht, j], sem_pair, z_peer(beside[ht]), j)

    def send_means():
        wait(score_in.at[:, of_means], sem_score, 1)
        whole = total_of(
            [score[comps : comps + 1]]
            + [score_in[a, comps : comps + 1] for a in range(XL * CORE - 1)]
        )
        for ht in range(H):
            for ref in (means_direct, means_out, means_paired):
                ref[ht, SCORE_ROW : SCORE_ROW + 1, :] = whole
            send(means_out.at[ht], means_out_in.at[ht], sem_means_out, z_peer(beside[ht]))
        for s, (ht, _, to) in enumerate(xy_peers):
            send(means_direct.at[ht], means_direct_in.at[s], sem_means, to)

    start_pair(0)
    send_means()
    start_direct(0)
    start_pair(1)
    start_direct(1)
    for j in range(2, len(PAIRED)):
        start_pair(j)
    for j, e in enumerate(PAIRED):
        for ht, yt, piece in pieces([z_tile(e)] * H):
            paired[ht, yt, j] = piece

    def fold_rows(values):
        for p, value in enumerate(values):
            turned[p : p + 1, :] = value
        flat = turned[...].T
        result = []
        for p in range(len(values)):
            folded = jnp.broadcast_to(flat[0:rows, p : p + 1], (rows, LANES))
            for b in range(1, Y):
                block = jnp.broadcast_to(flat[b * rows : (b + 1) * rows, p : p + 1], (rows, LANES))
                folded = jnp.where(group_at == b, block, folded)
            result.append(folded)
        return result

    def columns_of(means, yt):
        kept = jnp.where(group_at[0:8] == yt, means, 0.0)
        return total_of([kept] + [pltpu.roll(kept, k * width, 1) for k in range(1, Y)])

    groups = len(xy_offsets) + 1

    def plane_terms(level, weight, own, others):
        values = [own[h]] + [others[s] for s in range(groups - 1)]
        middle = total_of(values) * (1.0 / groups)
        apart = [value - middle for value in values]
        away = fold_rows([a[SCORE_ROW : SCORE_ROW + 1] * weight for a in apart])
        mean_xy[level] = columns_of(middle, y)
        for p, value in enumerate(apart):
            dev_mean[level, p] = columns_of(value, y)
        return middle[SCORE_ROW : SCORE_ROW + 1], away

    wait(means_out_in, sem_means_out)
    apart = [means_paired[ht] - means_out_in[ht] for ht in range(H)]
    pair_away = fold_rows([a[SCORE_ROW : SCORE_ROW + 1] * (0.5 * cells) for a in apart])
    for ht in range(H):
        means_paired[ht] = 0.5 * (means_paired[ht] + means_out_in[ht])
        for yt in range(Y):
            pair_dev[ht, yt] = columns_of(apart[ht], yt)
    for s, (ht, _, to) in enumerate(xy_peers):
        send(means_paired.at[ht], means_paired_in.at[s], sem_means_paired, to)

    def add_pair(j):
        wait(pair_in.at[:, j], sem_pair, j)
        for ht in range(H):
            for yt in range(Y):
                paired[ht, yt, j] = (paired[ht, yt, j] + pair_in[ht, j, yt]) + pair_away[
                    ht
                ] * pair_dev[ht, yt, j : j + 1, :]
        exchange(paired, paired_in, sem_paired, j, pl.ds(j, 1))

    leads = core == LEAD
    last = 2 * len(DIRECT) + len(PAIRED) - 1
    after_leads = (CORE - 1 - core) * last

    def lead_peer(o):
        return device(z_tile(o), h, y, xl, LEAD)

    def plane_sum(level, slot, own, others, i, away, middle, to):
        terms = [own[h, y, i]] + [others[i, s] for s in range(groups - 1)]
        terms += [away[p] * dev_mean[level, p, i : i + 1, :] for p in range(groups)]
        zpart[slot] = total_of(terms)
        zaux[slot, 0:1, :] = mean_xy[level, i : i + 1, :]
        zaux[slot, 1:2, :] = middle
        def send_sum():
            send(zpart.at[slot], zpart_in.at[slot + after_leads], sem_z, to)
            send(zaux.at[slot], zaux_in.at[slot + after_leads], sem_z, to, 1)

        if slot < last:
            send_sum()
        else:
            pl.when(jnp.logical_not(leads))(send_sum)

    def sum_direct(j):
        wait(direct_in.at[pl.ds(2 * j, 2)], sem_direct, j)
        for i in (2 * j, 2 * j + 1):
            to = lead_peer(DIRECT[j] + i % 2 * own_beside)
            plane_sum(0, i, direct, direct_in, i, away_direct, score_direct, to)

    for j in range(len(PAIRED) - 1):
        add_pair(j)
    wait(means_direct_in, sem_means)
    score_direct, away_direct = plane_terms(0, float(cells), means_direct, means_direct_in)
    pl.semaphore_wait(sem_far, 2)
    sum_direct(0)
    add_pair(len(PAIRED) - 1)
    sum_direct(1)
    wait(means_paired_in, sem_means_paired)
    score_paired, away_paired = plane_terms(1, 2.0 * cells, means_paired, means_paired_in)
    alone = 2 * len(DIRECT)
    for j, e in enumerate(PAIRED):
        wait(paired_in.at[pl.ds(j, 1)], sem_paired, j)
        plane_sum(1, alone + j, paired, paired_in, j, away_paired, score_paired, lead_peer(e))
    def columns(folded, group):
        turns = [pltpu.roll(folded, (Y - b + group) % Y * width, 1) if b != group else folded for b in range(Y)]
        return [jnp.where(group_at == group, turn, 0.0) for turn in turns]

    chips = plane // CORE

    @pl.when(leads)
    def _():
        wait_out(zpart.at[pl.ds(0, last)], sem_z)
        wait_out(zaux.at[pl.ds(0, last)], sem_z, 1)
        wait_in(zpart_in, sem_z)
        wait_in(zaux_in, sem_z, 1)
        shares = [1.0] * alone + [2.0] * len(PAIRED)
        scores_of = [zaux_in[i, 1:2, :] for i in range(last)] + [zaux[last, 1:2, :]]
        middle = total_of([v * w for v, w in zip(scores_of, shares)]) * (1.0 / Z)
        away = fold_rows([(v - middle) * (w * cells * groups) for v, w in zip(scores_of, shares)])
        own = [zpart_in[i] for i in range(last)] + [zpart[last]]
        own_means = [zaux_in[i, 0:1, :] for i in range(last)] + [zaux[last, 0:1, :]]
        others = [zpart_in[i] for i in range(last, 2 * last + 1)]
        other_means = [zaux_in[i, 0:1, :] for i in range(last, 2 * last + 1)]
        for t, (sums, means) in enumerate(((own, own_means), (others, other_means))):
            middle = total_of([v * w for v, w in zip(means, shares)]) * (1.0 / Z)
            tile[t] = total_of(sums + [far * (v - middle) for far, v in zip(away, means)])
        send(tile.at[1], tile.at[0], sem_tile, (z, h, y, xl, 1 - LEAD))
        both = [a + b for a, b in zip(columns(tile[0], 0), columns(tile[1], 1))]
        spread[...] = jnp.concatenate(both, axis=0)
        own_gram = lax.dot_general(
            spread[...], spread[...], NT, precision=lax.Precision.HIGHEST, preferred_element_type=F32
        )
        packed = jnp.concatenate([own_gram[0 : comps // 2], own_gram[comps // 2 :]], axis=1)
        for e in range(chips):
            gram[e] = packed[2 * e : 2 * e + 2]
        for s, offset in enumerate(chip_offsets):
            at, to = chip_peer(*offset)
            send(gram.at[at], gram_in.at[s], sem_gram, (*to, LEAD))
        wait_out(gram.at[pl.ds(0, chips - 1)], sem_gram)
        wait_in(gram_in.at[pl.ds(0, chips - 1)], sem_gram)
        gram_z[...] = jnp.sum(gram_in[0 : chips - 1], axis=0) + gram[chip]
        for s, (o,) in enumerate(z_offsets):
            send(gram_z, gram_z_in.at[s], sem_gram_z, z_peer(o))
        wait(gram_z_in, sem_gram_z)
        gram_all[chip] = jnp.sum(gram_z_in[...], axis=0) + gram_z[...]
        for offset in chip_offsets:
            for other in range(CORE):
                send(gram_all.at[chip], gram_all.at[chip], sem_all, (*chip_peer(*offset)[1], other))
        send(gram_all.at[chip], gram_all.at[chip], sem_all, (*chip_peer(0, 0)[1], 1 - LEAD))
        wait_out(tile.at[1], sem_tile)
        wait_out(gram_in, sem_all)
        wait_in(gram_all.at[pl.ds(0, chips - 1)], sem_all)

    @pl.when(jnp.logical_not(leads))
    def _():
        wait_out(zpart, sem_z)
        wait_out(zaux, sem_z, 1)
        wait_in(tile.at[0], sem_tile)
        spread[...] = jnp.concatenate(columns(tile[0], 0), axis=0)
        wait_in(gram_all, sem_all)

    packed = gram_all[...].reshape(comps // 2, LANES)
    gram_sum = jnp.concatenate([packed[:, 0:comps], packed[:, comps : 2 * comps]], axis=0)
    out[...] = solve(gram_sum, spread[...]).T[0:width]


def on_device(counts, occupancy, start_basis):
    comps, genes = start_basis.shape
    cells = counts.shape[0]
    rows = comps // Y
    plane = H * XL * CORE * Y
    tiles = 2 * len(DIRECT) + len(PAIRED)
    dma = pltpu.SemaphoreType.DMA
    hbm = pl.BlockSpec(memory_space=pltpu.HBM)
    basis_now = pl.pallas_call(
        kernel,
        out_shape=jax.ShapeDtypeStruct((LANES // Y, comps), F32),
        in_specs=[hbm, hbm, hbm],
        out_specs=pl.BlockSpec(memory_space=pltpu.VMEM),
        scratch_shapes=[
            pltpu.VMEM((cells, genes), BF16),
            pltpu.SMEM(occupancy.shape, jnp.int32),
            pltpu.VMEM((comps, genes), BF16),
            pltpu.VMEM((cells, genes), BF16),
            pltpu.VMEM((16, genes), BF16),
            pltpu.VMEM((H, Z, LANES), F32),
            pltpu.VMEM((H, 8, LANES), F32),
            pltpu.VMEM((H * Y - 1, 8, LANES), F32),
            pltpu.VMEM((H, 8, LANES), F32),
            pltpu.VMEM((H, 8, LANES), F32),
            pltpu.VMEM((H, 8, LANES), F32),
            pltpu.VMEM((H * Y - 1, 8, LANES), F32),
            pltpu.VMEM((comps + 8, LANES), F32),
            pltpu.VMEM((XL * CORE - 1, comps + 8, LANES), F32),
            pltpu.VMEM((H, Y, 2 * len(DIRECT), rows, LANES), F32),
            pltpu.VMEM((2 * len(DIRECT), H * Y - 1, rows, LANES), F32),
            pltpu.VMEM((H, Y, len(PAIRED), rows, LANES), F32),
            pltpu.VMEM((len(PAIRED), H * Y - 1, rows, LANES), F32),
            pltpu.VMEM((H, len(PAIRED), Y, rows, LANES), F32),
            pltpu.VMEM((H, len(PAIRED), Y, rows, LANES), F32),
            pltpu.VMEM((H, Y, 8, LANES), F32),
            pltpu.VMEM((2, H * Y, 8, LANES), F32),
            pltpu.VMEM((2, 8, LANES), F32),
            pltpu.VMEM((LANES, LANES), F32),
            pltpu.VMEM((tiles, rows, LANES), F32),
            pltpu.VMEM((tiles, 2, LANES), F32),
            pltpu.VMEM((CORE * tiles - 1, rows, LANES), F32),
            pltpu.VMEM((CORE * tiles - 1, 2, LANES), F32),
            pltpu.VMEM((CORE, rows, LANES), F32),
            pltpu.VMEM((comps, LANES), F32),
            pltpu.VMEM((plane // CORE, 2, LANES), F32),
            pltpu.VMEM((plane - 1, 2, LANES), F32),
            pltpu.VMEM((2, LANES), F32),
            pltpu.VMEM((Z - 1, 2, LANES), F32),
            pltpu.VMEM((plane // CORE, 2, LANES), F32),
            dma((len(LOADS) + 2,)),
            dma((2, 2)),
            dma((2, 1)),
            dma((2, 1)),
            dma((2, 1)),
            dma((2, len(DIRECT))),
            dma((2, len(PAIRED))),
            dma((2, len(PAIRED))),
            dma((2, 2)),
            dma((2, 1)),
            dma((2, 1)),
            dma((2, 1)),
            dma((2, 1)),
            pltpu.SemaphoreType.REGULAR,
            pltpu.SemaphoreType.REGULAR,
        ],
        compiler_params=pltpu.CompilerParams(
            collective_id=0, has_side_effects=True, vmem_limit_bytes=24 << 20
        ),
        name="subspace_step",
    )(*(pltpu.with_memory_space_constraint(a, pltpu.HBM) for a in (counts, occupancy, start_basis)))
    return basis_now.T * math.sqrt(genes * XL * CORE)


def solution(mesh):
    placed = (P("cells", "genes"), P("cells", "genes"), P(None, "genes"))
    return jax.shard_map(
        on_device, mesh=mesh, in_specs=placed, out_specs=P(None, ("genes", "cells")), check_vma=False
    )
```

```python
import math

import jax
import jax.numpy as jnp
from jax import lax
from jax.experimental import pallas as pl
from jax.experimental.pallas import tpu as pltpu
from jax.sharding import PartitionSpec as P

F32 = jnp.float32
BF16 = jnp.bfloat16
MESH = pl.DeviceIdType.MESH
Z, H, Y, XL, CORE = 16, 2, 4, 2, 2
LANES = 128
DIRECT = (8, 10)
PAIRED = (6, 4, 12, 2, 14, 0)
SCORE_ROW = 7
LEAD = 1
LOADS = (16, 16)
NT = (((1,), (1,)), ((), ()))


def device(z, h, y, xl, core):
    return ((z * H + h) * Y + y, xl * CORE + core)


def far_first(offsets, weights, sizes):
    def far(offset):
        return -sum(w * min(o, n - o) for o, w, n in zip(offset, weights, sizes))

    return sorted((o for o in offsets if any(o)), key=far)


def total_of(values):
    values = list(values)
    while len(values) > 1:
        values = [sum(values[i : i + 2][1:], values[i]) for i in range(0, len(values), 2)]
    return values[0]


def solve(gram, right):
    blocks = gram.shape[0] // 8
    left = [gram[8 * b : 8 * b + 8] for b in range(blocks)]
    right = [right[8 * b : 8 * b + 8] for b in range(blocks)]
    row_at = lax.broadcasted_iota(jnp.int32, (8, LANES), 0)
    done = []
    for kb in range(blocks):
        cols = [
            [
                jnp.broadcast_to(left[b][:, 8 * kb + j : 8 * kb + j + 1], (8, LANES))
                for j in range(8)
            ]
            for b in range(kb, blocks)
        ]
        rows_left, rows_right = left[kb], right[kb]
        scale = jnp.zeros((8, LANES), F32)
        steps = []
        for j in range(8):
            pivot = jnp.broadcast_to(cols[0][j][j : j + 1], (8, LANES))
            inv = lax.rsqrt(pivot)
            scale = jnp.where(row_at == j, inv, scale)
            lower = [c[j] * inv for c in cols]
            for m in range(j + 1, 8):
                entry = jnp.broadcast_to(lower[0][m : m + 1], (8, LANES))
                for c, low in zip(cols, lower):
                    c[m] = c[m] - low * entry
            below = jnp.where(row_at > j, lower[0], 0.0)
            unit_left = jnp.broadcast_to(rows_left[j : j + 1], rows_left.shape) * inv[:, : rows_left.shape[1]]
            unit_right = jnp.broadcast_to(rows_right[j : j + 1], rows_right.shape) * inv
            rows_left = rows_left - below[:, : rows_left.shape[1]] * unit_left
            rows_right = rows_right - below * unit_right
            steps.append((lower[1:], unit_left, unit_right))
        done.append(rows_right * scale)
        for at, b in enumerate(range(kb + 1, blocks)):
            for lower, unit_left, unit_right in steps:
                left[b] = left[b] - lower[at][:, : unit_left.shape[1]] * unit_left
                right[b] = right[b] - lower[at] * unit_right
    return jnp.concatenate(done, axis=0)


def kernel(
    counts_hbm,
    occupancy_hbm,
    basis_hbm,
    out,
    counts,
    occupancy,
    basis,
    cbuf,
    split_mean,
    mean_all,
    means_direct,
    means_direct_in,
    means_out,
    means_out_in,
    means_paired,
    means_paired_in,
    score,
    score_in,
    direct,
    direct_in,
    paired,
    paired_in,
    pair_out,
    pair_in,
    pair_dev,
    dev_mean,
    mean_xy,
    turned,
    zpart,
    zaux,
    zpart_in,
    zaux_in,
    tile,
    spread,
    gram,
    gram_in,
    gram_z,
    gram_z_in,
    gram_all,
    sem_in,
    sem_score,
    sem_means,
    sem_means_out,
    sem_means_paired,
    sem_direct,
    sem_pair,
    sem_paired,
    sem_z,
    sem_tile,
    sem_gram,
    sem_gram_z,
    sem_all,
    sem_beyond,
    sem_far,
):
    cells_at, genes_at = lax.axis_index("cells"), lax.axis_index("genes")
    z, h, y = cells_at // (H * Y), lax.rem(cells_at // Y, H), lax.rem(cells_at, Y)
    xl, core = genes_at // CORE, lax.rem(genes_at, CORE)
    comps = basis.shape[0]
    rows = comps // Y
    cells = counts.shape[0]
    width = LANES // Y
    plane = H * XL * CORE * Y

    loads = [pltpu.make_async_copy(occupancy_hbm, occupancy, sem_in.at[0])]
    tiles = [(sum(LOADS[:c]), sum(LOADS[: c + 1])) for c in range(len(LOADS))]
    spans = [pl.ds(first * LANES, (last - first) * LANES) for first, last in tiles]
    for c, span in enumerate(spans):
        loads.append(
            pltpu.make_async_copy(counts_hbm.at[:, span], counts.at[:, span], sem_in.at[c + 1])
        )
    loads.append(pltpu.make_async_copy(basis_hbm, basis, sem_in.at[len(LOADS) + 1]))
    for load in loads:
        load.start()

    def send(src, dst, sems, to, step=0):
        pltpu.make_async_remote_copy(
            src_ref=src,
            dst_ref=dst,
            send_sem=sems.at[0, step],
            recv_sem=sems.at[1, step],
            device_id=to if len(to) == 2 else device(*to),
            device_id_type=MESH,
        ).start()

    def waiting(all_bytes, sems, step):
        return pltpu.make_async_remote_copy(
            src_ref=all_bytes,
            dst_ref=all_bytes,
            send_sem=sems.at[0, step],
            recv_sem=sems.at[1, step],
            device_id=(cells_at, genes_at),
            device_id_type=MESH,
        )

    def wait_out(all_bytes, sems, step=0):
        waiting(all_bytes, sems, step).wait_send()

    def wait_in(all_bytes, sems, step=0):
        waiting(all_bytes, sems, step).wait_recv()

    def wait(all_bytes, sems, step=0):
        wait_out(all_bytes, sems, step)
        wait_in(all_bytes, sems, step)

    def gene_peer(a, b):
        return device(z, h, y, lax.rem(xl + a, XL), lax.rem(core + b, CORE))

    def z_peer(o):
        return device(lax.rem(z + o + Z, Z), h, y, xl, core)

    in_x = h * XL + xl
    chip = in_x * Y + y

    def chip_peer(a, c):
        xt, yt = lax.rem(in_x + a, H * XL), lax.rem(y + c, Y)
        return xt * Y + yt, (z, xt // XL, yt, lax.rem(xt, XL))

    def z_tile(o):
        return lax.rem(z + o + Z, Z)

    beside = [1 - 2 * lax.rem(z + ht, 2) for ht in range(H)]
    own_beside = 1 - 2 * lax.rem(z + h, 2)

    gene_offsets = [(1, 0), (1, 1), (0, 1)]
    xy_offsets = far_first([(a, b) for a in range(H) for b in range(Y)], (4, 2), (H, Y))
    xy_peers = []
    for a, b in xy_offsets:
        ht, yt = lax.rem(h + a, H), lax.rem(y + b, Y)
        xy_peers.append((ht, yt, device(z, ht, yt, xl, core)))
    chip_offsets = far_first([(a, c) for a in range(H * XL) for c in range(Y)], (1, 1), (H * XL, Y))
    z_offsets = far_first([(o,) for o in range(Z)], (1,), (Z,))

    barrier = pltpu.get_barrier_semaphore()
    beyond = [device(z, h, lax.rem(y + b, Y), xl, core) for b in range(1, Y)] + [z_peer(2), z_peer(-2)]
    peers = [gene_peer(a, b) for a, b in gene_offsets] + beyond
    peers += [device(z, 1 - h, y, xl, core), z_peer(1), z_peer(-1)]
    peers += [device(z_tile(o), h, y, xl, 1 - core) for o in (1, -1, 2, -2)]
    for peer in peers:
        pl.semaphore_signal(barrier, inc=1, device_id=peer, device_id_type=MESH)

    row_at = lax.broadcasted_iota(jnp.int32, (16, LANES), 0)
    group_at = lax.broadcasted_iota(jnp.int32, (16, LANES), 1) // width
    for ref in (means_direct, means_out, means_paired):
        ref[...] = jnp.zeros(ref.shape, F32)
    turned[...] = jnp.zeros((LANES, LANES), F32)

    def center(j):
        at = pl.ds(j * LANES, LANES)
        entries = counts[:, at].astype(F32)
        logged = jnp.log(1.0 + entries) * occupancy[0, j].astype(F32)
        mean = jnp.sum(logged, axis=0, keepdims=True) * (1.0 / cells)
        cbuf[:, at] = (logged - mean).astype(BF16)
        mean_all[j % H, j // H : j // H + 1, :] = mean

    def product_of(c):
        span = spans[c]
        return lax.dot_general(basis[:, span], cbuf[:, span], NT, preferred_element_type=F32)

    loads[0].wait()
    products = []
    for c in range(len(LOADS)):
        loads[c + 1].wait()
        if c == 1:
            loads[-1].wait()
        if c:
            products.append(product_of(c - 1))
        for j in range(*tiles[c]):
            center(j)
    products.append(product_of(len(LOADS) - 1))
    score[0:comps, :] = total_of(products)

    pl.semaphore_wait(barrier, len(peers))
    for peer in beyond:
        pl.semaphore_signal(sem_beyond, inc=1, device_id=peer, device_id_type=MESH)
    of_cells, of_means = pl.ds(0, comps), pl.ds(comps, 8)

    def send_scores(span, step):
        for s, (a, b) in enumerate(gene_offsets):
            send(score.at[span], score_in.at[s, span], sem_score, gene_peer(a, b), step)

    send_scores(of_cells, 0)
    for j in range(Z * H):
        mean = mean_all[j % H, j // H : j // H + 1, :]
        high = mean.astype(BF16).astype(F32)
        middle = (mean - high).astype(BF16).astype(F32)
        low = mean - high - middle
        stacked = jnp.where(
            row_at == 0, high, jnp.where(row_at == 1, middle, jnp.where(row_at == 2, low, 0.0))
        )
        split_mean[:, j * LANES : (j + 1) * LANES] = stacked.astype(BF16)
    of_mean = lax.dot_general(split_mean[...], basis[...], NT, preferred_element_type=F32)
    score[comps : comps + 8, :] = jnp.zeros((8, LANES), F32)
    score[comps : comps + 1, 0:comps] = of_mean[0:1] + of_mean[1:2] + of_mean[2:3]
    send_scores(of_means, 1)
    for ht in range(H):
        for i in range(2 * len(DIRECT)):
            at = z_tile(DIRECT[i // 2] + i % 2 * beside[ht])
            means_direct[ht, i : i + 1, :] = mean_all[ht, pl.ds(at, 1), :]
        for j, e in enumerate(PAIRED):
            means_out[ht, j : j + 1, :] = mean_all[ht, pl.ds(z_tile(e + beside[ht]), 1), :]
            means_paired[ht, j : j + 1, :] = mean_all[ht, pl.ds(z_tile(e), 1), :]
    pl.semaphore_wait(sem_beyond, len(beyond))
    for o in (4, -4):
        pl.semaphore_signal(sem_far, inc=1, device_id=z_peer(o), device_id_type=MESH)
    wait(score_in.at[:, of_cells], sem_score)
    scores = total_of([score[0:comps]] + [score_in[a, 0:comps] for a in range(XL * CORE - 1)])
    score_high = scores.astype(BF16)
    score_low = (scores - score_high.astype(F32)).astype(BF16)
    stacked = jnp.concatenate([score_high, score_low], axis=0)

    def pieces(tiles):
        columns = [
            cbuf[:, pl.ds(pl.multiple_of((tiles[ht] * H + ht) * LANES, LANES), LANES)] for ht in range(H)
        ]
        both = jnp.dot(stacked, jnp.concatenate(columns, axis=1), preferred_element_type=F32)
        product = both[:comps] + both[comps:]
        result = []
        for ht in range(H):
            turns = []
            for b in range(Y):
                block = product[b * rows : (b + 1) * rows, ht * LANES : (ht + 1) * LANES]
                turns.append([block] + [pltpu.roll(block, k * width, 1) for k in range(1, Y)])
            for yt in range(Y):
                piece = turns[0][(0 - yt) % Y]
                for b in range(1, Y):
                    piece = jnp.where(group_at == b, turns[b][(b - yt) % Y], piece)
                result.append((ht, yt, piece))
        return result

    def exchange(src, dst, sems, chunk, span):
        for s, (ht, yt, to) in enumerate(xy_peers):
            send(src.at[ht, yt, span], dst.at[span, s], sems, to, chunk)

    def start_direct(j):
        for i in (2 * j, 2 * j + 1):
            tiles = [z_tile(DIRECT[j] + i % 2 * beside[ht]) for ht in range(H)]
            for ht, yt, piece in pieces(tiles):
                direct[ht, yt, i] = piece
        exchange(direct, direct_in, sem_direct, j, pl.ds(2 * j, 2))

    def start_pair(j):
        for ht, yt, piece in pieces([z_tile(PAIRED[j] + beside[ht]) for ht in range(H)]):
            pair_out[ht, j, yt] = piece
        for ht in range(H):
            send(pair_out.at[ht, j], pair_in.at[ht, j], sem_pair, z_peer(beside[ht]), j)

    def send_means():
        wait(score_in.at[:, of_means], sem_score, 1)
        whole = total_of(
            [score[comps : comps + 1]]
            + [score_in[a, comps : comps + 1] for a in range(XL * CORE - 1)]
        )
        for ht in range(H):
            for ref in (means_direct, means_out, means_paired):
                ref[ht, SCORE_ROW : SCORE_ROW + 1, :] = whole
            send(means_out.at[ht], means_out_in.at[ht], sem_means_out, z_peer(beside[ht]))
        for s, (ht, _, to) in enumerate(xy_peers):
            send(means_direct.at[ht], means_direct_in.at[s], sem_means, to)

    start_pair(0)
    send_means()
    start_direct(0)
    start_pair(1)
    start_direct(1)
    for j in range(2, len(PAIRED)):
        start_pair(j)
    for j, e in enumerate(PAIRED):
        for ht, yt, piece in pieces([z_tile(e)] * H):
            paired[ht, yt, j] = piece

    def fold_rows(values):
        for p, value in enumerate(values):
            turned[p : p + 1, :] = value
        flat = turned[...].T
        result = []
        for p in range(len(values)):
            folded = jnp.broadcast_to(flat[0:rows, p : p + 1], (rows, LANES))
            for b in range(1, Y):
                block = jnp.broadcast_to(flat[b * rows : (b + 1) * rows, p : p + 1], (rows, LANES))
                folded = jnp.where(group_at == b, block, folded)
            result.append(folded)
        return result

    def columns_of(means, yt):
        kept = jnp.where(group_at[0:8] == yt, means, 0.0)
        return total_of([kept] + [pltpu.roll(kept, k * width, 1) for k in range(1, Y)])

    groups = len(xy_offsets) + 1

    def plane_terms(level, weight, own, others):
        values = [own[h]] + [others[s] for s in range(groups - 1)]
        middle = total_of(values) * (1.0 / groups)
        apart = [value - middle for value in values]
        away = fold_rows([a[SCORE_ROW : SCORE_ROW + 1] * weight for a in apart])
        mean_xy[level] = columns_of(middle, y)
        for p, value in enumerate(apart):
            dev_mean[level, p] = columns_of(value, y)
        return middle[SCORE_ROW : SCORE_ROW + 1], away

    wait(means_out_in, sem_means_out)
    apart = [means_paired[ht] - means_out_in[ht] for ht in range(H)]
    pair_away = fold_rows([a[SCORE_ROW : SCORE_ROW + 1] * (0.5 * cells) for a in apart])
    for ht in range(H):
        means_paired[ht] = 0.5 * (means_paired[ht] + means_out_in[ht])
        for yt in range(Y):
            pair_dev[ht, yt] = columns_of(apart[ht], yt)
    for s, (ht, _, to) in enumerate(xy_peers):
        send(means_paired.at[ht], means_paired_in.at[s], sem_means_paired, to)

    def add_pair(j):
        wait(pair_in.at[:, j], sem_pair, j)
        for ht in range(H):
            for yt in range(Y):
                paired[ht, yt, j] = (paired[ht, yt, j] + pair_in[ht, j, yt]) + pair_away[
                    ht
                ] * pair_dev[ht, yt, j : j + 1, :]
        exchange(paired, paired_in, sem_paired, j, pl.ds(j, 1))

    leads = core == LEAD
    last = 2 * len(DIRECT) + len(PAIRED) - 1
    after_leads = (CORE - 1 - core) * last

    def lead_peer(o):
        return device(z_tile(o), h, y, xl, LEAD)

    def plane_sum(level, slot, own, others, i, away, middle, to):
        terms = [own[h, y, i]] + [others[i, s] for s in range(groups - 1)]
        terms += [away[p] * dev_mean[level, p, i : i + 1, :] for p in range(groups)]
        zpart[slot] = total_of(terms)
        zaux[slot, 0:1, :] = mean_xy[level, i : i + 1, :]
        zaux[slot, 1:2, :] = middle
        def send_sum():
            send(zpart.at[slot], zpart_in.at[slot + after_leads], sem_z, to)
            send(zaux.at[slot], zaux_in.at[slot + after_leads], sem_z, to, 1)

        if slot < last:
            send_sum()
        else:
            pl.when(jnp.logical_not(leads))(send_sum)

    def sum_direct(j):
        wait(direct_in.at[pl.ds(2 * j, 2)], sem_direct, j)
        for i in (2 * j, 2 * j + 1):
            to = lead_peer(DIRECT[j] + i % 2 * own_beside)
            plane_sum(0, i, direct, direct_in, i, away_direct, score_direct, to)

    for j in range(len(PAIRED) - 1):
        add_pair(j)
    wait(means_direct_in, sem_means)
    score_direct, away_direct = plane_terms(0, float(cells), means_direct, means_direct_in)
    pl.semaphore_wait(sem_far, 2)
    sum_direct(0)
    add_pair(len(PAIRED) - 1)
    sum_direct(1)
    wait(means_paired_in, sem_means_paired)
    score_paired, away_paired = plane_terms(1, 2.0 * cells, means_paired, means_paired_in)
    alone = 2 * len(DIRECT)
    for j, e in enumerate(PAIRED):
        wait(paired_in.at[pl.ds(j, 1)], sem_paired, j)
        plane_sum(1, alone + j, paired, paired_in, j, away_paired, score_paired, lead_peer(e))
    def columns(folded, group):
        turns = [pltpu.roll(folded, (Y - b + group) % Y * width, 1) if b != group else folded for b in range(Y)]
        return [jnp.where(group_at == group, turn, 0.0) for turn in turns]

    chips = plane // CORE

    @pl.when(leads)
    def _():
        wait_out(zpart.at[pl.ds(0, last)], sem_z)
        wait_out(zaux.at[pl.ds(0, last)], sem_z, 1)
        wait_in(zpart_in, sem_z)
        wait_in(zaux_in, sem_z, 1)
        shares = [1.0] * alone + [2.0] * len(PAIRED)
        scores_of = [zaux_in[i, 1:2, :] for i in range(last)] + [zaux[last, 1:2, :]]
        middle = total_of([v * w for v, w in zip(scores_of, shares)]) * (1.0 / Z)
        away = fold_rows([(v - middle) * (w * cells * groups) for v, w in zip(scores_of, shares)])
        own = [zpart_in[i] for i in range(last)] + [zpart[last]]
        own_means = [zaux_in[i, 0:1, :] for i in range(last)] + [zaux[last, 0:1, :]]
        others = [zpart_in[i] for i in range(last, 2 * last + 1)]
        other_means = [zaux_in[i, 0:1, :] for i in range(last, 2 * last + 1)]
        for t, (sums, means) in enumerate(((own, own_means), (others, other_means))):
            middle = total_of([v * w for v, w in zip(means, shares)]) * (1.0 / Z)
            tile[t] = total_of(sums + [far * (v - middle) for far, v in zip(away, means)])
        send(tile.at[1], tile.at[0], sem_tile, (z, h, y, xl, 1 - LEAD))
        both = [a + b for a, b in zip(columns(tile[0], 0), columns(tile[1], 1))]
        spread[...] = jnp.concatenate(both, axis=0)
        own_gram = lax.dot_general(
            spread[...], spread[...], NT, precision=lax.Precision.HIGHEST, preferred_element_type=F32
        )
        packed = jnp.concatenate([own_gram[0 : comps // 2], own_gram[comps // 2 :]], axis=1)
        for e in range(chips):
            gram[e] = packed[2 * e : 2 * e + 2]
        for s, offset in enumerate(chip_offsets):
            at, to = chip_peer(*offset)
            send(gram.at[at], gram_in.at[s], sem_gram, (*to, LEAD))
        wait_out(gram.at[pl.ds(0, chips - 1)], sem_gram)
        wait_in(gram_in.at[pl.ds(0, chips - 1)], sem_gram)
        gram_z[...] = jnp.sum(gram_in[0 : chips - 1], axis=0) + gram[chip]
        for s, (o,) in enumerate(z_offsets):
            send(gram_z, gram_z_in.at[s], sem_gram_z, z_peer(o))
        wait(gram_z_in, sem_gram_z)
        gram_all[chip] = jnp.sum(gram_z_in[...], axis=0) + gram_z[...]
        for offset in chip_offsets:
            for other in range(CORE):
                send(gram_all.at[chip], gram_all.at[chip], sem_all, (*chip_peer(*offset)[1], other))
        send(gram_all.at[chip], gram_all.at[chip], sem_all, (*chip_peer(0, 0)[1], 1 - LEAD))
        wait_out(tile.at[1], sem_tile)
        wait_out(gram_in, sem_all)
        wait_in(gram_all.at[pl.ds(0, chips - 1)], sem_all)

    @pl.when(jnp.logical_not(leads))
    def _():
        wait_out(zpart, sem_z)
        wait_out(zaux, sem_z, 1)
        wait_in(tile.at[0], sem_tile)
        spread[...] = jnp.concatenate(columns(tile[0], 0), axis=0)
        wait_in(gram_all, sem_all)

    packed = gram_all[...].reshape(comps // 2, LANES)
    gram_sum = jnp.concatenate([packed[:, 0:comps], packed[:, comps : 2 * comps]], axis=0)
    out[...] = solve(gram_sum, spread[...]).T[0:width]


def on_device(counts, occupancy, start_basis):
    comps, genes = start_basis.shape
    cells = counts.shape[0]
    rows = comps // Y
    plane = H * XL * CORE * Y
    tiles = 2 * len(DIRECT) + len(PAIRED)
    dma = pltpu.SemaphoreType.DMA
    hbm = pl.BlockSpec(memory_space=pltpu.HBM)
    basis_now = pl.pallas_call(
        kernel,
        out_shape=jax.ShapeDtypeStruct((LANES // Y, comps), F32),
        in_specs=[hbm, hbm, hbm],
        out_specs=pl.BlockSpec(memory_space=pltpu.VMEM),
        scratch_shapes=[
            pltpu.VMEM((cells, genes), BF16),
            pltpu.SMEM(occupancy.shape, jnp.int32),
            pltpu.VMEM((comps, genes), BF16),
            pltpu.VMEM((cells, genes), BF16),
            pltpu.VMEM((16, genes), BF16),
            pltpu.VMEM((H, Z, LANES), F32),
            pltpu.VMEM((H, 8, LANES), F32),
            pltpu.VMEM((H * Y - 1, 8, LANES), F32),
            pltpu.VMEM((H, 8, LANES), F32),
            pltpu.VMEM((H, 8, LANES), F32),
            pltpu.VMEM((H, 8, LANES), F32),
            pltpu.VMEM((H * Y - 1, 8, LANES), F32),
            pltpu.VMEM((comps + 8, LANES), F32),
            pltpu.VMEM((XL * CORE - 1, comps + 8, LANES), F32),
            pltpu.VMEM((H, Y, 2 * len(DIRECT), rows, LANES), F32),
            pltpu.VMEM((2 * len(DIRECT), H * Y - 1, rows, LANES), F32),
            pltpu.VMEM((H, Y, len(PAIRED), rows, LANES), F32),
            pltpu.VMEM((len(PAIRED), H * Y - 1, rows, LANES), F32),
            pltpu.VMEM((H, len(PAIRED), Y, rows, LANES), F32),
            pltpu.VMEM((H, len(PAIRED), Y, rows, LANES), F32),
            pltpu.VMEM((H, Y, 8, LANES), F32),
            pltpu.VMEM((2, H * Y, 8, LANES), F32),
            pltpu.VMEM((2, 8, LANES), F32),
            pltpu.VMEM((LANES, LANES), F32),
            pltpu.VMEM((tiles, rows, LANES), F32),
            pltpu.VMEM((tiles, 2, LANES), F32),
            pltpu.VMEM((CORE * tiles - 1, rows, LANES), F32),
            pltpu.VMEM((CORE * tiles - 1, 2, LANES), F32),
            pltpu.VMEM((CORE, rows, LANES), F32),
            pltpu.VMEM((comps, LANES), F32),
            pltpu.VMEM((plane // CORE, 2, LANES), F32),
            pltpu.VMEM((plane - 1, 2, LANES), F32),
            pltpu.VMEM((2, LANES), F32),
            pltpu.VMEM((Z - 1, 2, LANES), F32),
            pltpu.VMEM((plane // CORE, 2, LANES), F32),
            dma((len(LOADS) + 2,)),
            dma((2, 2)),
            dma((2, 1)),
            dma((2, 1)),
            dma((2, 1)),
            dma((2, len(DIRECT))),
            dma((2, len(PAIRED))),
            dma((2, len(PAIRED))),
            dma((2, 2)),
            dma((2, 1)),
            dma((2, 1)),
            dma((2, 1)),
            dma((2, 1)),
            pltpu.SemaphoreType.REGULAR,
            pltpu.SemaphoreType.REGULAR,
        ],
        compiler_params=pltpu.CompilerParams(
            collective_id=0, has_side_effects=True, vmem_limit_bytes=24 << 20
        ),
        name="subspace_step",
    )(*(pltpu.with_memory_space_constraint(a, pltpu.HBM) for a in (counts, occupancy, start_basis)))
    return basis_now.T * math.sqrt(genes * XL * CORE)


def solution(mesh):
    placed = (P("cells", "genes"), P("cells", "genes"), P(None, "genes"))
    return jax.shard_map(
        on_device, mesh=mesh, in_specs=placed, out_specs=P(None, ("genes", "cells")), check_vma=False
    )
```

```python
import math

import jax
import jax.numpy as jnp
from jax import lax
from jax.experimental import pallas as pl
from jax.experimental.pallas import tpu as pltpu
from jax.sharding import PartitionSpec as P

F32 = jnp.float32
BF16 = jnp.bfloat16
MESH = pl.DeviceIdType.MESH
Z, H, Y, XL, CORE = 16, 2, 4, 2, 2
LANES = 128
DIRECT = (8, 10)
PAIRED = (6, 4, 12, 2, 14, 0)
SCORE_ROW = 7
LEAD = 1
LOADS = (16, 16)
NT = (((1,), (1,)), ((), ()))


def device(z, h, y, xl, core):
    return ((z * H + h) * Y + y, xl * CORE + core)


def far_first(offsets, weights, sizes):
    def far(offset):
        return -sum(w * min(o, n - o) for o, w, n in zip(offset, weights, sizes))

    return sorted((o for o in offsets if any(o)), key=far)


def total_of(values):
    values = list(values)
    while len(values) > 1:
        values = [sum(values[i : i + 2][1:], values[i]) for i in range(0, len(values), 2)]
    return values[0]


def solve(joint, start):
    blocks = joint.shape[0] // 8
    joint = [joint[8 * b : 8 * b + 8] for b in range(blocks)]
    row_at = lax.broadcasted_iota(jnp.int32, (8, LANES), 0)
    done = []
    for kb in range(blocks):
        cols = []
        for b in range(kb, blocks):
            at = start + 8 * kb
            cols.append(
                [jnp.broadcast_to(joint[b][:, at + j : at + j + 1], (8, LANES)) for j in range(8)]
            )
        block = joint[kb]
        scale = jnp.zeros((8, LANES), F32)
        steps = []
        for j in range(8):
            pivot = jnp.broadcast_to(cols[0][j][j : j + 1], (8, LANES))
            inv = lax.rsqrt(pivot)
            scale = jnp.where(row_at == j, inv, scale)
            lower = [c[j] * inv for c in cols]
            for m in range(j + 1, 8):
                entry = jnp.broadcast_to(lower[0][m : m + 1], (8, LANES))
                for c, low in zip(cols, lower):
                    c[m] = c[m] - low * entry
            unit = jnp.broadcast_to(block[j : j + 1], (8, LANES)) * inv
            block = block - jnp.where(row_at > j, lower[0], 0.0) * unit
            steps.append((lower[1:], unit))
        done.append(block * scale)
        for at, b in enumerate(range(kb + 1, blocks)):
            for lower, unit in steps:
                joint[b] = joint[b] - lower[at] * unit
    return jnp.concatenate(done, axis=0)


def kernel(
    counts_hbm,
    occupancy_hbm,
    basis_hbm,
    out,
    counts,
    occupancy,
    basis,
    cbuf,
    split_mean,
    mean_all,
    means_direct,
    means_direct_in,
    means_out,
    means_out_in,
    means_paired,
    means_paired_in,
    score,
    score_in,
    direct,
    direct_in,
    paired,
    paired_in,
    pair_out,
    pair_in,
    pair_dev,
    dev_mean,
    mean_xy,
    turned,
    zpart,
    zaux,
    zpart_in,
    zaux_in,
    tile,
    spread,
    gram,
    gram_in,
    gram_z,
    gram_z_in,
    gram_all,
    sem_in,
    sem_score,
    sem_means,
    sem_means_out,
    sem_means_paired,
    sem_direct,
    sem_pair,
    sem_paired,
    sem_z,
    sem_tile,
    sem_gram,
    sem_gram_z,
    sem_all,
    sem_beyond,
    sem_far,
):
    cells_at, genes_at = lax.axis_index("cells"), lax.axis_index("genes")
    z, h, y = cells_at // (H * Y), lax.rem(cells_at // Y, H), lax.rem(cells_at, Y)
    xl, core = genes_at // CORE, lax.rem(genes_at, CORE)
    comps = basis.shape[0]
    rows = comps // Y
    cells = counts.shape[0]
    width = LANES // Y
    plane = H * XL * CORE * Y

    loads = [pltpu.make_async_copy(occupancy_hbm, occupancy, sem_in.at[0])]
    tiles = [(sum(LOADS[:c]), sum(LOADS[: c + 1])) for c in range(len(LOADS))]
    spans = [pl.ds(first * LANES, (last - first) * LANES) for first, last in tiles]
    for c, span in enumerate(spans):
        loads.append(
            pltpu.make_async_copy(counts_hbm.at[:, span], counts.at[:, span], sem_in.at[c + 1])
        )
    loads.append(pltpu.make_async_copy(basis_hbm, basis, sem_in.at[len(LOADS) + 1]))
    for load in loads:
        load.start()

    def send(src, dst, sems, to, step=0):
        pltpu.make_async_remote_copy(
            src_ref=src,
            dst_ref=dst,
            send_sem=sems.at[0, step],
            recv_sem=sems.at[1, step],
            device_id=to if len(to) == 2 else device(*to),
            device_id_type=MESH,
        ).start()

    def waiting(all_bytes, sems, step):
        return pltpu.make_async_remote_copy(
            src_ref=all_bytes,
            dst_ref=all_bytes,
            send_sem=sems.at[0, step],
            recv_sem=sems.at[1, step],
            device_id=(cells_at, genes_at),
            device_id_type=MESH,
        )

    def wait_out(all_bytes, sems, step=0):
        waiting(all_bytes, sems, step).wait_send()

    def wait_in(all_bytes, sems, step=0):
        waiting(all_bytes, sems, step).wait_recv()

    def wait(all_bytes, sems, step=0):
        wait_out(all_bytes, sems, step)
        wait_in(all_bytes, sems, step)

    def gene_peer(a, b):
        return device(z, h, y, lax.rem(xl + a, XL), lax.rem(core + b, CORE))

    def z_peer(o):
        return device(lax.rem(z + o + Z, Z), h, y, xl, core)

    in_x = h * XL + xl
    chip = in_x * Y + y

    def chip_peer(a, c):
        xt, yt = lax.rem(in_x + a, H * XL), lax.rem(y + c, Y)
        return xt * Y + yt, (z, xt // XL, yt, lax.rem(xt, XL))

    def z_tile(o):
        return lax.rem(z + o + Z, Z)

    beside = [1 - 2 * lax.rem(z + ht, 2) for ht in range(H)]
    own_beside = 1 - 2 * lax.rem(z + h, 2)

    gene_offsets = [(1, 0), (1, 1), (0, 1)]
    xy_offsets = far_first([(a, b) for a in range(H) for b in range(Y)], (4, 2), (H, Y))
    xy_peers = []
    for a, b in xy_offsets:
        ht, yt = lax.rem(h + a, H), lax.rem(y + b, Y)
        xy_peers.append((ht, yt, device(z, ht, yt, xl, core)))
    chip_offsets = far_first([(a, c) for a in range(H * XL) for c in range(Y)], (1, 1), (H * XL, Y))
    z_offsets = far_first([(o,) for o in range(Z)], (1,), (Z,))

    barrier = pltpu.get_barrier_semaphore()
    beyond = [device(z, h, lax.rem(y + b, Y), xl, core) for b in range(1, Y)] + [z_peer(2), z_peer(-2)]
    peers = [gene_peer(a, b) for a, b in gene_offsets] + beyond
    peers += [device(z, 1 - h, y, xl, core), z_peer(1), z_peer(-1)]
    peers += [device(z_tile(o), h, y, xl, 1 - core) for o in (1, -1, 2, -2)]
    for peer in peers:
        pl.semaphore_signal(barrier, inc=1, device_id=peer, device_id_type=MESH)

    row_at = lax.broadcasted_iota(jnp.int32, (16, LANES), 0)
    group_at = lax.broadcasted_iota(jnp.int32, (16, LANES), 1) // width
    for ref in (means_direct, means_out, means_paired):
        ref[...] = jnp.zeros(ref.shape, F32)
    turned[...] = jnp.zeros((LANES, LANES), F32)

    def center(j):
        at = pl.ds(j * LANES, LANES)
        entries = counts[:, at].astype(F32)
        logged = jnp.log(1.0 + entries) * occupancy[0, j].astype(F32)
        mean = jnp.sum(logged, axis=0, keepdims=True) * (1.0 / cells)
        cbuf[:, at] = (logged - mean).astype(BF16)
        mean_all[j % H, j // H : j // H + 1, :] = mean

    def product_of(c):
        span = spans[c]
        return lax.dot_general(basis[:, span], cbuf[:, span], NT, preferred_element_type=F32)

    loads[0].wait()
    products = []
    for c in range(len(LOADS)):
        loads[c + 1].wait()
        if c == 1:
            loads[-1].wait()
        if c:
            products.append(product_of(c - 1))
        for j in range(*tiles[c]):
            center(j)
    products.append(product_of(len(LOADS) - 1))
    score[0:comps, :] = total_of(products)

    pl.semaphore_wait(barrier, len(peers))
    of_cells, of_means = pl.ds(0, comps), pl.ds(comps, 8)

    def send_scores(span, step):
        for s, (a, b) in enumerate(gene_offsets):
            send(score.at[span], score_in.at[s, span], sem_score, gene_peer(a, b), step)

    send_scores(of_cells, 0)
    for peer in beyond:
        pl.semaphore_signal(sem_beyond, inc=1, device_id=peer, device_id_type=MESH)
    for j in range(Z * H):
        mean = mean_all[j % H, j // H : j // H + 1, :]
        high = mean.astype(BF16).astype(F32)
        middle = (mean - high).astype(BF16).astype(F32)
        low = mean - high - middle
        stacked = jnp.where(
            row_at == 0, high, jnp.where(row_at == 1, middle, jnp.where(row_at == 2, low, 0.0))
        )
        split_mean[:, j * LANES : (j + 1) * LANES] = stacked.astype(BF16)
    of_mean = lax.dot_general(split_mean[...], basis[...], NT, preferred_element_type=F32)
    score[comps : comps + 8, :] = jnp.zeros((8, LANES), F32)
    score[comps : comps + 1, 0:comps] = of_mean[0:1] + of_mean[1:2] + of_mean[2:3]
    send_scores(of_means, 1)
    for ht in range(H):
        for i in range(2 * len(DIRECT)):
            at = z_tile(DIRECT[i // 2] + i % 2 * beside[ht])
            means_direct[ht, i : i + 1, :] = mean_all[ht, pl.ds(at, 1), :]
        for j, e in enumerate(PAIRED):
            means_out[ht, j : j + 1, :] = mean_all[ht, pl.ds(z_tile(e + beside[ht]), 1), :]
            means_paired[ht, j : j + 1, :] = mean_all[ht, pl.ds(z_tile(e), 1), :]
    pl.semaphore_wait(sem_beyond, len(beyond))
    for o in (4, -4):
        pl.semaphore_signal(sem_far, inc=1, device_id=z_peer(o), device_id_type=MESH)
    wait(score_in.at[:, of_cells], sem_score)
    scores = total_of([score[0:comps]] + [score_in[a, 0:comps] for a in range(XL * CORE - 1)])
    score_high = scores.astype(BF16)
    score_low = (scores - score_high.astype(F32)).astype(BF16)
    stacked = jnp.concatenate([score_high, score_low], axis=0)

    def pieces(tiles):
        columns = [
            cbuf[:, pl.ds(pl.multiple_of((tiles[ht] * H + ht) * LANES, LANES), LANES)] for ht in range(H)
        ]
        both = jnp.dot(stacked, jnp.concatenate(columns, axis=1), preferred_element_type=F32)
        product = both[:comps] + both[comps:]
        result = []
        for ht in range(H):
            turns = []
            for b in range(Y):
                block = product[b * rows : (b + 1) * rows, ht * LANES : (ht + 1) * LANES]
                turns.append([block] + [pltpu.roll(block, k * width, 1) for k in range(1, Y)])
            for yt in range(Y):
                piece = turns[0][(0 - yt) % Y]
                for b in range(1, Y):
                    piece = jnp.where(group_at == b, turns[b][(b - yt) % Y], piece)
                result.append((ht, yt, piece))
        return result

    def exchange(src, dst, sems, chunk, span):
        for s, (ht, yt, to) in enumerate(xy_peers):
            send(src.at[ht, yt, span], dst.at[span, s], sems, to, chunk)

    def start_direct(j):
        for i in (2 * j, 2 * j + 1):
            tiles = [z_tile(DIRECT[j] + i % 2 * beside[ht]) for ht in range(H)]
            for ht, yt, piece in pieces(tiles):
                direct[ht, yt, i] = piece
        exchange(direct, direct_in, sem_direct, j, pl.ds(2 * j, 2))

    def start_pair(j):
        for ht, yt, piece in pieces([z_tile(PAIRED[j] + beside[ht]) for ht in range(H)]):
            pair_out[ht, j, yt] = piece
        for ht in range(H):
            send(pair_out.at[ht, j], pair_in.at[ht, j], sem_pair, z_peer(beside[ht]), j)

    def send_means():
        wait(score_in.at[:, of_means], sem_score, 1)
        whole = total_of(
            [score[comps : comps + 1]]
            + [score_in[a, comps : comps + 1] for a in range(XL * CORE - 1)]
        )
        for ht in range(H):
            for ref in (means_direct, means_out, means_paired):
                ref[ht, SCORE_ROW : SCORE_ROW + 1, :] = whole
            send(means_out.at[ht], means_out_in.at[ht], sem_means_out, z_peer(beside[ht]))
        for s, (ht, _, to) in enumerate(xy_peers):
            send(means_direct.at[ht], means_direct_in.at[s], sem_means, to)

    start_pair(0)
    send_means()
    start_direct(0)
    start_pair(1)
    start_direct(1)
    for j in range(2, len(PAIRED)):
        start_pair(j)
    for j, e in enumerate(PAIRED):
        for ht, yt, piece in pieces([z_tile(e)] * H):
            paired[ht, yt, j] = piece

    def fold_rows(values):
        for p, value in enumerate(values):
            turned[p : p + 1, :] = value
        flat = turned[...].T
        result = []
        for p in range(len(values)):
            folded = jnp.broadcast_to(flat[0:rows, p : p + 1], (rows, LANES))
            for b in range(1, Y):
                block = jnp.broadcast_to(flat[b * rows : (b + 1) * rows, p : p + 1], (rows, LANES))
                folded = jnp.where(group_at == b, block, folded)
            result.append(folded)
        return result

    def columns_of(means, yt):
        kept = jnp.where(group_at[0:8] == yt, means, 0.0)
        return total_of([kept] + [pltpu.roll(kept, k * width, 1) for k in range(1, Y)])

    groups = len(xy_offsets) + 1

    def plane_terms(level, weight, own, others):
        values = [own[h]] + [others[s] for s in range(groups - 1)]
        middle = total_of(values) * (1.0 / groups)
        apart = [value - middle for value in values]
        away = fold_rows([a[SCORE_ROW : SCORE_ROW + 1] * weight for a in apart])
        mean_xy[level] = columns_of(middle, y)
        for p, value in enumerate(apart):
            dev_mean[level, p] = columns_of(value, y)
        return middle[SCORE_ROW : SCORE_ROW + 1], away

    wait(means_out_in, sem_means_out)
    apart = [means_paired[ht] - means_out_in[ht] for ht in range(H)]
    pair_away = fold_rows([a[SCORE_ROW : SCORE_ROW + 1] * (0.5 * cells) for a in apart])
    for ht in range(H):
        means_paired[ht] = 0.5 * (means_paired[ht] + means_out_in[ht])
        for yt in range(Y):
            pair_dev[ht, yt] = columns_of(apart[ht], yt)
    for s, (ht, _, to) in enumerate(xy_peers):
        send(means_paired.at[ht], means_paired_in.at[s], sem_means_paired, to)

    def add_pair(j):
        wait(pair_in.at[:, j], sem_pair, j)
        for ht in range(H):
            for yt in range(Y):
                paired[ht, yt, j] = (paired[ht, yt, j] + pair_in[ht, j, yt]) + pair_away[
                    ht
                ] * pair_dev[ht, yt, j : j + 1, :]
        exchange(paired, paired_in, sem_paired, j, pl.ds(j, 1))

    leads = core == LEAD
    last = 2 * len(DIRECT) + len(PAIRED) - 1
    after_leads = (CORE - 1 - core) * last

    def lead_peer(o):
        return device(z_tile(o), h, y, xl, LEAD)

    def plane_sum(level, slot, own, others, i, away, middle, to):
        terms = [own[h, y, i]] + [others[i, s] for s in range(groups - 1)]
        terms += [away[p] * dev_mean[level, p, i : i + 1, :] for p in range(groups)]
        zpart[slot] = total_of(terms)
        zaux[slot, 0:1, :] = mean_xy[level, i : i + 1, :]
        zaux[slot, 1:2, :] = middle
        def send_sum():
            send(zpart.at[slot], zpart_in.at[slot + after_leads], sem_z, to)
            send(zaux.at[slot], zaux_in.at[slot + after_leads], sem_z, to, 1)

        if slot < last:
            send_sum()
        else:
            pl.when(jnp.logical_not(leads))(send_sum)

    def sum_direct(j):
        wait(direct_in.at[pl.ds(2 * j, 2)], sem_direct, j)
        for i in (2 * j, 2 * j + 1):
            to = lead_peer(DIRECT[j] + i % 2 * own_beside)
            plane_sum(0, i, direct, direct_in, i, away_direct, score_direct, to)

    for j in range(len(PAIRED) - 1):
        add_pair(j)
    wait(means_direct_in, sem_means)
    score_direct, away_direct = plane_terms(0, float(cells), means_direct, means_direct_in)
    pl.semaphore_wait(sem_far, 2)
    sum_direct(0)
    add_pair(len(PAIRED) - 1)
    sum_direct(1)
    wait(means_paired_in, sem_means_paired)
    score_paired, away_paired = plane_terms(1, 2.0 * cells, means_paired, means_paired_in)
    alone = 2 * len(DIRECT)
    for j, e in enumerate(PAIRED):
        wait(paired_in.at[pl.ds(j, 1)], sem_paired, j)
        plane_sum(1, alone + j, paired, paired_in, j, away_paired, score_paired, lead_peer(e))
    def columns(folded, group):
        turns = [pltpu.roll(folded, (Y - b + group) % Y * width, 1) if b != group else folded for b in range(Y)]
        return [jnp.where(group_at == group, turn, 0.0) for turn in turns]

    chips = plane // CORE

    @pl.when(leads)
    def _():
        wait_out(zpart.at[pl.ds(0, last)], sem_z)
        wait_out(zaux.at[pl.ds(0, last)], sem_z, 1)
        wait_in(zpart_in, sem_z)
        wait_in(zaux_in, sem_z, 1)
        shares = [1.0] * alone + [2.0] * len(PAIRED)
        scores_of = [zaux_in[i, 1:2, :] for i in range(last)] + [zaux[last, 1:2, :]]
        middle = total_of([v * w for v, w in zip(scores_of, shares)]) * (1.0 / Z)
        away = fold_rows([(v - middle) * (w * cells * groups) for v, w in zip(scores_of, shares)])
        own = [zpart_in[i] for i in range(last)] + [zpart[last]]
        own_means = [zaux_in[i, 0:1, :] for i in range(last)] + [zaux[last, 0:1, :]]
        others = [zpart_in[i] for i in range(last, 2 * last + 1)]
        other_means = [zaux_in[i, 0:1, :] for i in range(last, 2 * last + 1)]
        for t, (sums, means) in enumerate(((own, own_means), (others, other_means))):
            middle = total_of([v * w for v, w in zip(means, shares)]) * (1.0 / Z)
            tile[t] = total_of(sums + [far * (v - middle) for far, v in zip(away, means)])
        send(tile.at[1], tile.at[0], sem_tile, (z, h, y, xl, 1 - LEAD))
        both = [a + b for a, b in zip(columns(tile[0], 0), columns(tile[1], 1))]
        spread[...] = jnp.concatenate(both, axis=0)
        own_gram = lax.dot_general(
            spread[...], spread[...], NT, precision=lax.Precision.HIGHEST, preferred_element_type=F32
        )
        packed = jnp.concatenate([own_gram[0 : comps // 2], own_gram[comps // 2 :]], axis=1)
        for e in range(chips):
            gram[e] = packed[2 * e : 2 * e + 2]
        for s, offset in enumerate(chip_offsets):
            at, to = chip_peer(*offset)
            send(gram.at[at], gram_in.at[s], sem_gram, (*to, LEAD))
        wait_out(gram.at[pl.ds(0, chips - 1)], sem_gram)
        wait_in(gram_in.at[pl.ds(0, chips - 1)], sem_gram)
        gram_z[...] = jnp.sum(gram_in[0 : chips - 1], axis=0) + gram[chip]
        for s, (o,) in enumerate(z_offsets):
            send(gram_z, gram_z_in.at[s], sem_gram_z, z_peer(o))
        wait(gram_z_in, sem_gram_z)
        gram_all[chip] = jnp.sum(gram_z_in[...], axis=0) + gram_z[...]
        for offset in chip_offsets:
            for other in range(CORE):
                send(gram_all.at[chip], gram_all.at[chip], sem_all, (*chip_peer(*offset)[1], other))
        send(gram_all.at[chip], gram_all.at[chip], sem_all, (*chip_peer(0, 0)[1], 1 - LEAD))
        wait_out(tile.at[1], sem_tile)
        wait_out(gram_in, sem_all)
        wait_in(gram_all.at[pl.ds(0, chips - 1)], sem_all)

    @pl.when(jnp.logical_not(leads))
    def _():
        wait_out(zpart, sem_z)
        wait_out(zaux, sem_z, 1)
        wait_in(tile.at[0], sem_tile)
        spread[...] = jnp.concatenate(columns(tile[0], 0), axis=0)
        wait_in(gram_all, sem_all)

    half = comps // 2
    packed = gram_all[...].reshape(half, LANES)
    in_gram = lax.broadcasted_iota(jnp.int32, (half, LANES), 1) >= comps
    joint = jnp.concatenate(
        [
            jnp.where(in_gram, pltpu.roll(packed, comps, 1), spread[0:half]),
            jnp.where(in_gram, packed, spread[half:comps]),
        ],
        axis=0,
    )
    out[...] = solve(joint, comps).T[0:width]


def on_device(counts, occupancy, start_basis):
    comps, genes = start_basis.shape
    cells = counts.shape[0]
    rows = comps // Y
    plane = H * XL * CORE * Y
    tiles = 2 * len(DIRECT) + len(PAIRED)
    dma = pltpu.SemaphoreType.DMA
    hbm = pl.BlockSpec(memory_space=pltpu.HBM)
    basis_now = pl.pallas_call(
        kernel,
        out_shape=jax.ShapeDtypeStruct((LANES // Y, comps), F32),
        in_specs=[hbm, hbm, hbm],
        out_specs=pl.BlockSpec(memory_space=pltpu.VMEM),
        scratch_shapes=[
            pltpu.VMEM((cells, genes), BF16),
            pltpu.SMEM(occupancy.shape, jnp.int32),
            pltpu.VMEM((comps, genes), BF16),
            pltpu.VMEM((cells, genes), BF16),
            pltpu.VMEM((16, genes), BF16),
            pltpu.VMEM((H, Z, LANES), F32),
            pltpu.VMEM((H, 8, LANES), F32),
            pltpu.VMEM((H * Y - 1, 8, LANES), F32),
            pltpu.VMEM((H, 8, LANES), F32),
            pltpu.VMEM((H, 8, LANES), F32),
            pltpu.VMEM((H, 8, LANES), F32),
            pltpu.VMEM((H * Y - 1, 8, LANES), F32),
            pltpu.VMEM((comps + 8, LANES), F32),
            pltpu.VMEM((XL * CORE - 1, comps + 8, LANES), F32),
            pltpu.VMEM((H, Y, 2 * len(DIRECT), rows, LANES), F32),
            pltpu.VMEM((2 * len(DIRECT), H * Y - 1, rows, LANES), F32),
            pltpu.VMEM((H, Y, len(PAIRED), rows, LANES), F32),
            pltpu.VMEM((len(PAIRED), H * Y - 1, rows, LANES), F32),
            pltpu.VMEM((H, len(PAIRED), Y, rows, LANES), F32),
            pltpu.VMEM((H, len(PAIRED), Y, rows, LANES), F32),
            pltpu.VMEM((H, Y, 8, LANES), F32),
            pltpu.VMEM((2, H * Y, 8, LANES), F32),
            pltpu.VMEM((2, 8, LANES), F32),
            pltpu.VMEM((LANES, LANES), F32),
            pltpu.VMEM((tiles, rows, LANES), F32),
            pltpu.VMEM((tiles, 2, LANES), F32),
            pltpu.VMEM((CORE * tiles - 1, rows, LANES), F32),
            pltpu.VMEM((CORE * tiles - 1, 2, LANES), F32),
            pltpu.VMEM((CORE, rows, LANES), F32),
            pltpu.VMEM((comps, LANES), F32),
            pltpu.VMEM((plane // CORE, 2, LANES), F32),
            pltpu.VMEM((plane - 1, 2, LANES), F32),
            pltpu.VMEM((2, LANES), F32),
            pltpu.VMEM((Z - 1, 2, LANES), F32),
            pltpu.VMEM((plane // CORE, 2, LANES), F32),
            dma((len(LOADS) + 2,)),
            dma((2, 2)),
            dma((2, 1)),
            dma((2, 1)),
            dma((2, 1)),
            dma((2, len(DIRECT))),
            dma((2, len(PAIRED))),
            dma((2, len(PAIRED))),
            dma((2, 2)),
            dma((2, 1)),
            dma((2, 1)),
            dma((2, 1)),
            dma((2, 1)),
            pltpu.SemaphoreType.REGULAR,
            pltpu.SemaphoreType.REGULAR,
        ],
        compiler_params=pltpu.CompilerParams(
            collective_id=0, has_side_effects=True, vmem_limit_bytes=24 << 20
        ),
        name="subspace_step",
    )(*(pltpu.with_memory_space_constraint(a, pltpu.HBM) for a in (counts, occupancy, start_basis)))
    return basis_now.T * math.sqrt(genes * XL * CORE)


def solution(mesh):
    placed = (P("cells", "genes"), P("cells", "genes"), P(None, "genes"))
    return jax.shard_map(
        on_device, mesh=mesh, in_specs=placed, out_specs=P(None, ("genes", "cells")), check_vma=False
    )
```

```python
import math

import jax
import jax.numpy as jnp
from jax import lax
from jax.experimental import pallas as pl
from jax.experimental.pallas import tpu as pltpu
from jax.sharding import PartitionSpec as P

F32 = jnp.float32
BF16 = jnp.bfloat16
MESH = pl.DeviceIdType.MESH
Z, H, Y, XL, CORE = 16, 2, 4, 2, 2
LANES = 128
DIRECT = (8, 10)
PAIRED = (6, 4, 12, 2, 14, 0)
SCORE_ROW = 7
LEAD = 1
LOADS = (16, 16)
NT = (((1,), (1,)), ((), ()))


def device(z, h, y, xl, core):
    return ((z * H + h) * Y + y, xl * CORE + core)


def far_first(offsets, weights, sizes):
    def far(offset):
        return -sum(w * min(o, n - o) for o, w, n in zip(offset, weights, sizes))

    return sorted((o for o in offsets if any(o)), key=far)


def total_of(values):
    values = list(values)
    while len(values) > 1:
        values = [sum(values[i : i + 2][1:], values[i]) for i in range(0, len(values), 2)]
    return values[0]


def solve(joint, start):
    blocks = joint.shape[0] // 8
    joint = [joint[8 * b : 8 * b + 8] for b in range(blocks)]
    row_at = lax.broadcasted_iota(jnp.int32, (8, LANES), 0)
    done = []
    for kb in range(blocks):
        cols = []
        for b in range(kb, blocks):
            at = start + 8 * kb
            cols.append(
                [jnp.broadcast_to(joint[b][:, at + j : at + j + 1], (8, LANES)) for j in range(8)]
            )
        block = joint[kb]
        scale = jnp.zeros((8, LANES), F32)
        steps = []
        for j in range(8):
            pivot = jnp.broadcast_to(cols[0][j][j : j + 1], (8, LANES))
            inv = lax.rsqrt(pivot)
            scale = jnp.where(row_at == j, inv, scale)
            lower = [c[j] * inv for c in cols]
            for m in range(j + 1, 8):
                entry = jnp.broadcast_to(lower[0][m : m + 1], (8, LANES))
                for c, low in zip(cols, lower):
                    c[m] = c[m] - low * entry
            unit = jnp.broadcast_to(block[j : j + 1], (8, LANES)) * inv
            block = block - jnp.where(row_at > j, lower[0], 0.0) * unit
            steps.append((lower[1:], unit))
        done.append(block * scale)
        for at, b in enumerate(range(kb + 1, blocks)):
            for lower, unit in steps:
                joint[b] = joint[b] - lower[at] * unit
    return jnp.concatenate(done, axis=0)


def kernel(
    counts_hbm,
    occupancy_hbm,
    basis_hbm,
    out,
    counts,
    occupancy,
    basis,
    cbuf,
    split_mean,
    mean_all,
    means_direct,
    means_direct_in,
    means_out,
    means_out_in,
    means_paired,
    means_paired_in,
    score,
    score_in,
    direct,
    direct_in,
    paired,
    paired_in,
    pair_out,
    pair_in,
    pair_dev,
    dev_mean,
    mean_xy,
    turned,
    zpart,
    zaux,
    zpart_in,
    zaux_in,
    tile,
    spread,
    gram,
    gram_in,
    gram_z,
    gram_z_in,
    gram_all,
    sem_in,
    sem_score,
    sem_means,
    sem_means_out,
    sem_means_paired,
    sem_direct,
    sem_pair,
    sem_paired,
    sem_z,
    sem_tile,
    sem_gram,
    sem_gram_z,
    sem_all,
    sem_beyond,
    sem_far,
):
    cells_at, genes_at = lax.axis_index("cells"), lax.axis_index("genes")
    z, h, y = cells_at // (H * Y), lax.rem(cells_at // Y, H), lax.rem(cells_at, Y)
    xl, core = genes_at // CORE, lax.rem(genes_at, CORE)
    comps = basis.shape[0]
    rows = comps // Y
    cells = counts.shape[0]
    width = LANES // Y
    plane = H * XL * CORE * Y

    loads = [pltpu.make_async_copy(occupancy_hbm, occupancy, sem_in.at[0])]
    tiles = [(sum(LOADS[:c]), sum(LOADS[: c + 1])) for c in range(len(LOADS))]
    spans = [pl.ds(first * LANES, (last - first) * LANES) for first, last in tiles]
    for c, span in enumerate(spans):
        loads.append(
            pltpu.make_async_copy(counts_hbm.at[:, span], counts.at[:, span], sem_in.at[c + 1])
        )
    loads.append(pltpu.make_async_copy(basis_hbm, basis, sem_in.at[len(LOADS) + 1]))
    for load in loads:
        load.start()

    def send(src, dst, sems, to, step=0):
        pltpu.make_async_remote_copy(
            src_ref=src,
            dst_ref=dst,
            send_sem=sems.at[0, step],
            recv_sem=sems.at[1, step],
            device_id=to if len(to) == 2 else device(*to),
            device_id_type=MESH,
        ).start()

    def waiting(all_bytes, sems, step):
        return pltpu.make_async_remote_copy(
            src_ref=all_bytes,
            dst_ref=all_bytes,
            send_sem=sems.at[0, step],
            recv_sem=sems.at[1, step],
            device_id=(cells_at, genes_at),
            device_id_type=MESH,
        )

    def wait_out(all_bytes, sems, step=0):
        waiting(all_bytes, sems, step).wait_send()

    def wait_in(all_bytes, sems, step=0):
        waiting(all_bytes, sems, step).wait_recv()

    def wait(all_bytes, sems, step=0):
        wait_out(all_bytes, sems, step)
        wait_in(all_bytes, sems, step)

    def gene_peer(a, b):
        return device(z, h, y, lax.rem(xl + a, XL), lax.rem(core + b, CORE))

    def z_peer(o):
        return device(lax.rem(z + o + Z, Z), h, y, xl, core)

    in_x = h * XL + xl
    chip = in_x * Y + y

    def chip_peer(a, c):
        xt, yt = lax.rem(in_x + a, H * XL), lax.rem(y + c, Y)
        return xt * Y + yt, (z, xt // XL, yt, lax.rem(xt, XL))

    def z_tile(o):
        return lax.rem(z + o + Z, Z)

    beside = [1 - 2 * lax.rem(z + ht, 2) for ht in range(H)]
    own_beside = 1 - 2 * lax.rem(z + h, 2)

    gene_offsets = [(1, 0), (1, 1), (0, 1)]
    xy_offsets = far_first([(a, b) for a in range(H) for b in range(Y)], (4, 2), (H, Y))
    xy_peers = []
    for a, b in xy_offsets:
        ht, yt = lax.rem(h + a, H), lax.rem(y + b, Y)
        xy_peers.append((ht, yt, device(z, ht, yt, xl, core)))
    chip_offsets = far_first([(a, c) for a in range(H * XL) for c in range(Y)], (1, 1), (H * XL, Y))
    z_offsets = far_first([(o,) for o in range(Z)], (1,), (Z,))

    barrier = pltpu.get_barrier_semaphore()
    beyond = [device(z, h, lax.rem(y + b, Y), xl, core) for b in range(1, Y)] + [z_peer(2), z_peer(-2)]
    peers = [gene_peer(a, b) for a, b in gene_offsets] + beyond
    peers += [device(z, 1 - h, y, xl, core), z_peer(1), z_peer(-1)]
    peers += [device(z_tile(o), h, y, xl, 1 - core) for o in (1, -1, 2, -2)]
    for peer in peers:
        pl.semaphore_signal(barrier, inc=1, device_id=peer, device_id_type=MESH)

    row_at = lax.broadcasted_iota(jnp.int32, (16, LANES), 0)
    group_at = lax.broadcasted_iota(jnp.int32, (16, LANES), 1) // width
    for ref in (means_direct, means_out, means_paired):
        ref[...] = jnp.zeros(ref.shape, F32)
    turned[...] = jnp.zeros((LANES, LANES), F32)

    def center(j):
        at = pl.ds(j * LANES, LANES)
        entries = counts[:, at].astype(F32)
        logged = jnp.log(1.0 + entries) * occupancy[0, j].astype(F32)
        mean = jnp.sum(logged, axis=0, keepdims=True) * (1.0 / cells)
        cbuf[:, at] = (logged - mean).astype(BF16)
        mean_all[j % H, j // H : j // H + 1, :] = mean

    def product_of(c):
        span = spans[c]
        return lax.dot_general(basis[:, span], cbuf[:, span], NT, preferred_element_type=F32)

    loads[0].wait()
    products = []
    for c in range(len(LOADS)):
        loads[c + 1].wait()
        if c == 1:
            loads[-1].wait()
        if c:
            products.append(product_of(c - 1))
        for j in range(*tiles[c]):
            center(j)
    products.append(product_of(len(LOADS) - 1))
    score[0:comps, :] = total_of(products)

    pl.semaphore_wait(barrier, len(peers))
    for peer in beyond:
        pl.semaphore_signal(sem_beyond, inc=1, device_id=peer, device_id_type=MESH)
    of_cells, of_means = pl.ds(0, comps), pl.ds(comps, 8)

    def send_scores(span, step):
        for s, (a, b) in enumerate(gene_offsets):
            send(score.at[span], score_in.at[s, span], sem_score, gene_peer(a, b), step)

    send_scores(of_cells, 0)
    for j in range(Z * H):
        mean = mean_all[j % H, j // H : j // H + 1, :]
        high = mean.astype(BF16).astype(F32)
        middle = (mean - high).astype(BF16).astype(F32)
        low = mean - high - middle
        stacked = jnp.where(
            row_at == 0, high, jnp.where(row_at == 1, middle, jnp.where(row_at == 2, low, 0.0))
        )
        split_mean[:, j * LANES : (j + 1) * LANES] = stacked.astype(BF16)
    of_mean = lax.dot_general(split_mean[...], basis[...], NT, preferred_element_type=F32)
    score[comps : comps + 8, :] = jnp.zeros((8, LANES), F32)
    score[comps : comps + 1, 0:comps] = of_mean[0:1] + of_mean[1:2] + of_mean[2:3]
    send_scores(of_means, 1)
    for ht in range(H):
        for i in range(2 * len(DIRECT)):
            at = z_tile(DIRECT[i // 2] + i % 2 * beside[ht])
            means_direct[ht, i : i + 1, :] = mean_all[ht, pl.ds(at, 1), :]
        for j, e in enumerate(PAIRED):
            means_out[ht, j : j + 1, :] = mean_all[ht, pl.ds(z_tile(e + beside[ht]), 1), :]
            means_paired[ht, j : j + 1, :] = mean_all[ht, pl.ds(z_tile(e), 1), :]
    pl.semaphore_wait(sem_beyond, len(beyond))
    for o in (4, -4):
        pl.semaphore_signal(sem_far, inc=1, device_id=z_peer(o), device_id_type=MESH)
    wait(score_in.at[:, of_cells], sem_score)
    scores = total_of([score[0:comps]] + [score_in[a, 0:comps] for a in range(XL * CORE - 1)])
    score_high = scores.astype(BF16)
    score_low = (scores - score_high.astype(F32)).astype(BF16)
    stacked = jnp.concatenate([score_high, score_low], axis=0)

    def pieces(tiles):
        columns = [
            cbuf[:, pl.ds(pl.multiple_of((tiles[ht] * H + ht) * LANES, LANES), LANES)] for ht in range(H)
        ]
        both = jnp.dot(stacked, jnp.concatenate(columns, axis=1), preferred_element_type=F32)
        product = both[:comps] + both[comps:]
        result = []
        for ht in range(H):
            turns = []
            for b in range(Y):
                block = product[b * rows : (b + 1) * rows, ht * LANES : (ht + 1) * LANES]
                turns.append([block] + [pltpu.roll(block, k * width, 1) for k in range(1, Y)])
            for yt in range(Y):
                piece = turns[0][(0 - yt) % Y]
                for b in range(1, Y):
                    piece = jnp.where(group_at == b, turns[b][(b - yt) % Y], piece)
                result.append((ht, yt, piece))
        return result

    def exchange(src, dst, sems, chunk, span):
        for s, (ht, yt, to) in enumerate(xy_peers):
            send(src.at[ht, yt, span], dst.at[span, s], sems, to, chunk)

    def start_direct(j):
        for i in (2 * j, 2 * j + 1):
            tiles = [z_tile(DIRECT[j] + i % 2 * beside[ht]) for ht in range(H)]
            for ht, yt, piece in pieces(tiles):
                direct[ht, yt, i] = piece
        exchange(direct, direct_in, sem_direct, j, pl.ds(2 * j, 2))

    def start_pair(j):
        for ht, yt, piece in pieces([z_tile(PAIRED[j] + beside[ht]) for ht in range(H)]):
            pair_out[ht, j, yt] = piece
        for ht in range(H):
            send(pair_out.at[ht, j], pair_in.at[ht, j], sem_pair, z_peer(beside[ht]), j)

    def send_means():
        wait(score_in.at[:, of_means], sem_score, 1)
        whole = total_of(
            [score[comps : comps + 1]]
            + [score_in[a, comps : comps + 1] for a in range(XL * CORE - 1)]
        )
        for ht in range(H):
            for ref in (means_direct, means_out, means_paired):
                ref[ht, SCORE_ROW : SCORE_ROW + 1, :] = whole
            send(means_out.at[ht], means_out_in.at[ht], sem_means_out, z_peer(beside[ht]))
        for s, (ht, _, to) in enumerate(xy_peers):
            send(means_direct.at[ht], means_direct_in.at[s], sem_means, to)

    start_pair(0)
    send_means()
    start_direct(0)
    start_pair(1)
    start_direct(1)
    for j in range(2, len(PAIRED)):
        start_pair(j)
    for j, e in enumerate(PAIRED):
        for ht, yt, piece in pieces([z_tile(e)] * H):
            paired[ht, yt, j] = piece

    def fold_rows(values):
        for p, value in enumerate(values):
            turned[p : p + 1, :] = value
        flat = turned[...].T
        result = []
        for p in range(len(values)):
            folded = jnp.broadcast_to(flat[0:rows, p : p + 1], (rows, LANES))
            for b in range(1, Y):
                block = jnp.broadcast_to(flat[b * rows : (b + 1) * rows, p : p + 1], (rows, LANES))
                folded = jnp.where(group_at == b, block, folded)
            result.append(folded)
        return result

    def columns_of(means, yt):
        kept = jnp.where(group_at[0:8] == yt, means, 0.0)
        return total_of([kept] + [pltpu.roll(kept, k * width, 1) for k in range(1, Y)])

    groups = len(xy_offsets) + 1

    def plane_terms(level, weight, own, others):
        values = [own[h]] + [others[s] for s in range(groups - 1)]
        middle = total_of(values) * (1.0 / groups)
        apart = [value - middle for value in values]
        away = fold_rows([a[SCORE_ROW : SCORE_ROW + 1] * weight for a in apart])
        mean_xy[level] = columns_of(middle, y)
        for p, value in enumerate(apart):
            dev_mean[level, p] = columns_of(value, y)
        return middle[SCORE_ROW : SCORE_ROW + 1], away

    wait(means_out_in, sem_means_out)
    apart = [means_paired[ht] - means_out_in[ht] for ht in range(H)]
    pair_away = fold_rows([a[SCORE_ROW : SCORE_ROW + 1] * (0.5 * cells) for a in apart])
    for ht in range(H):
        means_paired[ht] = 0.5 * (means_paired[ht] + means_out_in[ht])
        for yt in range(Y):
            pair_dev[ht, yt] = columns_of(apart[ht], yt)
    for s, (ht, _, to) in enumerate(xy_peers):
        send(means_paired.at[ht], means_paired_in.at[s], sem_means_paired, to)

    def add_pair(j):
        wait(pair_in.at[:, j], sem_pair, j)
        for ht in range(H):
            for yt in range(Y):
                paired[ht, yt, j] = (paired[ht, yt, j] + pair_in[ht, j, yt]) + pair_away[
                    ht
                ] * pair_dev[ht, yt, j : j + 1, :]
        exchange(paired, paired_in, sem_paired, j, pl.ds(j, 1))

    leads = core == LEAD
    last = 2 * len(DIRECT) + len(PAIRED) - 1
    after_leads = (CORE - 1 - core) * last

    def lead_peer(o):
        return device(z_tile(o), h, y, xl, LEAD)

    def plane_sum(level, slot, own, others, i, away, middle, to):
        terms = [own[h, y, i]] + [others[i, s] for s in range(groups - 1)]
        terms += [away[p] * dev_mean[level, p, i : i + 1, :] for p in range(groups)]
        zpart[slot] = total_of(terms)
        zaux[slot, 0:1, :] = mean_xy[level, i : i + 1, :]
        zaux[slot, 1:2, :] = middle
        def send_sum():
            send(zpart.at[slot], zpart_in.at[slot + after_leads], sem_z, to)
            send(zaux.at[slot], zaux_in.at[slot + after_leads], sem_z, to, 1)

        if slot < last:
            send_sum()
        else:
            pl.when(jnp.logical_not(leads))(send_sum)

    def sum_direct(j):
        wait(direct_in.at[pl.ds(2 * j, 2)], sem_direct, j)
        for i in (2 * j, 2 * j + 1):
            to = lead_peer(DIRECT[j] + i % 2 * own_beside)
            plane_sum(0, i, direct, direct_in, i, away_direct, score_direct, to)

    for j in range(len(PAIRED) - 1):
        add_pair(j)
    wait(means_direct_in, sem_means)
    score_direct, away_direct = plane_terms(0, float(cells), means_direct, means_direct_in)
    pl.semaphore_wait(sem_far, 2)
    sum_direct(0)
    add_pair(len(PAIRED) - 1)
    sum_direct(1)
    wait(means_paired_in, sem_means_paired)
    score_paired, away_paired = plane_terms(1, 2.0 * cells, means_paired, means_paired_in)
    alone = 2 * len(DIRECT)
    for j, e in enumerate(PAIRED):
        wait(paired_in.at[pl.ds(j, 1)], sem_paired, j)
        plane_sum(1, alone + j, paired, paired_in, j, away_paired, score_paired, lead_peer(e))
    def columns(folded, group):
        turns = [pltpu.roll(folded, (Y - b + group) % Y * width, 1) if b != group else folded for b in range(Y)]
        return [jnp.where(group_at == group, turn, 0.0) for turn in turns]

    chips = plane // CORE

    @pl.when(leads)
    def _():
        wait_out(zpart.at[pl.ds(0, last)], sem_z)
        wait_out(zaux.at[pl.ds(0, last)], sem_z, 1)
        wait_in(zpart_in, sem_z)
        wait_in(zaux_in, sem_z, 1)
        shares = [1.0] * alone + [2.0] * len(PAIRED)
        scores_of = [zaux_in[i, 1:2, :] for i in range(last)] + [zaux[last, 1:2, :]]
        middle = total_of([v * w for v, w in zip(scores_of, shares)]) * (1.0 / Z)
        away = fold_rows([(v - middle) * (w * cells * groups) for v, w in zip(scores_of, shares)])
        own = [zpart_in[i] for i in range(last)] + [zpart[last]]
        own_means = [zaux_in[i, 0:1, :] for i in range(last)] + [zaux[last, 0:1, :]]
        others = [zpart_in[i] for i in range(last, 2 * last + 1)]
        other_means = [zaux_in[i, 0:1, :] for i in range(last, 2 * last + 1)]
        for t, (sums, means) in enumerate(((own, own_means), (others, other_means))):
            middle = total_of([v * w for v, w in zip(means, shares)]) * (1.0 / Z)
            tile[t] = total_of(sums + [far * (v - middle) for far, v in zip(away, means)])
        send(tile.at[1], tile.at[0], sem_tile, (z, h, y, xl, 1 - LEAD))
        both = [a + b for a, b in zip(columns(tile[0], 0), columns(tile[1], 1))]
        spread[...] = jnp.concatenate(both, axis=0)
        own_gram = lax.dot_general(
            spread[...], spread[...], NT, precision=lax.Precision.HIGHEST, preferred_element_type=F32
        )
        packed = jnp.concatenate([own_gram[0 : comps // 2], own_gram[comps // 2 :]], axis=1)
        for e in range(chips):
            gram[e] = packed[2 * e : 2 * e + 2]
        for s, offset in enumerate(chip_offsets):
            at, to = chip_peer(*offset)
            send(gram.at[at], gram_in.at[s], sem_gram, (*to, LEAD))
        wait_out(gram.at[pl.ds(0, chips - 1)], sem_gram)
        wait_in(gram_in.at[pl.ds(0, chips - 1)], sem_gram)
        gram_z[...] = jnp.sum(gram_in[0 : chips - 1], axis=0) + gram[chip]
        for s, (o,) in enumerate(z_offsets):
            send(gram_z, gram_z_in.at[s], sem_gram_z, z_peer(o))
        wait(gram_z_in, sem_gram_z)
        gram_all[chip] = jnp.sum(gram_z_in[...], axis=0) + gram_z[...]
        for offset in chip_offsets:
            for other in range(CORE):
                send(gram_all.at[chip], gram_all.at[chip], sem_all, (*chip_peer(*offset)[1], other))
        send(gram_all.at[chip], gram_all.at[chip], sem_all, (*chip_peer(0, 0)[1], 1 - LEAD))
        wait_out(tile.at[1], sem_tile)
        wait_out(gram_in, sem_all)
        wait_in(gram_all.at[pl.ds(0, chips - 1)], sem_all)

    @pl.when(jnp.logical_not(leads))
    def _():
        wait_out(zpart, sem_z)
        wait_out(zaux, sem_z, 1)
        wait_in(tile.at[0], sem_tile)
        spread[...] = jnp.concatenate(columns(tile[0], 0), axis=0)
        wait_in(gram_all, sem_all)

    half = comps // 2
    packed = gram_all[...].reshape(half, LANES)
    in_gram = lax.broadcasted_iota(jnp.int32, (half, LANES), 1) >= comps
    joint = jnp.concatenate(
        [
            jnp.where(in_gram, pltpu.roll(packed, comps, 1), spread[0:half]),
            jnp.where(in_gram, packed, spread[half:comps]),
        ],
        axis=0,
    )
    out[...] = solve(joint, comps).T[0:width]


def on_device(counts, occupancy, start_basis):
    comps, genes = start_basis.shape
    cells = counts.shape[0]
    rows = comps // Y
    plane = H * XL * CORE * Y
    tiles = 2 * len(DIRECT) + len(PAIRED)
    dma = pltpu.SemaphoreType.DMA
    hbm = pl.BlockSpec(memory_space=pltpu.HBM)
    basis_now = pl.pallas_call(
        kernel,
        out_shape=jax.ShapeDtypeStruct((LANES // Y, comps), F32),
        in_specs=[hbm, hbm, hbm],
        out_specs=pl.BlockSpec(memory_space=pltpu.VMEM),
        scratch_shapes=[
            pltpu.VMEM((cells, genes), BF16),
            pltpu.SMEM(occupancy.shape, jnp.int32),
            pltpu.VMEM((comps, genes), BF16),
            pltpu.VMEM((cells, genes), BF16),
            pltpu.VMEM((16, genes), BF16),
            pltpu.VMEM((H, Z, LANES), F32),
            pltpu.VMEM((H, 8, LANES), F32),
            pltpu.VMEM((H * Y - 1, 8, LANES), F32),
            pltpu.VMEM((H, 8, LANES), F32),
            pltpu.VMEM((H, 8, LANES), F32),
            pltpu.VMEM((H, 8, LANES), F32),
            pltpu.VMEM((H * Y - 1, 8, LANES), F32),
            pltpu.VMEM((comps + 8, LANES), F32),
            pltpu.VMEM((XL * CORE - 1, comps + 8, LANES), F32),
            pltpu.VMEM((H, Y, 2 * len(DIRECT), rows, LANES), F32),
            pltpu.VMEM((2 * len(DIRECT), H * Y - 1, rows, LANES), F32),
            pltpu.VMEM((H, Y, len(PAIRED), rows, LANES), F32),
            pltpu.VMEM((len(PAIRED), H * Y - 1, rows, LANES), F32),
            pltpu.VMEM((H, len(PAIRED), Y, rows, LANES), F32),
            pltpu.VMEM((H, len(PAIRED), Y, rows, LANES), F32),
            pltpu.VMEM((H, Y, 8, LANES), F32),
            pltpu.VMEM((2, H * Y, 8, LANES), F32),
            pltpu.VMEM((2, 8, LANES), F32),
            pltpu.VMEM((LANES, LANES), F32),
            pltpu.VMEM((tiles, rows, LANES), F32),
            pltpu.VMEM((tiles, 2, LANES), F32),
            pltpu.VMEM((CORE * tiles - 1, rows, LANES), F32),
            pltpu.VMEM((CORE * tiles - 1, 2, LANES), F32),
            pltpu.VMEM((CORE, rows, LANES), F32),
            pltpu.VMEM((comps, LANES), F32),
            pltpu.VMEM((plane // CORE, 2, LANES), F32),
            pltpu.VMEM((plane - 1, 2, LANES), F32),
            pltpu.VMEM((2, LANES), F32),
            pltpu.VMEM((Z - 1, 2, LANES), F32),
            pltpu.VMEM((plane // CORE, 2, LANES), F32),
            dma((len(LOADS) + 2,)),
            dma((2, 2)),
            dma((2, 1)),
            dma((2, 1)),
            dma((2, 1)),
            dma((2, len(DIRECT))),
            dma((2, len(PAIRED))),
            dma((2, len(PAIRED))),
            dma((2, 2)),
            dma((2, 1)),
            dma((2, 1)),
            dma((2, 1)),
            dma((2, 1)),
            pltpu.SemaphoreType.REGULAR,
            pltpu.SemaphoreType.REGULAR,
        ],
        compiler_params=pltpu.CompilerParams(
            collective_id=0, has_side_effects=True, vmem_limit_bytes=24 << 20
        ),
        name="subspace_step",
    )(*(pltpu.with_memory_space_constraint(a, pltpu.HBM) for a in (counts, occupancy, start_basis)))
    return basis_now.T * math.sqrt(genes * XL * CORE)


def solution(mesh):
    placed = (P("cells", "genes"), P("cells", "genes"), P(None, "genes"))
    return jax.shard_map(
        on_device, mesh=mesh, in_specs=placed, out_specs=P(None, ("genes", "cells")), check_vma=False
    )
```
